32 devices in a mesh: groups: 2 (over y), section: 4 (over z), tp: 2 (over core), sp: 2 (over x).
Axes of the slice: x: 2, y: 2, z: 4, core: 2. Of those that a mesh axis runs over, the one named last changes fastest.
Arguments:
- hidden: bfloat16 [1024, 6144], P(('groups', 'sp', 'section'), 'tp'), parts along dimension 0, may hold values from -6 to 6
- modulation: float32 [2, 6144], P(None, 'tp'), may hold values from -2 to 2
- time_embed: float32 [12288], P(('groups', 'tp')), parts along dimension 0, may hold values from -2 to 2
- head_weight: bfloat16 [6144, 64], P('tp'), may hold values from -0.078125 to 0.078125
- head_bias: float32 [64], replicated, may hold values from -2 to 2
- noisy: bfloat16 [16, 16, 16, 16], P(('groups', 'sp'), None, 'section'), parts along dimension 0, may hold values from -6 to 6
- step_size: float32 [2], P('groups'), parts along dimension 0, may hold values from 0.2 to 0.6
- latent_mean: float32 [16], replicated, may hold values from -2 to 2
- latent_std: float32 [16], replicated, may hold values from 0.5 to 2
- in_weight: bfloat16 [27, 16, 512], P(None, None, 'tp'), may hold values from -0.3125 to 0.3125
- in_bias: float32 [512], P('tp'), may hold values from -2 to 2
- norm_gain: float32 [512], replicated, may hold values from 0.25 to 1.75
- conv_weight: bfloat16 [27, 512, 512], P(None, 'section', 'tp'), may hold values from -0.0546875 to 0.0546875
- conv_bias: float32 [512], P('tp'), may hold values from -2 to 2
Outputs:
- decoded: bfloat16 [16, 16, 16, 512], P(('groups', 'sp'), None, 'section', 'tp'), parts along dimension 0
The draws below stay inside these ranges and needn't reach their ends.
There are 2 independent parts, one for each index of `groups`. The reference program is written for one: setup_inputs(seed, part) draws one part's arguments, and reference() takes and returns one part's arrays. A program takes and returns all parts, laid end to end along the dimension named above; an argument that names none is the same for every part. Nothing has to cross between parts.
All inputs are finite; a program needn't handle non-finite values.
Results may differ from the reference program's by a relative error of at most 0.006.
Values may be sent and summed in bfloat16 or wider, within the bound.
A program may use at most 128 MiB of HBM per device.

```python
import math
import jax
import jax.numpy as jnp
from jax import lax

D = 6144
LAT_CH = 16
CH = 512
HEIGHT = 16
PCH = 64
FRAMES = 8
WIDTH = 16
TOKENS = 512


def block_scale(own_key, dims, shards, low, high):
    gain = 1.0
    for dim, blocks in shards:
        steps = jax.random.uniform(jax.random.fold_in(jax.random.fold_in(own_key, 6), dim), (blocks,), jnp.float32, low / len(shards), high / len(shards))
        gain = gain * jnp.repeat(jnp.exp(steps), dims[dim] // blocks).reshape((-1,) + (1,) * (len(dims) - 1 - dim))
    return gain


def gaussian(stream_key, dims, scale, bound, cuts=(), dtype=jnp.bfloat16):
    values = scale * jax.random.normal(stream_key, dims, jnp.float32)
    if cuts:
        values = values * block_scale(stream_key, dims, cuts, -0.22, 0.18)
    return jnp.clip(values, -bound, bound).astype(dtype)


def setup_inputs(seed: int = 0, part: int = 0) -> dict:
    arg_keys = jax.random.split(jax.random.key(seed), 15)
    part_splits = jax.random.split(jax.random.fold_in(arg_keys[14], part), 15)
    return {
        "hidden": gaussian(part_splits[0], (TOKENS, D), 1.0, 6.0, ((0, 8), (1, 2))),
        "modulation": gaussian(arg_keys[1], (2, D), 0.3, 2.0, ((1, 2),), jnp.float32),
        "time_embed": gaussian(part_splits[2], (D,), 0.3, 2.0, ((0, 2),), jnp.float32),
        "head_weight": gaussian(arg_keys[3], (D, PCH), D ** -0.5, 0.078125, ((0, 2),)),
        "head_bias": gaussian(arg_keys[4], (PCH,), 0.3, 2.0, (), jnp.float32),
        "noisy": gaussian(part_splits[5], (FRAMES, HEIGHT, WIDTH, LAT_CH), 1.0, 6.0, ((0, 2), (2, 4))),
        "step_size": jnp.clip(jax.random.uniform(part_splits[6], (1,), jnp.float32, 0.2, 0.6), 0.2, 0.6),
        "latent_mean": gaussian(arg_keys[7], (LAT_CH,), 0.5, 2.0, (), jnp.float32),
        "latent_std": jnp.clip(jnp.exp(jax.random.uniform(arg_keys[8], (LAT_CH,), jnp.float32, math.log(0.5), math.log(2.0))), 0.5, 2.0),
        "in_weight": gaussian(arg_keys[9], (27, LAT_CH, CH), (27 * LAT_CH) ** -0.5, 0.3125, ((2, 2),)),
        "in_bias": gaussian(arg_keys[10], (CH,), 0.3, 2.0, ((0, 2),), jnp.float32),
        "norm_gain": jnp.clip(1.0 + 0.15 * jax.random.normal(arg_keys[11], (CH,), jnp.float32), 0.25, 1.75),
        "conv_weight": gaussian(arg_keys[12], (27, CH, CH), (27 * CH) ** -0.5, 0.0546875, ((1, 4), (2, 2))),
        "conv_bias": gaussian(arg_keys[13], (CH,), 0.3, 2.0, ((0, 2),), jnp.float32),
    }


def conv_taps(padded, weight, frames, height, columns):
    channels = padded.shape[3]
    result = jnp.zeros((frames * height * columns, weight.shape[2]), jnp.float32)
    for offset_time in range(3):
        for offset_row in range(3):
            for offset_col in range(3):
                window = padded[offset_time:offset_time + frames, offset_row:offset_row + height, offset_col:offset_col + columns]
                result = result + jnp.dot(window.reshape(-1, channels), weight[9 * offset_time + 3 * offset_row + offset_col], preferred_element_type=jnp.float32)
    return result

def activate(source, gain_vector):
    values = source.astype(jnp.float32)
    squares = lax.optimization_barrier(jnp.mean(values * values, axis=-1, keepdims=True))
    return jax.nn.silu(values * lax.rsqrt(squares + 1e-06) * gain_vector).astype(jnp.bfloat16)

def reference(hidden, modulation, time_embed, head_weight, head_bias, noisy, step_size, latent_mean, latent_std, in_weight, in_bias, norm_gain, conv_weight, conv_bias):
    values = hidden.astype(jnp.float32)
    average = lax.optimization_barrier(jnp.sum(values, axis=1)) / D
    variance = lax.optimization_barrier(jnp.sum(values * values, axis=1)) / D - average * average
    shift_term = modulation[0] + time_embed
    scale_term = modulation[1] + time_embed
    modulated = ((values - average[:, None]) * lax.rsqrt(variance[:, None] + 1e-06) * (1.0 + scale_term) + shift_term).astype(jnp.bfloat16)
    velocity = (jnp.dot(modulated, head_weight, preferred_element_type=jnp.float32) + head_bias).astype(jnp.bfloat16)
    latent_field = velocity.reshape(FRAMES, HEIGHT // 2, WIDTH // 2, 2, 2, LAT_CH)
    latent_field = jnp.transpose(latent_field, (0, 1, 3, 2, 4, 5)).reshape(FRAMES, HEIGHT, WIDTH, LAT_CH)
    latent = ((noisy.astype(jnp.float32) - step_size[0] * latent_field.astype(jnp.float32)) * latent_std + latent_mean).astype(jnp.bfloat16)
    padded = jnp.pad(latent, ((2, 0), (1, 1), (1, 1), (0, 0)))
    upblock = (conv_taps(padded, in_weight, FRAMES, HEIGHT, WIDTH) + in_bias).astype(jnp.bfloat16)
    normed = activate(upblock, norm_gain).reshape(FRAMES, HEIGHT, WIDTH, CH)
    conv_input = jnp.pad(normed, ((2, 0), (1, 1), (1, 1), (0, 0)))
    mixed = conv_taps(conv_input, conv_weight, FRAMES, HEIGHT, WIDTH)
    decoded = (upblock.astype(jnp.float32) + mixed + conv_bias).astype(jnp.bfloat16)
    return decoded.reshape(FRAMES, HEIGHT, WIDTH, CH)
```

```python
import functools

import jax
import jax.numpy as jnp
from jax import lax
from jax.experimental import pallas as pl
from jax.experimental.pallas import tpu as pltpu
from jax.sharding import PartitionSpec as P

D = 6144


def padded_2(value, sides, width):
    for axis, dim in sides:
        count, length = (lax.axis_size(axis), value.shape[dim])
        up = [(i, (i + 1) % count) for i in range(count - 1)]
        down = [(j, i) for i, j in up]
        last = lax.slice_in_dim(value, length - width, length, axis=dim)
        leading = lax.slice_in_dim(value, 0, width, axis=dim)
        before = lax.ppermute(last, axis, up)
        after = lax.ppermute(leading, axis, down)
        value = jnp.concatenate([before, value, after], axis=dim)
    return value


def passed_along(value, axis, by):
    count = lax.axis_size(axis)
    pairs = [(i, i + by) for i in range(count) if 0 <= i + by < count]
    return lax.ppermute(value, axis, pairs)


def conv_taps(padded, weight, frames, height, columns):
    channels = padded.shape[3]
    result = jnp.zeros((frames * height * columns, weight.shape[2]), jnp.float32)
    for offset_time in range(3):
        for offset_row in range(3):
            slab = padded[offset_time : offset_time + frames, offset_row : offset_row + height]
            window = jnp.concatenate(
                [slab[:, :, 0:columns], slab[:, :, 1 : columns + 1], slab[:, :, 2 : columns + 2]],
                axis=3,
            )
            first = 9 * offset_time + 3 * offset_row
            taps = weight[first : first + 3].reshape(3 * channels, weight.shape[2])
            result = result + jnp.dot(
                window.reshape(-1, 3 * channels), taps, preferred_element_type=jnp.float32
            )
    return result


def activate(source, gain_vector):
    values = source.astype(jnp.float32)
    squares = jnp.mean(values * values, axis=-1, keepdims=True)
    return jax.nn.silu(values * lax.rsqrt(squares + 1e-06) * gain_vector).astype(jnp.bfloat16)


def pad_rows(source):
    return jnp.pad(source, ((0, 0), (1, 1), (0, 0), (0, 0)))


def shards(
    hidden,
    modulation,
    time_embed,
    head_weight,
    head_bias,
    noisy,
    step_size,
    latent_mean,
    latent_std,
    in_weight,
    in_bias,
    norm_gain,
    conv_weight,
    conv_bias,
):
    frames, height, columns, lat_channels = noisy.shape
    sections = lax.axis_size("section")
    half_channels = in_weight.shape[2]
    values = hidden.astype(jnp.float32)
    row_sums, square_sums = lax.psum(
        (jnp.sum(values, axis=1), jnp.sum(values * values, axis=1)), "tp"
    )
    average = row_sums / D
    variance = square_sums / D - average * average
    shift_term = modulation[0] + time_embed
    scale_term = modulation[1] + time_embed
    modulated = (
        (values - average[:, None]) * lax.rsqrt(variance[:, None] + 1e-06) * (1.0 + scale_term)
        + shift_term
    ).astype(jnp.bfloat16)
    partial_sum = jnp.dot(modulated, head_weight, preferred_element_type=jnp.float32)
    velocity = (lax.psum(partial_sum, "tp") + head_bias).astype(jnp.bfloat16)
    band_rows = velocity.shape[0] * 2 // (columns * sections)
    outgoing = velocity.reshape(band_rows, sections, -1)
    arrived = lax.all_to_all(outgoing, "section", split_axis=1, concat_axis=0, tiled=True)
    latent_field = arrived.reshape(frames, height // 2, columns // 2, 2, 2, lat_channels)
    latent_field = jnp.transpose(latent_field, (0, 1, 3, 2, 4, 5)).reshape(
        frames, height, columns, lat_channels
    )
    latent = (
        (noisy.astype(jnp.float32) - step_size[0] * latent_field.astype(jnp.float32)) * latent_std
        + latent_mean
    ).astype(jnp.bfloat16)
    latent_wide = padded_2(latent, (("section", 2),), 2)
    earlier = passed_along(latent_wide, "sp", 1)
    stacked = pad_rows(jnp.concatenate([earlier, latent_wide], axis=0))
    extended = (conv_taps(stacked, in_weight, frames + 2, height, columns + 2) + in_bias).astype(
        jnp.bfloat16
    )
    extended = extended.reshape(frames + 2, height, columns + 2, half_channels)
    upblock_half = extended[2:, :, 1 : columns + 1]
    extended_full = lax.all_gather(extended, "tp", axis=3, tiled=True)
    normed = activate(extended_full, norm_gain)
    frame_index = lax.axis_index("sp") * frames - 2 + jnp.arange(frames + 2, dtype=jnp.int32)
    column_index = (
        lax.axis_index("section") * columns - 1 + jnp.arange(columns + 2, dtype=jnp.int32)
    )
    inside_cols = (column_index >= 0) & (column_index < columns * sections)
    inside = (frame_index >= 0)[:, None, None, None] & inside_cols[None, None, :, None]
    conv_input = pad_rows(jnp.where(inside, normed, jnp.zeros_like(normed)))
    full_weight = lax.all_gather(conv_weight, "section", axis=1, tiled=True)
    mixed = conv_taps(conv_input, full_weight, frames, height, columns)
    decoded = (
        upblock_half.astype(jnp.float32).reshape(-1, half_channels) + mixed + conv_bias
    ).astype(jnp.bfloat16)
    return decoded.reshape(frames, height, columns, half_channels)


def iota(shape, dim):
    return lax.broadcasted_iota(jnp.int32, shape, dim)


def dot(left, right):
    return jnp.dot(left, right, preferred_element_type=jnp.float32)


def dot_rows(left, right):
    return lax.dot_general(
        left, right, (((1,), (1,)), ((), ())), preferred_element_type=jnp.float32
    )


def pieces(value):
    high = value.astype(jnp.bfloat16)
    rest = value - high.astype(jnp.float32)
    middle = rest.astype(jnp.bfloat16)
    low = (rest - middle.astype(jnp.float32)).astype(jnp.bfloat16)
    return high.astype(jnp.float32), middle.astype(jnp.float32), low.astype(jnp.float32)


def block_kernel(
    sizes,
    modulation_far,
    time_far,
    head_bias_far,
    noisy_far,
    step_size,
    std_far,
    mean_far,
    in_bias_far,
    gain_far,
    conv_bias_far,
    hidden_far,
    head_far,
    in_far,
    conv_far,
    out,
    modulation,
    time_embed,
    head_bias,
    noisy,
    latent_std,
    latent_mean,
    in_bias,
    norm_gain,
    conv_bias,
    hidden,
    head_weight,
    in_weight,
    weight,
    swap,
    noise_pick,
    noise_mask,
    places,
    part,
    peer_part,
    peer_weight,
    peer_bias,
    fields,
    noises,
    noise_lines,
    expanded,
    stacked,
    taps_in,
    ups,
    squares,
    wide,
    send_buf,
    recv_buf,
    held,
    acc,
    final,
    load_sems,
    pair_send,
    pair_recv,
    noise_send,
    noise_recv,
    field_send,
    field_recv,
    sum_send,
    sum_recv,
):
    sections, clips_sp, frames, height, columns, lat, channels = sizes
    rows_i, cols_j = height // 2, columns * sections // 2
    width = columns * sections
    tokens = rows_i * cols_j
    near = frames + 2
    half = in_weight.shape[2]
    lanes = 4 * lat
    folded = tokens // 2
    line_size = 4 * 2 * lat
    sec, core, spi = lax.axis_index("section"), lax.axis_index("tp"), lax.axis_index("sp")
    nxt = lax.rem(spi + 1, clips_sp)
    prv = lax.rem(spi + clips_sp - 1, clips_sp)
    has_next, has_prev = spi + 1 < clips_sp, spi > 0
    peer = {"tp": 1 - core}

    barrier = pltpu.get_barrier_semaphore()
    pl.semaphore_signal(barrier, inc=1, device_id=peer)
    for k in range(1, sections):
        pl.semaphore_signal(barrier, inc=1, device_id={"section": lax.rem(sec + k, sections)})

    @pl.when(has_prev)
    def _():
        for k in range(sections):
            pl.semaphore_signal(
                barrier, inc=1, device_id={"section": lax.rem(sec + k, sections), "sp": prv}
            )

    pairs = (
        (head_far, head_weight),
        (modulation_far, modulation),
        (time_far, time_embed),
        (hidden_far, hidden),
        (noisy_far, noisy),
        (in_far, in_weight),
        (in_bias_far, in_bias),
        (head_bias_far, head_bias),
        (std_far, latent_std),
        (mean_far, latent_mean),
        (gain_far, norm_gain),
        (conv_bias_far, conv_bias),
        (conv_far, weight),
    )
    loads = [
        pltpu.make_async_copy(source, target, load_sems.at[n])
        for n, (source, target) in enumerate(pairs)
    ]
    for c in loads:
        c.start()

    def pair_copy(n, source, target):
        return pltpu.make_async_remote_copy(
            source, target, pair_send.at[n], pair_recv.at[n], device_id=peer
        )

    def spread(target, send, recv):
        made, ahead = [], []
        source = target.at[0, 0]
        for k in range(1, sections):
            made.append(
                pltpu.make_async_remote_copy(
                    source, target.at[0, k], send.at[0, k], recv.at[0, k],
                    device_id={"section": lax.rem(sec + k, sections)},
                )
            )
        for k in range(sections):
            ahead.append(
                pltpu.make_async_remote_copy(
                    source, target.at[1, k], send.at[1, k], recv.at[1, k],
                    device_id={"section": lax.rem(sec + k, sections), "sp": nxt},
                )
            )
        return made, ahead

    def spread_start(copies):
        for c in copies[0]:
            c.start()

        @pl.when(has_next)
        def _():
            for c in copies[1]:
                c.start()

    def spread_wait(copies):
        for c in copies[0]:
            c.wait_recv()

        @pl.when(has_prev)
        def _():
            for c in copies[1]:
                c.wait_recv()

    def spread_drain(copies):
        for c in copies[0]:
            c.wait_send()

        @pl.when(has_next)
        def _():
            for c in copies[1]:
                c.wait_send()

    to, at = iota((tokens, tokens), 0), iota((tokens, tokens), 1)
    swap[...] = (lax.rem(to, rows_i) * cols_j + lax.div(to, rows_i) == at).astype(jnp.bfloat16)
    cells = frames * height * columns
    group = frames // 2
    r_line, r_col = lax.div(iota((cells, 2 * lanes), 0), columns), lax.rem(
        iota((cells, 2 * lanes), 0), columns
    )
    r_slot = lax.div(lax.div(r_line, height), group) * 4 + lax.rem(r_line, 2) * 2 + lax.rem(r_col, 2)
    noise_mask[...] = (lax.div(iota((cells, 2 * lanes), 1), lat) == r_slot).astype(jnp.float32)
    packed = cells // 8
    r_at, r_to = iota((packed, cells), 1), iota((packed, cells), 0)
    r_line, r_col = lax.div(r_at, columns), lax.rem(r_at, columns)
    r_home = (
        lax.rem(lax.div(r_line, height), group) * (columns // 2) + lax.div(r_col, 2)
    ) * rows_i + lax.div(lax.rem(r_line, height), 2)
    noise_pick[...] = (r_to == r_home).astype(jnp.bfloat16)
    shape = (2 * lanes, 2 * line_size)
    src, dst = iota(shape, 0), iota(shape, 1)
    same = lax.div(src, lanes) == lax.div(dst, line_size)
    src, dst = lax.rem(src, lanes), lax.rem(dst, line_size)
    places[0] = (same & (src == dst + 2 * lat) & (dst < 2 * lat)).astype(jnp.bfloat16)
    places[1] = (same & (src + 2 * lat == dst)).astype(jnp.bfloat16)
    places[2] = (same & (src + 6 * lat == dst) & (dst >= 6 * lat)).astype(jnp.bfloat16)
    expanded[...] = jnp.zeros_like(expanded)
    taps_in[...] = jnp.zeros_like(taps_in)
    wide[0] = jnp.zeros_like(wide[0])
    wide[width + 1] = jnp.zeros_like(wide[0])
    is_end = (sec == 0) | (sec == sections - 1)

    @pl.when(is_end)
    def _():
        recv_buf[3] = jnp.zeros_like(recv_buf[3])

    @pl.when(jnp.logical_not(has_prev))
    def _():
        fields[1] = jnp.zeros_like(fields[1])
        noises[1] = jnp.zeros_like(noises[1])

    features = hidden.shape[1]
    for c in loads[:3]:
        c.wait()
    scale = 1.0 + (modulation[1:2, :] + time_embed[...])
    shift = modulation[0:1, :] + time_embed[...]
    row = iota((16, features), 0)
    lines = jnp.zeros((16, features), jnp.float32)
    for n, piece in enumerate(pieces(scale) + pieces(shift)):
        lines = jnp.where(row == n, piece, lines)
    loads[3].wait()
    values = hidden[...].astype(jnp.float32)
    own_sum = jnp.sum(values, axis=1, keepdims=True)
    own_square = jnp.sum(values * values, axis=1, keepdims=True)
    center = own_sum / features
    centred = ((values - center) * scale).astype(jnp.bfloat16)
    stack = jnp.concatenate([centred, lines.astype(jnp.bfloat16)], axis=0)
    made = dot_rows(stack, head_weight[...])
    part[:tokens, :lanes] = made[:tokens]
    stat_shape = (tokens, 128 - lanes)
    part[:tokens, lanes:] = jnp.where(
        iota(stat_shape, 1) < stat_shape[1] // 2, own_sum, own_square
    )
    made = made[tokens:]
    line = iota(made.shape, 0)
    own_scale = jnp.sum(jnp.where(line < 3, made, 0.0), axis=0, keepdims=True)
    own_shift = jnp.sum(jnp.where(line < 3, 0.0, made), axis=0, keepdims=True)
    part[tokens:, :lanes] = jnp.where(iota((8, lanes), 0) == 0, own_scale, own_shift)
    part[tokens:, lanes:] = jnp.zeros((8, 128 - lanes), jnp.float32)
    pair = pair_copy(0, part, peer_part)
    early = [pair_copy(1, in_weight, peer_weight), pair_copy(2, in_bias, peer_bias)]
    pl.semaphore_wait(barrier, sections + jnp.where(has_next, sections, 0))
    pair.start()

    for c in loads[4:12]:
        c.wait()
    src, dst = iota((lat, 2 * lanes), 0), iota((lat, 2 * lanes), 1)
    tiled = dot(noisy[...], (src == lax.rem(dst, lat)).astype(jnp.bfloat16))
    tiled = (tiled * noise_mask[...]).astype(jnp.bfloat16)
    noises[0, 0] = dot(noise_pick[...], tiled).astype(jnp.bfloat16)
    noise_copies = spread(noises, noise_send, noise_recv)
    spread_start(noise_copies)
    for c in early:
        c.start()
    std = jnp.concatenate([latent_std[...]] * 8, axis=1)
    mean_latent = jnp.concatenate([latent_mean[...]] * 8, axis=1)
    pair.wait()
    far_sum = peer_part[:tokens, lanes : lanes + 1]
    far_square = peer_part[:tokens, lanes + (128 - lanes) // 2 : lanes + (128 - lanes) // 2 + 1]
    average = (own_sum + far_sum) / D
    variance = (own_square + far_square) / D - average * average
    body = (
        part[:tokens, :lanes]
        + peer_part[:tokens, :lanes]
        - (average - center) * own_scale
        - (average - far_sum / features) * peer_part[tokens : tokens + 1, :lanes]
    )
    velocity = (
        lax.rsqrt(variance + 1e-06) * body
        + (own_shift + peer_part[tokens + 1 : tokens + 2, :lanes])
        + head_bias[...]
    ).astype(jnp.bfloat16)
    field = dot(swap[...], velocity)
    fields[0, 0] = jnp.concatenate([field[:folded], field[folded:]], axis=1).astype(jnp.bfloat16)
    field_copies = spread(fields, field_send, field_recv)
    spread_start(field_copies)

    for c in early:
        c.wait()
    for q in range(2):
        for e in range(3):
            col = q + e
            step_j, odd = (col + 1) // 2 - q, (col + 1) % 2
            for a in range(3):
                for b in range(3):
                    tap = 9 * a + 3 * b + e
                    for p in range(2):
                        first = step_j * 3 * line_size + a * line_size + (p + b) * 2 * lat + odd * lat
                        left = p * 2 * half
                        taps_in[q, first : first + lat, left : left + half] = in_weight[tap]
                        taps_in[q, first : first + lat, left + half : left + 2 * half] = peer_weight[tap]
    spread_wait(noise_copies)
    lane = iota((folded, 2 * lanes), 1)
    side = folded // 2
    for slot in (1, 0):
        got = [
            noises[slot, lax.rem(sec + sections - g, sections)].astype(jnp.float32)
            for g in range(sections)
        ]
        for f in range(frames):
            r = f % group
            low, high = (
                jnp.concatenate(
                    [got[g][r * side : (r + 1) * side] for g in (2 * t, 2 * t + 1)], axis=0
                )
                for t in range(2)
            )
            if f < group:
                high = pltpu.roll(high, lanes, 1)
            else:
                low = pltpu.roll(low, lanes, 1)
            at_f = ((1 - slot) * frames + f) * folded
            noise_lines[at_f : at_f + folded, :] = jnp.where(lane < lanes, low, high)
    spread_wait(field_copies)

    lines_f = jnp.concatenate(
        [
            fields[slot, lax.rem(sec + sections - f, sections)]
            for slot in (1, 0)
            for f in range(frames)
        ],
        axis=0,
    ).astype(jnp.float32)
    lines_f = ((noise_lines[...] - step_size[0] * lines_f) * std + mean_latent).astype(
        jnp.bfloat16
    ).astype(jnp.float32)
    count = 2 * frames * folded
    f_row = iota((count, 2 * lanes), 0)
    i_row = lax.rem(f_row, rows_i)
    lines_f = jnp.where((f_row >= frames * folded) | has_prev, lines_f, 0.0)
    before = jnp.where(i_row == 0, 0.0, pltpu.roll(lines_f, 1, 0))
    after = jnp.where(i_row == rows_i - 1, 0.0, pltpu.roll(lines_f, count - 1, 0))
    line_values = (
        dot(before.astype(jnp.bfloat16), places[0])
        + dot(lines_f.astype(jnp.bfloat16), places[1])
        + dot(after.astype(jnp.bfloat16), places[2])
    )
    half_j = cols_j // 2
    for f in range(2 * frames):
        for side in range(2):
            expanded[1 + side * half_j : 1 + (side + 1) * half_j, f] = line_values[
                f * folded : (f + 1) * folded, side * line_size : (side + 1) * line_size
            ].reshape(half_j, rows_i, line_size)
    block = near * rows_i
    for j in range(cols_j + 2):
        for a in range(3):
            stacked[j * block : (j + 1) * block, a * line_size : (a + 1) * line_size] = (
                expanded[j, a : a + near].reshape(block, line_size).astype(jnp.bfloat16)
            )
    parts = half // channels
    tall = near * height
    for q in range(2):
        lhs = jnp.concatenate(
            [
                stacked[q * block : (q + cols_j) * block, :],
                stacked[(q + 1) * block : (q + 1 + cols_j) * block, :],
            ],
            axis=1,
        )
        for p in range(2):
            total = jnp.zeros((cols_j * block, channels), jnp.float32)
            for h in range(2):
                left = (p * 2 + h) * half
                bias = in_bias[...] if h == 0 else peer_bias[...]
                up = dot(lhs, taps_in[q, :, left : left + half]) + bias
                up = up.astype(jnp.bfloat16).astype(jnp.float32)
                for n in range(parts):
                    chunk = up[:, n * channels : (n + 1) * channels]
                    total = total + chunk * chunk
                for j in range(cols_j):
                    for n in range(parts):
                        ups[
                            h * parts + n, pl.ds((2 * j + q) * tall + p, block, stride=2), :
                        ] = up[j * block : (j + 1) * block, n * channels : (n + 1) * channels]
            for j in range(cols_j):
                squares[pl.ds((2 * j + q) * tall + p, block, stride=2), :] = total[
                    j * block : (j + 1) * block
                ]

    mine = lax.rem(sec + parts * core, 2 * parts)
    gain = norm_gain[pl.ds(sec, 1), :]
    h_row = lax.rem(iota((tall, channels), 0), height)
    valid = has_prev | (iota((tall, channels), 0) >= 2 * height)

    def normalise(w):
        at_w = pl.ds(pl.multiple_of(w * tall, tall), tall)
        mean = jnp.sum(squares[at_w, :], axis=1, keepdims=True) / (2 * half)
        v = ups[mine, at_w, :] * lax.rsqrt(mean + 1e-06) * gain
        v = jnp.where(valid, v / (1.0 + jnp.exp(-v)), 0.0)
        above = jnp.where(h_row == 0, 0.0, pltpu.roll(v, 1, 0))
        below = jnp.where(h_row == height - 1, 0.0, pltpu.roll(v, tall - 1, 0))
        for b, line_v in enumerate((above, v, below)):
            wide[w + 1, :, b * channels : (b + 1) * channels] = line_v.astype(jnp.bfloat16)

    span = frames * height
    pair_columns = columns // 2
    rows = pair_columns * span

    def partial(d, m):
        windows, taps = [], []
        for a in range(3):
            for e in range(3):
                window = wide[
                    pl.ds(d * columns + e + m * pair_columns, pair_columns),
                    a * height : a * height + span,
                    :,
                ]
                windows.append(window.reshape(rows, 3 * channels))
                taps += [weight[9 * a + 3 * b + e] for b in range(3)]
        return dot(jnp.concatenate(windows, axis=1), jnp.concatenate(taps, axis=0))

    up_side = sec < sections // 2
    away = jnp.where(up_side, sec, sections - 1 - sec)

    def mirrored(value):
        return jnp.where(up_side, value, sections - 1 - value)

    inner = jnp.logical_not(is_end)
    dests = [
        mirrored(jnp.where(is_end, sections - 1, sections // 2)),
        mirrored(jnp.where(is_end, sections - 2, 0)),
        mirrored(jnp.where(is_end, 1, sections - 1)),
    ]
    hop = mirrored(jnp.where(is_end, 1, sections // 2))
    first_slot = jnp.where(is_end, 0, 3)

    def sum_copy(n, m):
        slot = first_slot if n == 0 else n
        return pltpu.make_async_remote_copy(
            send_buf.at[n, m], recv_buf.at[slot, m], sum_send.at[n, m], sum_recv.at[slot, m],
            device_id={"section": hop if n == 0 else dests[n]},
        )

    def arrival(slot, m):
        return pltpu.make_async_remote_copy(
            send_buf.at[0, m], recv_buf.at[slot, m], sum_send.at[0, m], sum_recv.at[slot, m],
            device_id={"section": hop},
        )

    for t in range(columns + 2):
        normalise(lax.rem(dests[0] * columns + width - 1 + t, width))
    loads[12].wait()
    for m in range(2):
        send_buf[0, m] = partial(dests[0], m).astype(jnp.bfloat16)
        sum_copy(0, m).start()
    for t in range(width - columns - 2):
        normalise(lax.rem(dests[0] * columns + columns + 1 + t, width))
    for m in range(2):
        send_buf[1, m] = partial(dests[1], m).astype(jnp.bfloat16)
        sum_copy(1, m).start()
    for m in range(2):
        value = partial(dests[2], m)

        @pl.when(is_end)
        def _():
            send_buf[2, m] = value.astype(jnp.bfloat16)
            sum_copy(2, m).start()

        @pl.when(inner)
        def _():
            held[m] = value

    for m in range(2):
        value = partial(sec, m) + conv_bias[...]
        residual = []
        for w in range(pair_columns):
            first = pl.multiple_of(
                (sec * columns + m * pair_columns + w) * tall + 2 * height, height
            )
            residual.append(
                jnp.concatenate([ups[n, pl.ds(first, span), :] for n in range(parts)], axis=1)
            )
        acc[m] = value + jnp.concatenate(residual, axis=0)

    @pl.when(inner)
    def _():
        for m in range(2):
            arrival(0, m).wait_recv()
            send_buf[2, m] = (held[m] + recv_buf[0, m].astype(jnp.float32)).astype(jnp.bfloat16)
            sum_copy(2, m).start()
        for m in range(2):
            arrival(3, m).wait_recv()

    for m in range(2):
        arrival(1, m).wait_recv()
        acc[m] = (
            acc[m] + recv_buf[1, m].astype(jnp.float32) + recv_buf[3, m].astype(jnp.float32)
        )
    for m in range(2):
        arrival(2, m).wait_recv()
        total = acc[m] + recv_buf[2, m].astype(jnp.float32)
        for w in range(pair_columns):
            for n in range(parts):
                final[n, pl.ds(m * pair_columns + w, span, stride=columns), :] = total[
                    w * span : (w + 1) * span, n * channels : (n + 1) * channels
                ]
    for n in range(parts):
        out[:, n * channels : (n + 1) * channels] = final[n].astype(out.dtype)
    for n in range(3):
        for m in range(2):
            sum_copy(n, m).wait_send()
    spread_drain(noise_copies)
    spread_drain(field_copies)


def fused_shards(sizes, *arrays):
    (
        hidden, modulation, time_embed, head_weight, head_bias, noisy, step_size, latent_mean,
        latent_std, in_weight, in_bias, norm_gain, conv_weight, conv_bias,
    ) = arrays
    sections, clips_sp, frames, height, columns, lat, channels = sizes
    rows_i, cols_j, half = height // 2, columns * sections // 2, in_weight.shape[2]
    width, near, tokens, lanes = columns * sections, frames + 2, hidden.shape[0], 4 * lat
    line_size = 8 * lat
    f32, bf16 = jnp.float32, jnp.bfloat16
    vmem, dma = pltpu.VMEM, pltpu.SemaphoreType.DMA
    rows = columns * frames * height
    operands = (
        modulation, time_embed[None], head_bias[None], noisy.reshape(-1, lat),
        latent_std[None], latent_mean[None], in_bias[None], norm_gain.reshape(-1, channels),
        conv_bias[None], hidden, head_weight.T, in_weight, conv_weight,
    )
    operands = [pltpu.with_memory_space_constraint(value, pltpu.HBM) for value in operands]
    far = pl.BlockSpec(memory_space=pltpu.HBM)
    out = pl.pallas_call(
        functools.partial(block_kernel, sizes),
        out_shape=pltpu.VMEM((rows, half), bf16),
        in_specs=[far] * 4
        + [pl.BlockSpec(memory_space=pltpu.SMEM)]
        + [far] * (len(operands) - 4),
        out_specs=pl.BlockSpec(memory_space=pltpu.VMEM),
        scratch_shapes=[vmem(value.shape, value.dtype) for value in operands]
        + [
            vmem((tokens, tokens), bf16),
            vmem((rows // 8, rows), bf16),
            vmem((rows, 2 * lanes), f32),
            vmem((3, 2 * lanes, 2 * line_size), bf16),
            vmem((tokens + 8, 128), f32),
            vmem((tokens + 8, 128), f32),
            vmem(in_weight.shape, bf16),
            vmem((1, half), f32),
            vmem((2, sections, tokens // 2, 2 * lanes), bf16),
            vmem((2, sections, rows // 8, 2 * lanes), bf16),
            vmem((2 * frames * tokens // 2, 2 * lanes), f32),
            vmem((cols_j + 2, 2 * frames, rows_i, line_size), f32),
            vmem(((cols_j + 2) * near * rows_i, 3 * line_size), bf16),
            vmem((2, 6 * line_size, 4 * half), bf16),
            vmem((2 * half // channels, width * near * height, channels), f32),
            vmem((width * near * height, channels), f32),
            vmem((width + 2, near * height, 3 * channels), bf16),
            vmem((3, 2, rows // 2, half), bf16),
            vmem((4, 2, rows // 2, half), bf16),
            vmem((2, rows // 2, half), f32),
            vmem((2, rows // 2, half), f32),
            vmem((half // channels, rows, channels), f32),
            dma((len(operands),)),
            dma((3,)),
            dma((3,)),
            dma((2, sections)),
            dma((2, sections)),
            dma((2, sections)),
            dma((2, sections)),
            dma((3, 2)),
            dma((4, 2)),
        ],
        compiler_params=pltpu.CompilerParams(
            collective_id=0, has_side_effects=True, vmem_limit_bytes=40 * 2**20
        ),
    )(*operands[:4], step_size, *operands[4:])
    return out.reshape(frames, height, columns, half)


def dispatch(*arrays):
    hidden, noisy, in_weight, conv_weight = arrays[0], arrays[5], arrays[9], arrays[12]
    frames, height, columns, lat = noisy.shape
    sections, cores, clips_sp = (lax.axis_size(axis) for axis in ("section", "tp", "sp"))
    channels, half = conv_weight.shape[1:]
    whole_frame = hidden.shape[0] == height // 2 * (columns * sections // 2)
    if (
        whole_frame
        and cores == 2
        and clips_sp > 1
        and frames == sections
        and sections == 4
        and columns % 2 == 0
        and channels % 128 == 0
        and half % channels == 0
        and lat == 16
        and height == 16
    ):
        sizes = (sections, clips_sp, frames, height, columns, lat, channels)
        return fused_shards(sizes, *arrays)
    return shards(*arrays)


def solution(mesh):
    placed = (
        P(("groups", "sp", "section"), "tp"),
        P(None, "tp"),
        P(("groups", "tp")),
        P("tp", None),
        P(),
        P(("groups", "sp"), None, "section", None),
        P("groups"),
        P(),
        P(),
        P(None, None, "tp"),
        P("tp"),
        P(),
        P(None, "section", "tp"),
        P("tp"),
    )
    return jax.shard_map(
        dispatch,
        mesh=mesh,
        in_specs=placed,
        out_specs=P(("groups", "sp"), None, "section", "tp"),
        check_vma=False,
    )
```

```python
import functools

import jax
import jax.numpy as jnp
from jax import lax
from jax.experimental import pallas as pl
from jax.experimental.pallas import tpu as pltpu
from jax.sharding import PartitionSpec as P

D = 6144


def padded_2(value, sides, width):
    for axis, dim in sides:
        count, length = (lax.axis_size(axis), value.shape[dim])
        up = [(i, (i + 1) % count) for i in range(count - 1)]
        down = [(j, i) for i, j in up]
        last = lax.slice_in_dim(value, length - width, length, axis=dim)
        leading = lax.slice_in_dim(value, 0, width, axis=dim)
        before = lax.ppermute(last, axis, up)
        after = lax.ppermute(leading, axis, down)
        value = jnp.concatenate([before, value, after], axis=dim)
    return value


def passed_along(value, axis, by):
    count = lax.axis_size(axis)
    pairs = [(i, i + by) for i in range(count) if 0 <= i + by < count]
    return lax.ppermute(value, axis, pairs)


def conv_taps(padded, weight, frames, height, columns):
    channels = padded.shape[3]
    result = jnp.zeros((frames * height * columns, weight.shape[2]), jnp.float32)
    for offset_time in range(3):
        for offset_row in range(3):
            slab = padded[offset_time : offset_time + frames, offset_row : offset_row + height]
            window = jnp.concatenate(
                [slab[:, :, 0:columns], slab[:, :, 1 : columns + 1], slab[:, :, 2 : columns + 2]],
                axis=3,
            )
            first = 9 * offset_time + 3 * offset_row
            taps = weight[first : first + 3].reshape(3 * channels, weight.shape[2])
            result = result + jnp.dot(
                window.reshape(-1, 3 * channels), taps, preferred_element_type=jnp.float32
            )
    return result


def activate(source, gain_vector):
    values = source.astype(jnp.float32)
    squares = jnp.mean(values * values, axis=-1, keepdims=True)
    return jax.nn.silu(values * lax.rsqrt(squares + 1e-06) * gain_vector).astype(jnp.bfloat16)


def pad_rows(source):
    return jnp.pad(source, ((0, 0), (1, 1), (0, 0), (0, 0)))


def shards(
    hidden,
    modulation,
    time_embed,
    head_weight,
    head_bias,
    noisy,
    step_size,
    latent_mean,
    latent_std,
    in_weight,
    in_bias,
    norm_gain,
    conv_weight,
    conv_bias,
):
    frames, height, columns, lat_channels = noisy.shape
    sections = lax.axis_size("section")
    half_channels = in_weight.shape[2]
    values = hidden.astype(jnp.float32)
    row_sums, square_sums = lax.psum(
        (jnp.sum(values, axis=1), jnp.sum(values * values, axis=1)), "tp"
    )
    average = row_sums / D
    variance = square_sums / D - average * average
    shift_term = modulation[0] + time_embed
    scale_term = modulation[1] + time_embed
    modulated = (
        (values - average[:, None]) * lax.rsqrt(variance[:, None] + 1e-06) * (1.0 + scale_term)
        + shift_term
    ).astype(jnp.bfloat16)
    partial_sum = jnp.dot(modulated, head_weight, preferred_element_type=jnp.float32)
    velocity = (lax.psum(partial_sum, "tp") + head_bias).astype(jnp.bfloat16)
    band_rows = velocity.shape[0] * 2 // (columns * sections)
    outgoing = velocity.reshape(band_rows, sections, -1)
    arrived = lax.all_to_all(outgoing, "section", split_axis=1, concat_axis=0, tiled=True)
    latent_field = arrived.reshape(frames, height // 2, columns // 2, 2, 2, lat_channels)
    latent_field = jnp.transpose(latent_field, (0, 1, 3, 2, 4, 5)).reshape(
        frames, height, columns, lat_channels
    )
    latent = (
        (noisy.astype(jnp.float32) - step_size[0] * latent_field.astype(jnp.float32)) * latent_std
        + latent_mean
    ).astype(jnp.bfloat16)
    latent_wide = padded_2(latent, (("section", 2),), 2)
    earlier = passed_along(latent_wide, "sp", 1)
    stacked = pad_rows(jnp.concatenate([earlier, latent_wide], axis=0))
    extended = (conv_taps(stacked, in_weight, frames + 2, height, columns + 2) + in_bias).astype(
        jnp.bfloat16
    )
    extended = extended.reshape(frames + 2, height, columns + 2, half_channels)
    upblock_half = extended[2:, :, 1 : columns + 1]
    extended_full = lax.all_gather(extended, "tp", axis=3, tiled=True)
    normed = activate(extended_full, norm_gain)
    frame_index = lax.axis_index("sp") * frames - 2 + jnp.arange(frames + 2, dtype=jnp.int32)
    column_index = (
        lax.axis_index("section") * columns - 1 + jnp.arange(columns + 2, dtype=jnp.int32)
    )
    inside_cols = (column_index >= 0) & (column_index < columns * sections)
    inside = (frame_index >= 0)[:, None, None, None] & inside_cols[None, None, :, None]
    conv_input = pad_rows(jnp.where(inside, normed, jnp.zeros_like(normed)))
    full_weight = lax.all_gather(conv_weight, "section", axis=1, tiled=True)
    mixed = conv_taps(conv_input, full_weight, frames, height, columns)
    decoded = (
        upblock_half.astype(jnp.float32).reshape(-1, half_channels) + mixed + conv_bias
    ).astype(jnp.bfloat16)
    return decoded.reshape(frames, height, columns, half_channels)


def iota(shape, dim):
    return lax.broadcasted_iota(jnp.int32, shape, dim)


def dot(left, right):
    return jnp.dot(left, right, preferred_element_type=jnp.float32)


def dot_rows(left, right):
    return lax.dot_general(
        left, right, (((1,), (1,)), ((), ())), preferred_element_type=jnp.float32
    )


def pieces(value):
    high = value.astype(jnp.bfloat16)
    rest = value - high.astype(jnp.float32)
    middle = rest.astype(jnp.bfloat16)
    low = (rest - middle.astype(jnp.float32)).astype(jnp.bfloat16)
    return high.astype(jnp.float32), middle.astype(jnp.float32), low.astype(jnp.float32)


def block_kernel(
    sizes,
    modulation_far,
    time_far,
    head_bias_far,
    noisy_far,
    step_size,
    std_far,
    mean_far,
    in_bias_far,
    gain_far,
    conv_bias_far,
    hidden_far,
    head_far,
    in_far,
    conv_far,
    out,
    modulation,
    time_embed,
    head_bias,
    noisy,
    latent_std,
    latent_mean,
    in_bias,
    norm_gain,
    conv_bias,
    hidden,
    head_weight,
    in_weight,
    weight,
    swap,
    noise_pick,
    noise_mask,
    places,
    part,
    peer_part,
    peer_weight,
    peer_bias,
    fields,
    noise_lines,
    expanded,
    stacked,
    taps_in,
    ups,
    squares,
    wide,
    send_buf,
    recv_buf,
    held,
    acc,
    final,
    load_sems,
    pair_send,
    pair_recv,
    field_send,
    field_recv,
    sum_send,
    sum_recv,
):
    sections, clips_sp, frames, height, columns, lat, channels = sizes
    rows_i, cols_j = height // 2, columns * sections // 2
    width = columns * sections
    tokens = rows_i * cols_j
    near = frames + 2
    half = in_weight.shape[2]
    lanes = 4 * lat
    folded = tokens // 2
    line_size = 4 * 2 * lat
    sec, core, spi = lax.axis_index("section"), lax.axis_index("tp"), lax.axis_index("sp")
    nxt = lax.rem(spi + 1, clips_sp)
    prv = lax.rem(spi + clips_sp - 1, clips_sp)
    has_next, has_prev = spi + 1 < clips_sp, spi > 0
    peer = {"tp": 1 - core}

    lead = core == 1
    barrier = pltpu.get_barrier_semaphore()
    pl.semaphore_signal(barrier, inc=1, device_id=peer)
    for k in range(1, sections):
        pl.semaphore_signal(
            barrier, inc=1, device_id={"section": lax.rem(sec + k, sections), "tp": 1}
        )

    @pl.when(has_prev)
    def _():
        for k in range(sections):
            pl.semaphore_signal(
                barrier,
                inc=1,
                device_id={"section": lax.rem(sec + k, sections), "sp": prv, "tp": 1},
            )


    def quarters(ref):
        size = ref.shape[0] // 4
        return [pl.ds(n * size, size) for n in range(4)]

    groups = (
        (
            *((head_far.at[part_of], head_weight.at[part_of]) for part_of in quarters(head_far)),
            (modulation_far, modulation),
            (time_far, time_embed),
            *((hidden_far.at[part_of], hidden.at[part_of]) for part_of in quarters(hidden_far)),
        ),
        (
            (noisy_far, noisy),
            (in_bias_far, in_bias),
            (head_bias_far, head_bias),
            (std_far, latent_std),
            (mean_far, latent_mean),
            (gain_far, norm_gain),
            (conv_bias_far, conv_bias),
            (in_far, in_weight),
        ),
        ((conv_far, weight),),
    )
    loads = [
        [pltpu.make_async_copy(source, target, load_sems.at[n]) for source, target in members]
        for n, members in enumerate(groups)
    ]
    for c in loads[0] + loads[1]:
        c.start()

    def pair_copy(n, source, target):
        return pltpu.make_async_remote_copy(
            source, target, pair_send.at[n], pair_recv.at[n], device_id=peer
        )

    def wait_rows(count, sem):
        view = ups.at[0, pl.ds(0, count), :]
        pltpu.make_async_copy(view, view, sem).wait()

    up_side = sec < sections // 2
    is_end = (sec == 0) | (sec == sections - 1)
    inner = jnp.logical_not(is_end)

    def mirrored(value):
        return jnp.where(up_side, value, sections - 1 - value)

    others = [mirrored(jnp.where(is_end, sections - 1 - n, (3, 2, 0)[n])) for n in range(3)]

    def spread_copy(z, ahead, c):
        slot = lax.rem(z - sec + sections, sections)
        return pltpu.make_async_remote_copy(
            fields.at[0, 0], fields.at[ahead, slot], field_send.at[0], field_recv.at[0],
            device_id={"section": z, "sp": nxt if ahead else spi, "tp": c},
        )

    def spread():
        for z in [*others, sec]:
            if z is not sec:
                for c in (1, 0):
                    spread_copy(z, 0, c).start()

            @pl.when(has_next)
            def _():
                for c in (1, 0):
                    spread_copy(z, 1, c).start()

        pltpu.make_async_remote_copy(
            fields.at[0, 0], fields.at[0, 0], field_send.at[0], field_recv.at[0], device_id=peer
        ).start()

    field_rows = 2 * folded * 2 * lanes * 2 // 512

    to, at = iota((tokens, tokens), 0), iota((tokens, tokens), 1)
    swap[...] = (lax.rem(to, rows_i) * cols_j + lax.div(to, rows_i) == at).astype(jnp.bfloat16)
    cells = frames * height * columns
    group = frames // 2
    r_line, r_col = lax.div(iota((cells, 2 * lanes), 0), columns), lax.rem(
        iota((cells, 2 * lanes), 0), columns
    )
    r_slot = lax.div(lax.div(r_line, height), group) * 4 + lax.rem(r_line, 2) * 2 + lax.rem(r_col, 2)
    noise_mask[...] = (lax.div(iota((cells, 2 * lanes), 1), lat) == r_slot).astype(jnp.float32)
    packed = cells // 8
    r_at, r_to = iota((packed, cells), 1), iota((packed, cells), 0)
    r_line, r_col = lax.div(r_at, columns), lax.rem(r_at, columns)
    r_home = (
        lax.rem(lax.div(r_line, height), group) * (columns // 2) + lax.div(r_col, 2)
    ) * rows_i + lax.div(lax.rem(r_line, height), 2)
    noise_pick[...] = (r_to == r_home).astype(jnp.bfloat16)
    shape = (2 * lanes, 2 * line_size)
    src, dst = iota(shape, 0), iota(shape, 1)
    same = lax.div(src, lanes) == lax.div(dst, line_size)
    src, dst = lax.rem(src, lanes), lax.rem(dst, line_size)
    places[0] = (same & (src == dst + 2 * lat) & (dst < 2 * lat)).astype(jnp.bfloat16)
    places[1] = (same & (src + 2 * lat == dst)).astype(jnp.bfloat16)
    places[2] = (same & (src + 6 * lat == dst) & (dst >= 6 * lat)).astype(jnp.bfloat16)
    expanded[...] = jnp.zeros_like(expanded)
    taps_in[...] = jnp.zeros_like(taps_in)
    wide[0] = jnp.zeros_like(wide[0])
    wide[width + 1] = jnp.zeros_like(wide[0])

    @pl.when(jnp.logical_not(has_prev))
    def _():
        fields[1] = jnp.zeros_like(fields[1])

    features = hidden.shape[1]
    for c in loads[0]:
        c.wait()
    loads[2][0].start()
    scale = 1.0 + (modulation[1:2, :] + time_embed[...])
    shift = modulation[0:1, :] + time_embed[...]
    row = iota((16, features), 0)
    lines = jnp.zeros((16, features), jnp.float32)
    for n, piece in enumerate(pieces(scale) + pieces(shift)):
        lines = jnp.where(row == n, piece, lines)
    values = hidden[...].astype(jnp.float32)
    own_sum = jnp.sum(values, axis=1, keepdims=True)
    own_square = jnp.sum(values * values, axis=1, keepdims=True)
    center = own_sum / features
    centred = ((values - center) * scale).astype(jnp.bfloat16)
    stack = jnp.concatenate([centred, lines.astype(jnp.bfloat16)], axis=0)
    made = dot_rows(stack, head_weight[...])
    part[:tokens, :lanes] = made[:tokens]
    stat_shape = (tokens, 128 - lanes)
    part[:tokens, lanes:] = jnp.where(
        iota(stat_shape, 1) < stat_shape[1] // 2, own_sum, own_square
    )
    made = made[tokens:]
    line = iota(made.shape, 0)
    own_scale = jnp.sum(jnp.where(line < 3, made, 0.0), axis=0, keepdims=True)
    own_shift = jnp.sum(jnp.where(line < 3, 0.0, made), axis=0, keepdims=True)
    part[tokens:, :lanes] = jnp.where(iota((8, lanes), 0) == 0, own_scale, own_shift)
    part[tokens:, lanes:] = jnp.zeros((8, 128 - lanes), jnp.float32)
    pair = pair_copy(0, part, peer_part)
    early = [pair_copy(1, in_weight, peer_weight), pair_copy(2, in_bias, peer_bias)]
    for c in loads[1]:
        c.wait()
    std = jnp.concatenate([latent_std[...]] * 8, axis=1)
    mean_latent = jnp.concatenate([latent_mean[...]] * 8, axis=1)

    @pl.when(core == 0)
    def _():
        pl.semaphore_wait(barrier, 1)
        pair.start()
        for c in early:
            c.start()

    @pl.when(lead)
    def _():
        src, dst = iota((lat, 2 * lanes), 0), iota((lat, 2 * lanes), 1)
        tiled = dot(noisy[...], (src == lax.rem(dst, lat)).astype(jnp.bfloat16))
        tiled = (tiled * noise_mask[...]).astype(jnp.bfloat16)
        fields[0, 0, 1] = dot(noise_pick[...], tiled).astype(jnp.bfloat16)
        pair.wait_recv()
        far_sum = peer_part[:tokens, lanes : lanes + 1]
        far_square = peer_part[
            :tokens, lanes + (128 - lanes) // 2 : lanes + (128 - lanes) // 2 + 1
        ]
        average = (own_sum + far_sum) / D
        variance = (own_square + far_square) / D - average * average
        body = (
            part[:tokens, :lanes]
            + peer_part[:tokens, :lanes]
            - (average - center) * own_scale
            - (average - far_sum / features) * peer_part[tokens : tokens + 1, :lanes]
        )
        velocity = (
            lax.rsqrt(variance + 1e-06) * body
            + (own_shift + peer_part[tokens + 1 : tokens + 2, :lanes])
            + head_bias[...]
        ).astype(jnp.bfloat16)
        field = dot(swap[...], velocity)
        fields[0, 0, 0] = jnp.concatenate([field[:folded], field[folded:]], axis=1).astype(
            jnp.bfloat16
        )
        pl.semaphore_wait(
            barrier, 2 * sections - 1 + jnp.where(has_next, 2 * sections, 0)
        )
        spread()
        for c in early:
            c.start()

    for c in early:
        c.wait_recv()
    for q in range(2):
        for e in range(3):
            col = q + e
            step_j, odd = (col + 1) // 2 - q, (col + 1) % 2
            for a in range(3):
                for b in range(3):
                    tap = 9 * a + 3 * b + e
                    for p in range(2):
                        first = step_j * 3 * line_size + a * line_size + (p + b) * 2 * lat + odd * lat
                        left = p * 2 * half
                        taps_in[q, first : first + lat, left : left + half] = in_weight[tap]
                        taps_in[q, first : first + lat, left + half : left + 2 * half] = peer_weight[tap]

    for on_lead in (True, False):
        for first in (True, False):

            @pl.when((lead == on_lead) & (has_prev != first))
            def _():
                count = sections - 1 + (0 if first else sections) + (0 if on_lead else 1)
                wait_rows(count * field_rows, field_recv.at[0])

    lane = iota((folded, 2 * lanes), 1)
    side = folded // 2
    for slot in (1, 0):
        got = [
            fields[slot, lax.rem(sec + sections - g, sections), 1].astype(jnp.float32)
            for g in range(sections)
        ]
        for f in range(frames):
            r = f % group
            low, high = (
                jnp.concatenate(
                    [got[g][r * side : (r + 1) * side] for g in (2 * t, 2 * t + 1)], axis=0
                )
                for t in range(2)
            )
            if f < group:
                high = pltpu.roll(high, lanes, 1)
            else:
                low = pltpu.roll(low, lanes, 1)
            at_f = ((1 - slot) * frames + f) * folded
            noise_lines[at_f : at_f + folded, :] = jnp.where(lane < lanes, low, high)

    lines_f = jnp.concatenate(
        [
            fields[slot, lax.rem(sec + sections - f, sections), 0]
            for slot in (1, 0)
            for f in range(frames)
        ],
        axis=0,
    ).astype(jnp.float32)
    lines_f = ((noise_lines[...] - step_size[0] * lines_f) * std + mean_latent).astype(
        jnp.bfloat16
    ).astype(jnp.float32)
    count = 2 * frames * folded
    f_row = iota((count, 2 * lanes), 0)
    i_row = lax.rem(f_row, rows_i)
    lines_f = jnp.where((f_row >= frames * folded) | has_prev, lines_f, 0.0)
    before = jnp.where(i_row == 0, 0.0, pltpu.roll(lines_f, 1, 0))
    after = jnp.where(i_row == rows_i - 1, 0.0, pltpu.roll(lines_f, count - 1, 0))
    line_values = (
        dot(before.astype(jnp.bfloat16), places[0])
        + dot(lines_f.astype(jnp.bfloat16), places[1])
        + dot(after.astype(jnp.bfloat16), places[2])
    )
    half_j = cols_j // 2
    for f in range(2 * frames):
        for side in range(2):
            expanded[1 + side * half_j : 1 + (side + 1) * half_j, f] = line_values[
                f * folded : (f + 1) * folded, side * line_size : (side + 1) * line_size
            ].reshape(half_j, rows_i, line_size)
    block = near * rows_i
    for j in range(cols_j + 2):
        for a in range(3):
            stacked[j * block : (j + 1) * block, a * line_size : (a + 1) * line_size] = (
                expanded[j, a : a + near].reshape(block, line_size).astype(jnp.bfloat16)
            )
    dests = [
        jnp.where(is_end, mirrored(sections - 1), 0),
        mirrored(sections - 2),
        jnp.where(is_end, mirrored(1), sections - 1),
    ]
    parts = half // channels
    tall = near * height

    def upblock(homes):
        for q in range(2):
            lhs = jnp.concatenate(
                [
                    jnp.concatenate(
                        [
                            stacked[pl.ds(pl.multiple_of((j + q + n) * block, block), block), :]
                            for n in range(2)
                        ],
                        axis=1,
                    )
                    for j in homes
                ],
                axis=0,
            )
            for p in range(2):
                total = jnp.zeros((len(homes) * block, channels), jnp.float32)
                for h in range(2):
                    left = (p * 2 + h) * half
                    bias = in_bias[...] if h == 0 else peer_bias[...]
                    up = dot(lhs, taps_in[q, :, left : left + half]) + bias
                    up = up.astype(jnp.bfloat16).astype(jnp.float32)
                    for n in range(parts):
                        chunk = up[:, n * channels : (n + 1) * channels]
                        total = total + chunk * chunk
                    for m, j in enumerate(homes):
                        at_j = pl.ds(pl.multiple_of(2 * j * tall, tall) + q * tall + p, block, stride=2)
                        for n in range(parts):
                            ups[h * parts + n, at_j, :] = up[
                                m * block : (m + 1) * block, n * channels : (n + 1) * channels
                            ]
                for m, j in enumerate(homes):
                    at_j = pl.ds(pl.multiple_of(2 * j * tall, tall) + q * tall + p, block, stride=2)
                    squares[at_j, :] = total[m * block : (m + 1) * block]

    def homes_from(first):
        return [
            lax.rem(dests[0] * columns // 2 + cols_j + first + n, cols_j)
            for n in range(cols_j // 2)
        ]

    upblock(homes_from(-1))

    mine = lax.rem(sec + parts * core, 2 * parts)
    gain = norm_gain[pl.ds(sec, 1), :]
    h_row = lax.rem(iota((tall, channels), 0), height)
    valid = has_prev | (iota((tall, channels), 0) >= 2 * height)

    def normalise(w):
        at_w = pl.ds(pl.multiple_of(w * tall, tall), tall)
        mean = jnp.sum(squares[at_w, :], axis=1, keepdims=True) / (2 * half)
        v = ups[mine, at_w, :] * lax.rsqrt(mean + 1e-06) * gain
        v = jnp.where(valid, v / (1.0 + jnp.exp(-v)), 0.0)
        above = jnp.where(h_row == 0, 0.0, pltpu.roll(v, 1, 0))
        below = jnp.where(h_row == height - 1, 0.0, pltpu.roll(v, tall - 1, 0))
        for b, line_v in enumerate((above, v, below)):
            wide[w + 1, :, b * channels : (b + 1) * channels] = line_v.astype(jnp.bfloat16)

    span = frames * height
    pair_columns = columns // 2
    rows = pair_columns * span

    unit = jnp.where(core >= 0, 1.0, 0.0)

    def partial(d, m):
        windows, taps = [], []
        for a in range(3):
            for e in range(3):
                window = wide[
                    pl.ds(d * columns + e + m * pair_columns, pair_columns),
                    a * height : a * height + span,
                    :,
                ]
                windows.append(window.reshape(rows, 3 * channels))
                taps += [weight[9 * a + 3 * b + e] for b in range(3)]
        low, high = (
            dot(
                jnp.concatenate(windows[first:last], axis=1),
                jnp.concatenate(taps[3 * first : 3 * last], axis=0),
            )
            for first, last in ((0, 5), (5, 9))
        )
        return low + high * unit

    neighbour = mirrored(1)
    far_slot = jnp.where(up_side, 2, 0)
    targets = [dests[0], jnp.where(is_end, neighbour, dests[1]), dests[2]]
    slots = [jnp.where(is_end, 1, far_slot), jnp.where(is_end, 3, 1), jnp.where(is_end, 2, 2 - far_slot)]

    def sum_copy(n, w):
        return pltpu.make_async_remote_copy(
            send_buf.at[n, w], recv_buf.at[slots[n], w], sum_send.at[0],
            sum_recv.at[slots[n], w], device_id={"section": targets[n]},
        )

    def arrived(slot, w):
        pltpu.make_async_copy(
            recv_buf.at[slot, w], recv_buf.at[slot, w], sum_recv.at[slot, w]
        ).wait()
        return recv_buf[slot, w].astype(jnp.float32)

    def by_column(value):
        return [value[w * span : (w + 1) * span] for w in range(pair_columns)]

    for t in range(columns + 2):
        normalise(lax.rem(dests[0] * columns + width - 1 + t, width))
    loads[2][0].wait()
    for m in range(2):
        for w, value in enumerate(by_column(partial(dests[0], m))):
            send_buf[0, m * pair_columns + w] = value.astype(jnp.bfloat16)
        for w in range(pair_columns):
            sum_copy(0, m * pair_columns + w).start()
    upblock(homes_from(cols_j // 2 - 1))
    for t in range(width - columns - 2):
        normalise(lax.rem(dests[0] * columns + columns + 1 + t, width))
    for m in range(2):
        for w, value in enumerate(by_column(partial(dests[1], m))):
            held[m * pair_columns + w] = value

    @pl.when(is_end)
    def _():
        send_buf[1] = held[...].astype(jnp.bfloat16)
        for w in range(columns):
            sum_copy(1, w).start()

    for m in range(2):
        for w, value in enumerate(by_column(partial(dests[2], m))):
            send_buf[2, m * pair_columns + w] = value.astype(jnp.bfloat16)
    for w in range(columns):
        sum_copy(2, w).start()

    for m in range(2):
        value = partial(sec, m) + conv_bias[...]
        residual = []
        for w in range(pair_columns):
            first = pl.multiple_of(
                (sec * columns + m * pair_columns + w) * tall + 2 * height, height
            )
            residual.append(
                jnp.concatenate([ups[n, pl.ds(first, span), :] for n in range(parts)], axis=1)
            )
        for w, own in enumerate(by_column(value)):
            acc[m * pair_columns + w] = own + residual[w]

    @pl.when(inner)
    def _():
        for w in range(columns):
            send_buf[1, w] = (held[w] + arrived(3, w)).astype(jnp.bfloat16)
            sum_copy(1, w).start()


    def finish(order):
        for n in order[:-1]:
            for w in range(columns):
                acc[w] = acc[w] + arrived(n, w)
        for w in range(columns):
            total = acc[w] + arrived(order[-1], w)
            for c in range(parts):
                final[c, pl.ds(w, span, stride=columns), :] = total[
                    :, c * channels : (c + 1) * channels
                ]

    @pl.when(is_end)
    def _():
        finish((2, 0, 1))

    @pl.when(inner)
    def _():
        finish((2, 1))

    for n in range(parts):
        out[:, n * channels : (n + 1) * channels] = final[n].astype(out.dtype)
    wait_rows(3 * columns * span * half * 2 // 512, sum_send.at[0])
    for c in early:
        c.wait_send()

    @pl.when(core == 0)
    def _():
        pair.wait_send()

    for first in (True, False):

        @pl.when(lead & (has_next != first))
        def _():
            count = 2 * (sections - 1) + (0 if first else 2 * sections) + 1
            wait_rows(count * field_rows, field_send.at[0])


def fused_shards(sizes, *arrays):
    (
        hidden, modulation, time_embed, head_weight, head_bias, noisy, step_size, latent_mean,
        latent_std, in_weight, in_bias, norm_gain, conv_weight, conv_bias,
    ) = arrays
    sections, clips_sp, frames, height, columns, lat, channels = sizes
    rows_i, cols_j, half = height // 2, columns * sections // 2, in_weight.shape[2]
    width, near, tokens, lanes = columns * sections, frames + 2, hidden.shape[0], 4 * lat
    line_size = 8 * lat
    f32, bf16 = jnp.float32, jnp.bfloat16
    vmem, dma = pltpu.VMEM, pltpu.SemaphoreType.DMA
    rows = columns * frames * height
    operands = (
        modulation, time_embed[None], head_bias[None], noisy.reshape(-1, lat),
        latent_std[None], latent_mean[None], in_bias[None], norm_gain.reshape(-1, channels),
        conv_bias[None], hidden, head_weight.T, in_weight, conv_weight,
    )
    operands = [pltpu.with_memory_space_constraint(value, pltpu.HBM) for value in operands]
    far = pl.BlockSpec(memory_space=pltpu.HBM)
    out = pl.pallas_call(
        functools.partial(block_kernel, sizes),
        out_shape=pltpu.VMEM((rows, half), bf16),
        in_specs=[far] * 4
        + [pl.BlockSpec(memory_space=pltpu.SMEM)]
        + [far] * (len(operands) - 4),
        out_specs=pl.BlockSpec(memory_space=pltpu.VMEM),
        scratch_shapes=[vmem(value.shape, value.dtype) for value in operands]
        + [
            vmem((tokens, tokens), bf16),
            vmem((rows // 8, rows), bf16),
            vmem((rows, 2 * lanes), f32),
            vmem((3, 2 * lanes, 2 * line_size), bf16),
            vmem((tokens + 8, 128), f32),
            vmem((tokens + 8, 128), f32),
            vmem(in_weight.shape, bf16),
            vmem((1, half), f32),
            vmem((2, sections, 2, tokens // 2, 2 * lanes), bf16),
            vmem((2 * frames * tokens // 2, 2 * lanes), f32),
            vmem((cols_j + 2, 2 * frames, rows_i, line_size), f32),
            vmem(((cols_j + 2) * near * rows_i, 3 * line_size), bf16),
            vmem((2, 6 * line_size, 4 * half), bf16),
            vmem((2 * half // channels, width * near * height, channels), f32),
            vmem((width * near * height, channels), f32),
            vmem((width + 2, near * height, 3 * channels), bf16),
            vmem((3, columns, rows // columns, half), bf16),
            vmem((4, columns, rows // columns, half), bf16),
            vmem((columns, rows // columns, half), f32),
            vmem((columns, rows // columns, half), f32),
            vmem((half // channels, rows, channels), f32),
            dma((3,)),
            dma((3,)),
            dma((3,)),
            dma((1,)),
            dma((1,)),
            dma((1,)),
            dma((4, columns)),
        ],
        compiler_params=pltpu.CompilerParams(
            collective_id=0, has_side_effects=True, vmem_limit_bytes=40 * 2**20
        ),
    )(*operands[:4], step_size, *operands[4:])
    return out.reshape(frames, height, columns, half)


def dispatch(*arrays):
    hidden, noisy, in_weight, conv_weight = arrays[0], arrays[5], arrays[9], arrays[12]
    frames, height, columns, lat = noisy.shape
    sections, cores, clips_sp = (lax.axis_size(axis) for axis in ("section", "tp", "sp"))
    channels, half = conv_weight.shape[1:]
    whole_frame = hidden.shape[0] == height // 2 * (columns * sections // 2)
    if (
        whole_frame
        and cores == 2
        and clips_sp > 1
        and frames == sections
        and sections == 4
        and columns % 2 == 0
        and channels % 128 == 0
        and half % channels == 0
        and lat == 16
        and height == 16
    ):
        sizes = (sections, clips_sp, frames, height, columns, lat, channels)
        return fused_shards(sizes, *arrays)
    return shards(*arrays)


def solution(mesh):
    placed = (
        P(("groups", "sp", "section"), "tp"),
        P(None, "tp"),
        P(("groups", "tp")),
        P("tp", None),
        P(),
        P(("groups", "sp"), None, "section", None),
        P("groups"),
        P(),
        P(),
        P(None, None, "tp"),
        P("tp"),
        P(),
        P(None, "section", "tp"),
        P("tp"),
    )
    return jax.shard_map(
        dispatch,
        mesh=mesh,
        in_specs=placed,
        out_specs=P(("groups", "sp"), None, "section", "tp"),
        check_vma=False,
    )
```

```python
import functools

import jax
import jax.numpy as jnp
from jax import lax
from jax.experimental import pallas as pl
from jax.experimental.pallas import tpu as pltpu
from jax.sharding import PartitionSpec as P

D = 6144


def padded_2(value, sides, width):
    for axis, dim in sides:
        count, length = (lax.axis_size(axis), value.shape[dim])
        up = [(i, (i + 1) % count) for i in range(count - 1)]
        down = [(j, i) for i, j in up]
        last = lax.slice_in_dim(value, length - width, length, axis=dim)
        leading = lax.slice_in_dim(value, 0, width, axis=dim)
        before = lax.ppermute(last, axis, up)
        after = lax.ppermute(leading, axis, down)
        value = jnp.concatenate([before, value, after], axis=dim)
    return value


def passed_along(value, axis, by):
    count = lax.axis_size(axis)
    pairs = [(i, i + by) for i in range(count) if 0 <= i + by < count]
    return lax.ppermute(value, axis, pairs)


def conv_taps(padded, weight, frames, height, columns):
    channels = padded.shape[3]
    result = jnp.zeros((frames * height * columns, weight.shape[2]), jnp.float32)
    for offset_time in range(3):
        for offset_row in range(3):
            slab = padded[offset_time : offset_time + frames, offset_row : offset_row + height]
            window = jnp.concatenate(
                [slab[:, :, 0:columns], slab[:, :, 1 : columns + 1], slab[:, :, 2 : columns + 2]],
                axis=3,
            )
            first = 9 * offset_time + 3 * offset_row
            taps = weight[first : first + 3].reshape(3 * channels, weight.shape[2])
            result = result + jnp.dot(
                window.reshape(-1, 3 * channels), taps, preferred_element_type=jnp.float32
            )
    return result


def activate(source, gain_vector):
    values = source.astype(jnp.float32)
    squares = jnp.mean(values * values, axis=-1, keepdims=True)
    return jax.nn.silu(values * lax.rsqrt(squares + 1e-06) * gain_vector).astype(jnp.bfloat16)


def pad_rows(source):
    return jnp.pad(source, ((0, 0), (1, 1), (0, 0), (0, 0)))


def shards(
    hidden,
    modulation,
    time_embed,
    head_weight,
    head_bias,
    noisy,
    step_size,
    latent_mean,
    latent_std,
    in_weight,
    in_bias,
    norm_gain,
    conv_weight,
    conv_bias,
):
    frames, height, columns, lat_channels = noisy.shape
    sections = lax.axis_size("section")
    half_channels = in_weight.shape[2]
    values = hidden.astype(jnp.float32)
    row_sums, square_sums = lax.psum(
        (jnp.sum(values, axis=1), jnp.sum(values * values, axis=1)), "tp"
    )
    average = row_sums / D
    variance = square_sums / D - average * average
    shift_term = modulation[0] + time_embed
    scale_term = modulation[1] + time_embed
    modulated = (
        (values - average[:, None]) * lax.rsqrt(variance[:, None] + 1e-06) * (1.0 + scale_term)
        + shift_term
    ).astype(jnp.bfloat16)
    partial_sum = jnp.dot(modulated, head_weight, preferred_element_type=jnp.float32)
    velocity = (lax.psum(partial_sum, "tp") + head_bias).astype(jnp.bfloat16)
    band_rows = velocity.shape[0] * 2 // (columns * sections)
    outgoing = velocity.reshape(band_rows, sections, -1)
    arrived = lax.all_to_all(outgoing, "section", split_axis=1, concat_axis=0, tiled=True)
    latent_field = arrived.reshape(frames, height // 2, columns // 2, 2, 2, lat_channels)
    latent_field = jnp.transpose(latent_field, (0, 1, 3, 2, 4, 5)).reshape(
        frames, height, columns, lat_channels
    )
    latent = (
        (noisy.astype(jnp.float32) - step_size[0] * latent_field.astype(jnp.float32)) * latent_std
        + latent_mean
    ).astype(jnp.bfloat16)
    latent_wide = padded_2(latent, (("section", 2),), 2)
    earlier = passed_along(latent_wide, "sp", 1)
    stacked = pad_rows(jnp.concatenate([earlier, latent_wide], axis=0))
    extended = (conv_taps(stacked, in_weight, frames + 2, height, columns + 2) + in_bias).astype(
        jnp.bfloat16
    )
    extended = extended.reshape(frames + 2, height, columns + 2, half_channels)
    upblock_half = extended[2:, :, 1 : columns + 1]
    extended_full = lax.all_gather(extended, "tp", axis=3, tiled=True)
    normed = activate(extended_full, norm_gain)
    frame_index = lax.axis_index("sp") * frames - 2 + jnp.arange(frames + 2, dtype=jnp.int32)
    column_index = (
        lax.axis_index("section") * columns - 1 + jnp.arange(columns + 2, dtype=jnp.int32)
    )
    inside_cols = (column_index >= 0) & (column_index < columns * sections)
    inside = (frame_index >= 0)[:, None, None, None] & inside_cols[None, None, :, None]
    conv_input = pad_rows(jnp.where(inside, normed, jnp.zeros_like(normed)))
    full_weight = lax.all_gather(conv_weight, "section", axis=1, tiled=True)
    mixed = conv_taps(conv_input, full_weight, frames, height, columns)
    decoded = (
        upblock_half.astype(jnp.float32).reshape(-1, half_channels) + mixed + conv_bias
    ).astype(jnp.bfloat16)
    return decoded.reshape(frames, height, columns, half_channels)


def iota(shape, dim):
    return lax.broadcasted_iota(jnp.int32, shape, dim)


def dot(left, right):
    return jnp.dot(left, right, preferred_element_type=jnp.float32)


def dot_rows(left, right):
    return lax.dot_general(
        left, right, (((1,), (1,)), ((), ())), preferred_element_type=jnp.float32
    )


def pieces(value):
    high = value.astype(jnp.bfloat16)
    rest = value - high.astype(jnp.float32)
    middle = rest.astype(jnp.bfloat16)
    low = (rest - middle.astype(jnp.float32)).astype(jnp.bfloat16)
    return high.astype(jnp.float32), middle.astype(jnp.float32), low.astype(jnp.float32)


def block_kernel(
    sizes,
    modulation_far,
    time_far,
    head_bias_far,
    noisy_far,
    step_size,
    std_far,
    mean_far,
    in_bias_far,
    gain_far,
    conv_bias_far,
    hidden_far,
    head_far,
    in_far,
    conv_far,
    out,
    modulation,
    time_embed,
    head_bias,
    noisy,
    latent_std,
    latent_mean,
    in_bias,
    norm_gain,
    conv_bias,
    hidden,
    head_weight,
    in_weight,
    weight,
    swap,
    noise_pick,
    noise_mask,
    places,
    part,
    peer_part,
    peer_weight,
    peer_bias,
    fields,
    noise_lines,
    expanded,
    stacked,
    taps_in,
    ups,
    squares,
    wide,
    send_buf,
    recv_buf,
    held,
    acc,
    final,
    load_sems,
    pair_send,
    pair_recv,
    field_send,
    field_recv,
    sum_send,
    sum_recv,
):
    sections, clips_sp, frames, height, columns, lat, channels = sizes
    rows_i, cols_j = height // 2, columns * sections // 2
    width = columns * sections
    tokens = rows_i * cols_j
    near = frames + 2
    half = in_weight.shape[2]
    lanes = 4 * lat
    folded = tokens // 2
    line_size = 4 * 2 * lat
    sec, core, spi = lax.axis_index("section"), lax.axis_index("tp"), lax.axis_index("sp")
    nxt = lax.rem(spi + 1, clips_sp)
    prv = lax.rem(spi + clips_sp - 1, clips_sp)
    has_next, has_prev = spi + 1 < clips_sp, spi > 0
    peer = {"tp": 1 - core}

    lead = core == 1
    barrier = pltpu.get_barrier_semaphore()
    pl.semaphore_signal(barrier, inc=1, device_id=peer)
    for k in range(1, sections):
        pl.semaphore_signal(
            barrier, inc=1, device_id={"section": lax.rem(sec + k, sections), "tp": 1}
        )

    @pl.when(has_prev)
    def _():
        for k in range(sections):
            pl.semaphore_signal(
                barrier,
                inc=1,
                device_id={"section": lax.rem(sec + k, sections), "sp": prv, "tp": 1},
            )


    groups = (
        ((hidden_far, hidden),),
        ((modulation_far, modulation), (time_far, time_embed), (head_far, head_weight)),
        (
            (noisy_far, noisy),
            (in_bias_far, in_bias),
            (head_bias_far, head_bias),
            (std_far, latent_std),
            (mean_far, latent_mean),
            (gain_far, norm_gain),
            (conv_bias_far, conv_bias),
            (in_far, in_weight),
        ),
        ((conv_far, weight),),
    )
    loads = [
        [pltpu.make_async_copy(source, target, load_sems.at[n]) for source, target in members]
        for n, members in enumerate(groups)
    ]
    for c in loads[1] + loads[0] + loads[2]:
        c.start()

    def pair_copy(n, source, target):
        return pltpu.make_async_remote_copy(
            source, target, pair_send.at[n], pair_recv.at[n], device_id=peer
        )

    def wait_rows(count, sem):
        view = ups.at[0, pl.ds(0, count), :]
        pltpu.make_async_copy(view, view, sem).wait()

    up_side = sec < sections // 2
    is_end = (sec == 0) | (sec == sections - 1)
    inner = jnp.logical_not(is_end)

    def mirrored(value):
        return jnp.where(up_side, value, sections - 1 - value)

    others = [mirrored(jnp.where(is_end, sections - 1 - n, (3, 2, 0)[n])) for n in range(3)]

    def spread_copy(z, ahead, c):
        slot = lax.rem(z - sec + sections, sections)
        return pltpu.make_async_remote_copy(
            fields.at[0, 0], fields.at[ahead, slot], field_send.at[0], field_recv.at[0],
            device_id={"section": z, "sp": nxt if ahead else spi, "tp": c},
        )

    def spread():
        for z in [*others, sec]:
            if z is not sec:
                for c in (1, 0):
                    spread_copy(z, 0, c).start()

            @pl.when(has_next)
            def _():
                for c in (1, 0):
                    spread_copy(z, 1, c).start()

        pltpu.make_async_remote_copy(
            fields.at[0, 0], fields.at[0, 0], field_send.at[0], field_recv.at[0], device_id=peer
        ).start()

    field_rows = 2 * folded * 2 * lanes * 2 // 512

    to, at = iota((tokens, tokens), 0), iota((tokens, tokens), 1)
    swap[...] = (lax.rem(to, rows_i) * cols_j + lax.div(to, rows_i) == at).astype(jnp.bfloat16)
    cells = frames * height * columns
    group = frames // 2
    r_line, r_col = lax.div(iota((cells, 2 * lanes), 0), columns), lax.rem(
        iota((cells, 2 * lanes), 0), columns
    )
    r_slot = lax.div(lax.div(r_line, height), group) * 4 + lax.rem(r_line, 2) * 2 + lax.rem(r_col, 2)
    noise_mask[...] = (lax.div(iota((cells, 2 * lanes), 1), lat) == r_slot).astype(jnp.float32)
    packed = cells // 8
    r_at, r_to = iota((packed, cells), 1), iota((packed, cells), 0)
    r_line, r_col = lax.div(r_at, columns), lax.rem(r_at, columns)
    r_home = (
        lax.rem(lax.div(r_line, height), group) * (columns // 2) + lax.div(r_col, 2)
    ) * rows_i + lax.div(lax.rem(r_line, height), 2)
    noise_pick[...] = (r_to == r_home).astype(jnp.bfloat16)
    shape = (2 * lanes, 2 * line_size)
    src, dst = iota(shape, 0), iota(shape, 1)
    same = lax.div(src, lanes) == lax.div(dst, line_size)
    src, dst = lax.rem(src, lanes), lax.rem(dst, line_size)
    places[0] = (same & (src == dst + 2 * lat) & (dst < 2 * lat)).astype(jnp.bfloat16)
    places[1] = (same & (src + 2 * lat == dst)).astype(jnp.bfloat16)
    places[2] = (same & (src + 6 * lat == dst) & (dst >= 6 * lat)).astype(jnp.bfloat16)
    expanded[...] = jnp.zeros_like(expanded)
    taps_in[...] = jnp.zeros_like(taps_in)
    wide[0] = jnp.zeros_like(wide[0])
    wide[width + 1] = jnp.zeros_like(wide[0])

    @pl.when(jnp.logical_not(has_prev))
    def _():
        fields[1] = jnp.zeros_like(fields[1])

    features = hidden.shape[1]
    for c in loads[1]:
        c.wait()
    scale = 1.0 + (modulation[1:2, :] + time_embed[...])
    shift = modulation[0:1, :] + time_embed[...]
    row = iota((8, features), 0)
    lines = jnp.zeros((8, features), jnp.float32)
    for n, piece in enumerate(pieces(scale) + pieces(shift)):
        lines = jnp.where(row == n, piece, lines)
    lines = jnp.concatenate([lines, jnp.zeros_like(lines)], axis=0).astype(jnp.bfloat16)
    loads[0][0].wait()
    loads[3][0].start()
    values = hidden[...].astype(jnp.float32)
    own_sum = jnp.sum(values, axis=1, keepdims=True)
    own_square = jnp.sum(values * values, axis=1, keepdims=True)
    center = own_sum / features
    centred = ((values - center) * scale).astype(jnp.bfloat16)
    stack = jnp.concatenate([centred, lines], axis=0)
    made = dot_rows(stack, head_weight[...])
    part[:tokens, :lanes] = made[:tokens]
    stat_shape = (tokens, 128 - lanes)
    part[:tokens, lanes:] = jnp.where(
        iota(stat_shape, 1) < stat_shape[1] // 2, own_sum, own_square
    )
    made = made[tokens:]
    line = iota(made.shape, 0)
    own_scale = jnp.sum(jnp.where(line < 3, made, 0.0), axis=0, keepdims=True)
    own_shift = jnp.sum(jnp.where(line < 3, 0.0, made), axis=0, keepdims=True)
    part[tokens:, :lanes] = jnp.where(iota((8, lanes), 0) == 0, own_scale, own_shift)
    part[tokens:, lanes:] = jnp.zeros((8, 128 - lanes), jnp.float32)
    pair = pair_copy(0, part, peer_part)
    early = [pair_copy(1, in_weight, peer_weight), pair_copy(2, in_bias, peer_bias)]
    for c in loads[2]:
        c.wait()
    std = jnp.concatenate([latent_std[...]] * 8, axis=1)
    mean_latent = jnp.concatenate([latent_mean[...]] * 8, axis=1)

    @pl.when(core == 0)
    def _():
        pl.semaphore_wait(barrier, 1)
        pair.start()
        for c in early:
            c.start()

    @pl.when(lead)
    def _():
        src, dst = iota((lat, 2 * lanes), 0), iota((lat, 2 * lanes), 1)
        tiled = dot(noisy[...], (src == lax.rem(dst, lat)).astype(jnp.bfloat16))
        tiled = (tiled * noise_mask[...]).astype(jnp.bfloat16)
        fields[0, 0, 1] = dot(noise_pick[...], tiled).astype(jnp.bfloat16)
        pair.wait_recv()
        far_sum = peer_part[:tokens, lanes : lanes + 1]
        far_square = peer_part[
            :tokens, lanes + (128 - lanes) // 2 : lanes + (128 - lanes) // 2 + 1
        ]
        average = (own_sum + far_sum) / D
        variance = (own_square + far_square) / D - average * average
        body = (
            part[:tokens, :lanes]
            + peer_part[:tokens, :lanes]
            - (average - center) * own_scale
            - (average - far_sum / features) * peer_part[tokens : tokens + 1, :lanes]
        )
        velocity = (
            lax.rsqrt(variance + 1e-06) * body
            + (own_shift + peer_part[tokens + 1 : tokens + 2, :lanes])
            + head_bias[...]
        ).astype(jnp.bfloat16)
        field = dot(swap[...], velocity)
        fields[0, 0, 0] = jnp.concatenate([field[:folded], field[folded:]], axis=1).astype(
            jnp.bfloat16
        )
        pl.semaphore_wait(
            barrier, 2 * sections - 1 + jnp.where(has_next, 2 * sections, 0)
        )
        spread()
        for c in early:
            c.start()

    for c in early:
        c.wait_recv()
    for q in range(2):
        for e in range(3):
            col = q + e
            step_j, odd = (col + 1) // 2 - q, (col + 1) % 2
            for a in range(3):
                for b in range(3):
                    tap = 9 * a + 3 * b + e
                    for p in range(2):
                        first = step_j * 3 * line_size + a * line_size + (p + b) * 2 * lat + odd * lat
                        left = p * 2 * half
                        taps_in[q, first : first + lat, left : left + half] = in_weight[tap]
                        taps_in[q, first : first + lat, left + half : left + 2 * half] = peer_weight[tap]

    for on_lead in (True, False):
        for first in (True, False):

            @pl.when((lead == on_lead) & (has_prev != first))
            def _():
                count = sections - 1 + (0 if first else sections) + (0 if on_lead else 1)
                wait_rows(count * field_rows, field_recv.at[0])

    lane = iota((folded, 2 * lanes), 1)
    side = folded // 2
    for slot in (1, 0):
        got = [
            fields[slot, lax.rem(sec + sections - g, sections), 1].astype(jnp.float32)
            for g in range(sections)
        ]
        for f in range(frames):
            r = f % group
            low, high = (
                jnp.concatenate(
                    [got[g][r * side : (r + 1) * side] for g in (2 * t, 2 * t + 1)], axis=0
                )
                for t in range(2)
            )
            if f < group:
                high = pltpu.roll(high, lanes, 1)
            else:
                low = pltpu.roll(low, lanes, 1)
            at_f = ((1 - slot) * frames + f) * folded
            noise_lines[at_f : at_f + folded, :] = jnp.where(lane < lanes, low, high)

    lines_f = jnp.concatenate(
        [
            fields[slot, lax.rem(sec + sections - f, sections), 0]
            for slot in (1, 0)
            for f in range(frames)
        ],
        axis=0,
    ).astype(jnp.float32)
    lines_f = ((noise_lines[...] - step_size[0] * lines_f) * std + mean_latent).astype(
        jnp.bfloat16
    ).astype(jnp.float32)
    count = 2 * frames * folded
    f_row = iota((count, 2 * lanes), 0)
    i_row = lax.rem(f_row, rows_i)
    lines_f = jnp.where((f_row >= frames * folded) | has_prev, lines_f, 0.0)
    before = jnp.where(i_row == 0, 0.0, pltpu.roll(lines_f, 1, 0))
    after = jnp.where(i_row == rows_i - 1, 0.0, pltpu.roll(lines_f, count - 1, 0))
    line_values = (
        dot(before.astype(jnp.bfloat16), places[0])
        + dot(lines_f.astype(jnp.bfloat16), places[1])
        + dot(after.astype(jnp.bfloat16), places[2])
    )
    half_j = cols_j // 2
    for f in range(2 * frames):
        for side in range(2):
            expanded[1 + side * half_j : 1 + (side + 1) * half_j, f] = line_values[
                f * folded : (f + 1) * folded, side * line_size : (side + 1) * line_size
            ].reshape(half_j, rows_i, line_size)
    block = near * rows_i
    for j in range(cols_j + 2):
        for a in range(3):
            stacked[j * block : (j + 1) * block, a * line_size : (a + 1) * line_size] = (
                expanded[j, a : a + near].reshape(block, line_size).astype(jnp.bfloat16)
            )
    dests = [
        jnp.where(is_end, mirrored(sections - 1), 0),
        jnp.where(is_end, mirrored(sections - 2), sections - 1),
        mirrored(jnp.where(is_end, 1, sections - 2)),
    ]
    parts = half // channels
    tall = near * height

    def upblock(homes):
        for q in range(2):
            lhs = jnp.concatenate(
                [
                    jnp.concatenate(
                        [
                            stacked[pl.ds(pl.multiple_of((j + q + n) * block, block), block), :]
                            for n in range(2)
                        ],
                        axis=1,
                    )
                    for j in homes
                ],
                axis=0,
            )
            for p in range(2):
                total = jnp.zeros((len(homes) * block, channels), jnp.float32)
                for h in range(2):
                    left = (p * 2 + h) * half
                    bias = in_bias[...] if h == 0 else peer_bias[...]
                    up = dot(lhs, taps_in[q, :, left : left + half]) + bias
                    up = up.astype(jnp.bfloat16).astype(jnp.float32)
                    for n in range(parts):
                        chunk = up[:, n * channels : (n + 1) * channels]
                        total = total + chunk * chunk
                    for m, j in enumerate(homes):
                        at_j = pl.ds(pl.multiple_of(2 * j * tall, tall) + q * tall + p, block, stride=2)
                        for n in range(parts):
                            ups[h * parts + n, at_j, :] = up[
                                m * block : (m + 1) * block, n * channels : (n + 1) * channels
                            ]
                for m, j in enumerate(homes):
                    at_j = pl.ds(pl.multiple_of(2 * j * tall, tall) + q * tall + p, block, stride=2)
                    squares[at_j, :] = total[m * block : (m + 1) * block]

    def homes_from(first):
        return [
            lax.rem(dests[0] * columns // 2 + cols_j + first + n, cols_j)
            for n in range(cols_j // 2)
        ]

    upblock(homes_from(-1))

    mine = lax.rem(sec + parts * core, 2 * parts)
    gain = norm_gain[pl.ds(sec, 1), :]
    h_row = lax.rem(iota((tall, channels), 0), height)
    valid = has_prev | (iota((tall, channels), 0) >= 2 * height)

    def normalise(w):
        at_w = pl.ds(pl.multiple_of(w * tall, tall), tall)
        mean = jnp.sum(squares[at_w, :], axis=1, keepdims=True) / (2 * half)
        v = ups[mine, at_w, :] * lax.rsqrt(mean + 1e-06) * gain
        v = jnp.where(valid, v / (1.0 + jnp.exp(-v)), 0.0)
        above = jnp.where(h_row == 0, 0.0, pltpu.roll(v, 1, 0))
        below = jnp.where(h_row == height - 1, 0.0, pltpu.roll(v, tall - 1, 0))
        for b, line_v in enumerate((above, v, below)):
            wide[w + 1, :, b * channels : (b + 1) * channels] = line_v.astype(jnp.bfloat16)

    span = frames * height
    pair_columns = columns // 2
    rows = pair_columns * span

    unit = jnp.where(core >= 0, 1.0, 0.0)

    def partial(d, m):
        windows, taps = [], []
        for a in range(3):
            for e in range(3):
                window = wide[
                    pl.ds(d * columns + e + m * pair_columns, pair_columns),
                    a * height : a * height + span,
                    :,
                ]
                windows.append(window.reshape(rows, 3 * channels))
                taps += [weight[9 * a + 3 * b + e] for b in range(3)]
        low, high = (
            dot(
                jnp.concatenate(windows[first:last], axis=1),
                jnp.concatenate(taps[3 * first : 3 * last], axis=0),
            )
            for first, last in ((0, 5), (5, 9))
        )
        return low + high * unit

    neighbour = mirrored(1)
    targets = [jnp.where(is_end, neighbour, d) for d in dests]
    far_n = jnp.where(up_side, 1, 0)
    slots = [
        jnp.where(is_end, 2, 1 - far_n),
        jnp.where(is_end, 3, far_n),
        jnp.where(is_end, 0, 1),
    ]
    direct = [is_end | up_side, is_end | jnp.logical_not(up_side), is_end]

    def sum_copy(n, w):
        return pltpu.make_async_remote_copy(
            send_buf.at[n, w], recv_buf.at[slots[n], w], sum_send.at[0],
            sum_recv.at[slots[n], w], device_id={"section": targets[n]},
        )

    def far_copy(w):
        return pltpu.make_async_remote_copy(
            send_buf.at[far_n, w], recv_buf.at[1, w], sum_send.at[0], sum_recv.at[1, w],
            device_id={"section": mirrored(sections - 1)},
        )

    def relay_far(*pieces_w):
        @pl.when(inner)
        def _():
            for w in pieces_w:
                send_buf[far_n, w] = (held[far_n, w] + arrived(2, w)).astype(jnp.bfloat16)
                far_copy(w).start()

    def arrived(slot, w):
        pltpu.make_async_copy(
            recv_buf.at[slot, w], recv_buf.at[slot, w], sum_recv.at[slot, w]
        ).wait()
        return recv_buf[slot, w].astype(jnp.float32)

    def by_column(value):
        return [value[w * span : (w + 1) * span] for w in range(pair_columns)]

    for t in range(columns + 2):
        normalise(lax.rem(dests[0] * columns + width - 1 + t, width))
    loads[3][0].wait()
    def hold(n, m):
        for c, value in enumerate(by_column(partial(dests[n], m))):
            w = m * pair_columns + c
            send_buf[n, w] = value.astype(jnp.bfloat16)
            held[n, w] = value

    def send(n, pieces_w):
        @pl.when(direct[n])
        def _():
            for w in pieces_w:
                sum_copy(n, w).start()

    for m in range(2):
        hold(0, m)
        send(0, range(m * pair_columns, (m + 1) * pair_columns))
    upblock(homes_from(cols_j // 2 - 1))
    for t in range(width - columns - 2):
        normalise(lax.rem(dests[0] * columns + columns + 1 + t, width))
    for m in range(2):
        hold(1, m)
    send(1, range(columns))
    relay_far(0)
    for m in range(2):
        hold(2, m)
    send(2, range(columns))
    relay_far(1, 2)

    for m in range(2):
        value = partial(sec, m) + conv_bias[...]
        residual = []
        for w in range(pair_columns):
            first = pl.multiple_of(
                (sec * columns + m * pair_columns + w) * tall + 2 * height, height
            )
            residual.append(
                jnp.concatenate([ups[n, pl.ds(first, span), :] for n in range(parts)], axis=1)
            )
        for w, own in enumerate(by_column(value)):
            acc[m * pair_columns + w] = own + residual[w]

    relay_far(*range(3, columns))

    @pl.when(inner)
    def _():
        for w in range(columns):
            send_buf[2, w] = (held[2, w] + arrived(3, w)).astype(jnp.bfloat16)
            sum_copy(2, w).start()


    def finish(order):
        for n in order[:-1]:
            for w in range(columns):
                acc[w] = acc[w] + arrived(n, w)
        for w in range(columns):
            total = acc[w] + arrived(order[-1], w)
            for c in range(parts):
                final[c, pl.ds(w, span, stride=columns), :] = total[
                    :, c * channels : (c + 1) * channels
                ]

    @pl.when(is_end)
    def _():
        finish((0, 1))

    @pl.when(inner)
    def _():
        finish((1, 0))

    for n in range(parts):
        out[:, n * channels : (n + 1) * channels] = final[n].astype(out.dtype)
    wait_rows(3 * columns * span * half * 2 // 512, sum_send.at[0])
    for c in early:
        c.wait_send()

    @pl.when(core == 0)
    def _():
        pair.wait_send()

    for first in (True, False):

        @pl.when(lead & (has_next != first))
        def _():
            count = 2 * (sections - 1) + (0 if first else 2 * sections) + 1
            wait_rows(count * field_rows, field_send.at[0])


def fused_shards(sizes, *arrays):
    (
        hidden, modulation, time_embed, head_weight, head_bias, noisy, step_size, latent_mean,
        latent_std, in_weight, in_bias, norm_gain, conv_weight, conv_bias,
    ) = arrays
    sections, clips_sp, frames, height, columns, lat, channels = sizes
    rows_i, cols_j, half = height // 2, columns * sections // 2, in_weight.shape[2]
    width, near, tokens, lanes = columns * sections, frames + 2, hidden.shape[0], 4 * lat
    line_size = 8 * lat
    f32, bf16 = jnp.float32, jnp.bfloat16
    vmem, dma = pltpu.VMEM, pltpu.SemaphoreType.DMA
    rows = columns * frames * height
    operands = (
        modulation, time_embed[None], head_bias[None], noisy.reshape(-1, lat),
        latent_std[None], latent_mean[None], in_bias[None], norm_gain.reshape(-1, channels),
        conv_bias[None], hidden, head_weight.T, in_weight, conv_weight,
    )
    operands = [pltpu.with_memory_space_constraint(value, pltpu.HBM) for value in operands]
    far = pl.BlockSpec(memory_space=pltpu.HBM)
    out = pl.pallas_call(
        functools.partial(block_kernel, sizes),
        out_shape=pltpu.VMEM((rows, half), bf16),
        in_specs=[far] * 4
        + [pl.BlockSpec(memory_space=pltpu.SMEM)]
        + [far] * (len(operands) - 4),
        out_specs=pl.BlockSpec(memory_space=pltpu.VMEM),
        scratch_shapes=[vmem(value.shape, value.dtype) for value in operands]
        + [
            vmem((tokens, tokens), bf16),
            vmem((rows // 8, rows), bf16),
            vmem((rows, 2 * lanes), f32),
            vmem((3, 2 * lanes, 2 * line_size), bf16),
            vmem((tokens + 8, 128), f32),
            vmem((tokens + 8, 128), f32),
            vmem(in_weight.shape, bf16),
            vmem((1, half), f32),
            vmem((2, sections, 2, tokens // 2, 2 * lanes), bf16),
            vmem((2 * frames * tokens // 2, 2 * lanes), f32),
            vmem((cols_j + 2, 2 * frames, rows_i, line_size), f32),
            vmem(((cols_j + 2) * near * rows_i, 3 * line_size), bf16),
            vmem((2, 6 * line_size, 4 * half), bf16),
            vmem((2 * half // channels, width * near * height, channels), f32),
            vmem((width * near * height, channels), f32),
            vmem((width + 2, near * height, 3 * channels), bf16),
            vmem((3, columns, rows // columns, half), bf16),
            vmem((4, columns, rows // columns, half), bf16),
            vmem((3, columns, rows // columns, half), f32),
            vmem((columns, rows // columns, half), f32),
            vmem((half // channels, rows, channels), f32),
            dma((4,)),
            dma((3,)),
            dma((3,)),
            dma((1,)),
            dma((1,)),
            dma((1,)),
            dma((4, columns)),
        ],
        compiler_params=pltpu.CompilerParams(
            collective_id=0, has_side_effects=True, vmem_limit_bytes=40 * 2**20
        ),
    )(*operands[:4], step_size, *operands[4:])
    return out.reshape(frames, height, columns, half)


def dispatch(*arrays):
    hidden, noisy, in_weight, conv_weight = arrays[0], arrays[5], arrays[9], arrays[12]
    frames, height, columns, lat = noisy.shape
    sections, cores, clips_sp = (lax.axis_size(axis) for axis in ("section", "tp", "sp"))
    channels, half = conv_weight.shape[1:]
    whole_frame = hidden.shape[0] == height // 2 * (columns * sections // 2)
    if (
        whole_frame
        and cores == 2
        and clips_sp > 1
        and frames == sections
        and sections == 4
        and columns % 2 == 0
        and channels % 128 == 0
        and half % channels == 0
        and lat == 16
        and height == 16
    ):
        sizes = (sections, clips_sp, frames, height, columns, lat, channels)
        return fused_shards(sizes, *arrays)
    return shards(*arrays)


def solution(mesh):
    placed = (
        P(("groups", "sp", "section"), "tp"),
        P(None, "tp"),
        P(("groups", "tp")),
        P("tp", None),
        P(),
        P(("groups", "sp"), None, "section", None),
        P("groups"),
        P(),
        P(),
        P(None, None, "tp"),
        P("tp"),
        P(),
        P(None, "section", "tp"),
        P("tp"),
    )
    return jax.shard_map(
        dispatch,
        mesh=mesh,
        in_specs=placed,
        out_specs=P(("groups", "sp"), None, "section", "tp"),
        check_vma=False,
    )
```

```python
import functools

import jax
import jax.numpy as jnp
from jax import lax
from jax.experimental import pallas as pl
from jax.experimental.pallas import tpu as pltpu
from jax.sharding import PartitionSpec as P

D = 6144


def padded_2(value, sides, width):
    for axis, dim in sides:
        count, length = (lax.axis_size(axis), value.shape[dim])
        up = [(i, (i + 1) % count) for i in range(count - 1)]
        down = [(j, i) for i, j in up]
        last = lax.slice_in_dim(value, length - width, length, axis=dim)
        leading = lax.slice_in_dim(value, 0, width, axis=dim)
        before = lax.ppermute(last, axis, up)
        after = lax.ppermute(leading, axis, down)
        value = jnp.concatenate([before, value, after], axis=dim)
    return value


def passed_along(value, axis, by):
    count = lax.axis_size(axis)
    pairs = [(i, i + by) for i in range(count) if 0 <= i + by < count]
    return lax.ppermute(value, axis, pairs)


def conv_taps(padded, weight, frames, height, columns):
    channels = padded.shape[3]
    result = jnp.zeros((frames * height * columns, weight.shape[2]), jnp.float32)
    for offset_time in range(3):
        for offset_row in range(3):
            slab = padded[offset_time : offset_time + frames, offset_row : offset_row + height]
            window = jnp.concatenate(
                [slab[:, :, 0:columns], slab[:, :, 1 : columns + 1], slab[:, :, 2 : columns + 2]],
                axis=3,
            )
            first = 9 * offset_time + 3 * offset_row
            taps = weight[first : first + 3].reshape(3 * channels, weight.shape[2])
            result = result + jnp.dot(
                window.reshape(-1, 3 * channels), taps, preferred_element_type=jnp.float32
            )
    return result


def activate(source, gain_vector):
    values = source.astype(jnp.float32)
    squares = jnp.mean(values * values, axis=-1, keepdims=True)
    return jax.nn.silu(values * lax.rsqrt(squares + 1e-06) * gain_vector).astype(jnp.bfloat16)


def pad_rows(source):
    return jnp.pad(source, ((0, 0), (1, 1), (0, 0), (0, 0)))


def shards(
    hidden,
    modulation,
    time_embed,
    head_weight,
    head_bias,
    noisy,
    step_size,
    latent_mean,
    latent_std,
    in_weight,
    in_bias,
    norm_gain,
    conv_weight,
    conv_bias,
):
    frames, height, columns, lat_channels = noisy.shape
    sections = lax.axis_size("section")
    half_channels = in_weight.shape[2]
    values = hidden.astype(jnp.float32)
    row_sums, square_sums = lax.psum(
        (jnp.sum(values, axis=1), jnp.sum(values * values, axis=1)), "tp"
    )
    average = row_sums / D
    variance = square_sums / D - average * average
    shift_term = modulation[0] + time_embed
    scale_term = modulation[1] + time_embed
    modulated = (
        (values - average[:, None]) * lax.rsqrt(variance[:, None] + 1e-06) * (1.0 + scale_term)
        + shift_term
    ).astype(jnp.bfloat16)
    partial_sum = jnp.dot(modulated, head_weight, preferred_element_type=jnp.float32)
    velocity = (lax.psum(partial_sum, "tp") + head_bias).astype(jnp.bfloat16)
    band_rows = velocity.shape[0] * 2 // (columns * sections)
    outgoing = velocity.reshape(band_rows, sections, -1)
    arrived = lax.all_to_all(outgoing, "section", split_axis=1, concat_axis=0, tiled=True)
    latent_field = arrived.reshape(frames, height // 2, columns // 2, 2, 2, lat_channels)
    latent_field = jnp.transpose(latent_field, (0, 1, 3, 2, 4, 5)).reshape(
        frames, height, columns, lat_channels
    )
    latent = (
        (noisy.astype(jnp.float32) - step_size[0] * latent_field.astype(jnp.float32)) * latent_std
        + latent_mean
    ).astype(jnp.bfloat16)
    latent_wide = padded_2(latent, (("section", 2),), 2)
    earlier = passed_along(latent_wide, "sp", 1)
    stacked = pad_rows(jnp.concatenate([earlier, latent_wide], axis=0))
    extended = (conv_taps(stacked, in_weight, frames + 2, height, columns + 2) + in_bias).astype(
        jnp.bfloat16
    )
    extended = extended.reshape(frames + 2, height, columns + 2, half_channels)
    upblock_half = extended[2:, :, 1 : columns + 1]
    extended_full = lax.all_gather(extended, "tp", axis=3, tiled=True)
    normed = activate(extended_full, norm_gain)
    frame_index = lax.axis_index("sp") * frames - 2 + jnp.arange(frames + 2, dtype=jnp.int32)
    column_index = (
        lax.axis_index("section") * columns - 1 + jnp.arange(columns + 2, dtype=jnp.int32)
    )
    inside_cols = (column_index >= 0) & (column_index < columns * sections)
    inside = (frame_index >= 0)[:, None, None, None] & inside_cols[None, None, :, None]
    conv_input = pad_rows(jnp.where(inside, normed, jnp.zeros_like(normed)))
    full_weight = lax.all_gather(conv_weight, "section", axis=1, tiled=True)
    mixed = conv_taps(conv_input, full_weight, frames, height, columns)
    decoded = (
        upblock_half.astype(jnp.float32).reshape(-1, half_channels) + mixed + conv_bias
    ).astype(jnp.bfloat16)
    return decoded.reshape(frames, height, columns, half_channels)


def iota(shape, dim):
    return lax.broadcasted_iota(jnp.int32, shape, dim)


def dot(left, right):
    return jnp.dot(left, right, preferred_element_type=jnp.float32)


def dot_rows(left, right):
    return lax.dot_general(
        left, right, (((1,), (1,)), ((), ())), preferred_element_type=jnp.float32
    )


def pieces(value):
    high = value.astype(jnp.bfloat16)
    rest = value - high.astype(jnp.float32)
    middle = rest.astype(jnp.bfloat16)
    low = (rest - middle.astype(jnp.float32)).astype(jnp.bfloat16)
    return high.astype(jnp.float32), middle.astype(jnp.float32), low.astype(jnp.float32)


def block_kernel(
    sizes,
    modulation_far,
    time_far,
    head_bias_far,
    noisy_far,
    step_size,
    std_far,
    mean_far,
    in_bias_far,
    gain_far,
    conv_bias_far,
    hidden_far,
    head_far,
    in_far,
    conv_far,
    out,
    modulation,
    time_embed,
    head_bias,
    noisy,
    latent_std,
    latent_mean,
    in_bias,
    norm_gain,
    conv_bias,
    hidden,
    head_weight,
    in_weight,
    weight,
    swap,
    noise_pick,
    noise_mask,
    places,
    part,
    peer_part,
    peer_weight,
    peer_bias,
    fields,
    noise_lines,
    expanded,
    stacked,
    taps_in,
    ups,
    squares,
    wide,
    send_buf,
    recv_buf,
    held,
    acc,
    final,
    load_sems,
    pair_send,
    pair_recv,
    field_send,
    field_recv,
    sum_send,
    sum_recv,
):
    sections, clips_sp, frames, height, columns, lat, channels = sizes
    rows_i, cols_j = height // 2, columns * sections // 2
    width = columns * sections
    tokens = rows_i * cols_j
    near = frames + 2
    half = in_weight.shape[2]
    lanes = 4 * lat
    folded = tokens // 2
    line_size = 4 * 2 * lat
    sec, core, spi = lax.axis_index("section"), lax.axis_index("tp"), lax.axis_index("sp")
    nxt = lax.rem(spi + 1, clips_sp)
    prv = lax.rem(spi + clips_sp - 1, clips_sp)
    has_next, has_prev = spi + 1 < clips_sp, spi > 0
    peer = {"tp": 1 - core}

    lead = core == 1
    unit = jnp.where(core >= 0, 1.0, 0.0)
    barrier = pltpu.get_barrier_semaphore()
    pl.semaphore_signal(barrier, inc=1, device_id=peer)
    for k in range(1, sections):
        pl.semaphore_signal(
            barrier, inc=1, device_id={"section": lax.rem(sec + k, sections), "tp": 1}
        )

    @pl.when(has_prev)
    def _():
        for k in range(sections):
            pl.semaphore_signal(
                barrier,
                inc=1,
                device_id={"section": lax.rem(sec + k, sections), "sp": prv, "tp": 1},
            )


    groups = (
        ((hidden_far, hidden), (head_far, head_weight)),
        ((modulation_far, modulation), (time_far, time_embed)),
        (
            (noisy_far, noisy),
            (in_bias_far, in_bias),
            (head_bias_far, head_bias),
            (std_far, latent_std),
            (mean_far, latent_mean),
            (gain_far, norm_gain),
            (conv_bias_far, conv_bias),
        ),
        ((conv_far, weight),),
        ((in_far, in_weight),),
    )
    loads = [
        [pltpu.make_async_copy(source, target, load_sems.at[n]) for source, target in members]
        for n, members in enumerate(groups)
    ]
    for c in loads[1] + loads[0] + loads[2]:
        c.start()

    def pair_copy(n, source, target):
        return pltpu.make_async_remote_copy(
            source, target, pair_send.at[n], pair_recv.at[n], device_id=peer
        )

    def wait_rows(count, sem):
        view = ups.at[0, pl.ds(0, count), :]
        pltpu.make_async_copy(view, view, sem).wait()

    up_side = sec < sections // 2
    is_end = (sec == 0) | (sec == sections - 1)
    inner = jnp.logical_not(is_end)

    def mirrored(value):
        return jnp.where(up_side, value, sections - 1 - value)

    others = [mirrored(jnp.where(is_end, sections - 1 - n, (3, 2, 0)[n])) for n in range(3)]

    def spread_copy(z, ahead, c):
        slot = lax.rem(z - sec + sections, sections)
        return pltpu.make_async_remote_copy(
            fields.at[0, 0], fields.at[ahead, slot], field_send.at[0], field_recv.at[0],
            device_id={"section": z, "sp": nxt if ahead else spi, "tp": c},
        )

    def spread():
        for z in [*others, sec]:
            for c in (0, 1):
                if z is not sec:
                    spread_copy(z, 0, c).start()

                @pl.when(has_next)
                def _():
                    spread_copy(z, 1, c).start()

        pltpu.make_async_remote_copy(
            fields.at[0, 0], fields.at[0, 0], field_send.at[0], field_recv.at[0], device_id=peer
        ).start()

    field_rows = 2 * folded * 2 * lanes * 2 // 512

    to, at = iota((tokens, tokens), 0), iota((tokens, tokens), 1)
    swap[...] = (lax.rem(to, rows_i) * cols_j + lax.div(to, rows_i) == at).astype(jnp.bfloat16)
    cells = frames * height * columns
    group = frames // 2
    r_line, r_col = lax.div(iota((cells, 2 * lanes), 0), columns), lax.rem(
        iota((cells, 2 * lanes), 0), columns
    )
    r_slot = lax.div(lax.div(r_line, height), group) * 4 + lax.rem(r_line, 2) * 2 + lax.rem(r_col, 2)
    noise_mask[...] = (lax.div(iota((cells, 2 * lanes), 1), lat) == r_slot).astype(jnp.float32)
    packed = cells // 8
    r_at, r_to = iota((packed, cells), 1), iota((packed, cells), 0)
    r_line, r_col = lax.div(r_at, columns), lax.rem(r_at, columns)
    r_home = (
        lax.rem(lax.div(r_line, height), group) * (columns // 2) + lax.div(r_col, 2)
    ) * rows_i + lax.div(lax.rem(r_line, height), 2)
    noise_pick[...] = (r_to == r_home).astype(jnp.bfloat16)
    shape = (2 * lanes, 2 * line_size)
    src, dst = iota(shape, 0), iota(shape, 1)
    same = lax.div(src, lanes) == lax.div(dst, line_size)
    src, dst = lax.rem(src, lanes), lax.rem(dst, line_size)
    places[0 * shape[0] : (0 + 1) * shape[0]] = (same & (src == dst + 2 * lat) & (dst < 2 * lat)).astype(jnp.bfloat16)
    places[1 * shape[0] : (1 + 1) * shape[0]] = (same & (src + 2 * lat == dst)).astype(jnp.bfloat16)
    places[2 * shape[0] : (2 + 1) * shape[0]] = (same & (src + 6 * lat == dst) & (dst >= 6 * lat)).astype(jnp.bfloat16)
    expanded[...] = jnp.zeros_like(expanded)
    taps_in[...] = jnp.zeros_like(taps_in)
    wide[0] = jnp.zeros_like(wide[0])
    wide[width + 1] = jnp.zeros_like(wide[0])

    @pl.when(jnp.logical_not(has_prev))
    def _():
        fields[1] = jnp.zeros_like(fields[1])

    features = hidden.shape[1]
    for c in loads[1]:
        c.wait()
    scale = 1.0 + (modulation[1:2, :] + time_embed[...])
    shift = modulation[0:1, :] + time_embed[...]
    row = iota((8, features), 0)
    lines = jnp.zeros((8, features), jnp.float32)
    for n, piece in enumerate(pieces(scale) + pieces(shift)):
        lines = jnp.where(row == n, piece, lines)
    lines = jnp.concatenate([lines, jnp.zeros_like(lines)], axis=0).astype(jnp.bfloat16)
    for c in loads[0]:
        c.wait()
    loads[4][0].start()
    loads[3][0].start()
    values = hidden[...].astype(jnp.float32)
    own_sum = jnp.sum(values, axis=1, keepdims=True)
    own_square = jnp.sum(values * values, axis=1, keepdims=True)
    center = own_sum / features
    centred = ((values - center) * scale).astype(jnp.bfloat16)
    stack = jnp.concatenate([centred, lines], axis=0)
    cut = features // 2
    made = dot_rows(stack[:, :cut], head_weight[:, :cut])
    made = made + dot_rows(stack[:, cut:], head_weight[:, cut:]) * unit
    part[:tokens, :lanes] = made[:tokens]
    stat_shape = (tokens, 128 - lanes)
    part[:tokens, lanes:] = jnp.where(
        iota(stat_shape, 1) < stat_shape[1] // 2, own_sum, own_square
    )
    made = made[tokens:]
    line = iota(made.shape, 0)
    own_scale = jnp.sum(jnp.where(line < 3, made, 0.0), axis=0, keepdims=True)
    own_shift = jnp.sum(jnp.where(line < 3, 0.0, made), axis=0, keepdims=True)
    part[tokens:, :lanes] = jnp.where(iota((8, lanes), 0) == 0, own_scale, own_shift)
    part[tokens:, lanes:] = jnp.zeros((8, 128 - lanes), jnp.float32)
    pair = pair_copy(0, part, peer_part)
    early = [pair_copy(1, in_weight, peer_weight), pair_copy(2, in_bias, peer_bias)]
    for c in loads[2]:
        c.wait()
    std = jnp.concatenate([latent_std[...]] * 8, axis=1)
    mean_latent = jnp.concatenate([latent_mean[...]] * 8, axis=1)

    @pl.when(core == 0)
    def _():
        pl.semaphore_wait(barrier, 1)
        pair.start()
        loads[4][0].wait()
        for c in early:
            c.start()

    @pl.when(lead)
    def _():
        src, dst = iota((lat, 2 * lanes), 0), iota((lat, 2 * lanes), 1)
        tiled = dot(noisy[...], (src == lax.rem(dst, lat)).astype(jnp.bfloat16))
        tiled = (tiled * noise_mask[...]).astype(jnp.bfloat16)
        fields[0, 0, 1] = dot(noise_pick[...], tiled).astype(jnp.bfloat16)
        pair.wait_recv()
        far_sum = peer_part[:tokens, lanes : lanes + 1]
        far_square = peer_part[
            :tokens, lanes + (128 - lanes) // 2 : lanes + (128 - lanes) // 2 + 1
        ]
        average = (own_sum + far_sum) / D
        variance = (own_square + far_square) / D - average * average
        body = (
            part[:tokens, :lanes]
            + peer_part[:tokens, :lanes]
            - (average - center) * own_scale
            - (average - far_sum / features) * peer_part[tokens : tokens + 1, :lanes]
        )
        velocity = (
            lax.rsqrt(variance + 1e-06) * body
            + (own_shift + peer_part[tokens + 1 : tokens + 2, :lanes])
            + head_bias[...]
        ).astype(jnp.bfloat16)
        field = dot(swap[...], velocity)
        fields[0, 0, 0] = jnp.concatenate([field[:folded], field[folded:]], axis=1).astype(
            jnp.bfloat16
        )
        pl.semaphore_wait(
            barrier, 2 * sections - 1 + jnp.where(has_next, 2 * sections, 0)
        )
        spread()
        loads[4][0].wait()
        for c in early:
            c.start()

    for c in early:
        c.wait_recv()
    for q in range(2):
        for e in range(3):
            col = q + e
            step_j, odd = (col + 1) // 2 - q, (col + 1) % 2
            for a in range(3):
                for b in range(3):
                    tap = 9 * a + 3 * b + e
                    for p in range(2):
                        first = step_j * 3 * line_size + a * line_size + (p + b) * 2 * lat + odd * lat
                        left = p * 2 * half
                        taps_in[q, first : first + lat, left : left + half] = in_weight[tap]
                        taps_in[q, first : first + lat, left + half : left + 2 * half] = peer_weight[tap]

    for on_lead in (True, False):
        for first in (True, False):

            @pl.when((lead == on_lead) & (has_prev != first))
            def _():
                count = sections - 1 + (0 if first else sections) + (0 if on_lead else 1)
                wait_rows(count * field_rows, field_recv.at[0])

    lane = iota((folded, 2 * lanes), 1)
    side = folded // 2
    for slot in (1, 0):
        got = [
            fields[slot, lax.rem(sec + sections - g, sections), 1].astype(jnp.float32)
            for g in range(sections)
        ]
        for f in range(frames):
            r = f % group
            low, high = (
                jnp.concatenate(
                    [got[g][r * side : (r + 1) * side] for g in (2 * t, 2 * t + 1)], axis=0
                )
                for t in range(2)
            )
            if f < group:
                high = pltpu.roll(high, lanes, 1)
            else:
                low = pltpu.roll(low, lanes, 1)
            at_f = ((1 - slot) * frames + f) * folded
            noise_lines[at_f : at_f + folded, :] = jnp.where(lane < lanes, low, high)

    lines_f = jnp.concatenate(
        [
            fields[slot, lax.rem(sec + sections - f, sections), 0]
            for slot in (1, 0)
            for f in range(frames)
        ],
        axis=0,
    ).astype(jnp.float32)
    lines_f = ((noise_lines[...] - step_size[0] * lines_f) * std + mean_latent).astype(
        jnp.bfloat16
    ).astype(jnp.float32)
    count = 2 * frames * folded
    f_row = iota((count, 2 * lanes), 0)
    i_row = lax.rem(f_row, rows_i)
    lines_f = jnp.where((f_row >= frames * folded) | has_prev, lines_f, 0.0)
    before = jnp.where(i_row == 0, 0.0, pltpu.roll(lines_f, 1, 0))
    after = jnp.where(i_row == rows_i - 1, 0.0, pltpu.roll(lines_f, count - 1, 0))
    shifted = jnp.concatenate([before, lines_f, after], axis=1).astype(jnp.bfloat16)
    line_values = jnp.concatenate(
        [
            dot(shifted[n * count // 2 : (n + 1) * count // 2], places[...])
            for n in range(2)
        ],
        axis=0,
    )
    half_j = cols_j // 2
    for f in range(2 * frames):
        for side in range(2):
            expanded[1 + side * half_j : 1 + (side + 1) * half_j, f] = line_values[
                f * folded : (f + 1) * folded, side * line_size : (side + 1) * line_size
            ].reshape(half_j, rows_i, line_size)
    block = near * rows_i
    for j in range(cols_j + 2):
        for a in range(3):
            stacked[j * block : (j + 1) * block, a * line_size : (a + 1) * line_size] = (
                expanded[j, a : a + near].reshape(block, line_size).astype(jnp.bfloat16)
            )
    dests = [
        jnp.where(is_end, mirrored(sections - 1), 0),
        jnp.where(is_end, mirrored(sections - 2), sections - 1),
        mirrored(jnp.where(is_end, 1, sections - 2)),
    ]
    parts = half // channels
    tall = near * height

    def upblock(homes):
        for q in range(2):
            lhs = jnp.concatenate(
                [
                    jnp.concatenate(
                        [
                            stacked[pl.ds(pl.multiple_of((j + q + n) * block, block), block), :]
                            for n in range(2)
                        ],
                        axis=1,
                    )
                    for j in homes
                ],
                axis=0,
            )
            for p in range(2):
                total = jnp.zeros((len(homes) * block, channels), jnp.float32)
                for h in range(2):
                    left = (p * 2 + h) * half
                    bias = in_bias[...] if h == 0 else peer_bias[...]
                    up = dot(lhs, taps_in[q, :, left : left + half]) + bias
                    up = up.astype(jnp.bfloat16).astype(jnp.float32)
                    for n in range(parts):
                        chunk = up[:, n * channels : (n + 1) * channels]
                        total = total + chunk * chunk
                    for m, j in enumerate(homes):
                        at_j = pl.ds(pl.multiple_of(2 * j * tall, tall) + q * tall + p, block, stride=2)
                        for n in range(parts):
                            ups[h * parts + n, at_j, :] = up[
                                m * block : (m + 1) * block, n * channels : (n + 1) * channels
                            ]
                for m, j in enumerate(homes):
                    at_j = pl.ds(pl.multiple_of(2 * j * tall, tall) + q * tall + p, block, stride=2)
                    squares[at_j, :] = total[m * block : (m + 1) * block]

    edge_high = dests[0] > 0
    first_home = jnp.where(edge_high, cols_j - 2, 0)
    upblock([first_home, first_home + 1])

    mine = lax.rem(sec + parts * core, 2 * parts)
    gain = norm_gain[pl.ds(sec, 1), :]
    h_row = lax.rem(iota((tall, channels), 0), height)
    valid = has_prev | (iota((tall, channels), 0) >= 2 * height)

    def normalise(w):
        at_w = pl.ds(pl.multiple_of(w * tall, tall), tall)
        mean = jnp.sum(squares[at_w, :], axis=1, keepdims=True) / (2 * half)
        v = ups[mine, at_w, :] * lax.rsqrt(mean + 1e-06) * gain
        v = jnp.where(valid, v / (1.0 + jnp.exp(-v)), 0.0)
        above = jnp.where(h_row == 0, 0.0, pltpu.roll(v, 1, 0))
        below = jnp.where(h_row == height - 1, 0.0, pltpu.roll(v, tall - 1, 0))
        for b, line_v in enumerate((above, v, below)):
            wide[w + 1, :, b * channels : (b + 1) * channels] = line_v.astype(jnp.bfloat16)

    span = frames * height
    pair_columns = columns // 2

    def partial(d, first_column, count):
        windows, taps = [], []
        for a in range(3):
            for e in range(3):
                window = wide[
                    pl.ds(d * columns + e + first_column, count),
                    a * height : a * height + span,
                    :,
                ]
                windows.append(window.reshape(count * span, 3 * channels))
                taps += [weight[9 * a + 3 * b + e] for b in range(3)]
        low, high = (
            dot(
                jnp.concatenate(windows[first:last], axis=1),
                jnp.concatenate(taps[3 * first : 3 * last], axis=0),
            )
            for first, last in ((0, 5), (5, 9))
        )
        value = low + high * unit
        return [value[w * span : (w + 1) * span] for w in range(count)]

    neighbour = mirrored(1)
    targets = [jnp.where(is_end, neighbour, d) for d in dests]
    far_n = jnp.where(up_side, 1, 0)
    slots = [
        jnp.where(is_end, 2, 1 - far_n),
        jnp.where(is_end, 3, far_n),
        jnp.where(is_end, 0, 1),
    ]
    direct = [is_end | up_side, is_end | jnp.logical_not(up_side), is_end]

    def sum_copy(n, w):
        return pltpu.make_async_remote_copy(
            send_buf.at[n, w], recv_buf.at[slots[n], w], sum_send.at[0],
            sum_recv.at[slots[n], w], device_id={"section": targets[n]},
        )

    def far_copy(w):
        return pltpu.make_async_remote_copy(
            send_buf.at[far_n, w], recv_buf.at[1, w], sum_send.at[0], sum_recv.at[1, w],
            device_id={"section": mirrored(sections - 1)},
        )

    def relay_far(side, *pieces_w):
        @pl.when(inner & (up_side if side else jnp.logical_not(up_side)))
        def _():
            for n in pieces_w:
                w = jnp.where(up_side, (2, 3, 1, 0)[n], n)
                send_buf[far_n, w] = (held[far_n, w] + arrived(2, w)).astype(jnp.bfloat16)
                far_copy(w).start()

    def arrived(slot, w):
        pltpu.make_async_copy(
            recv_buf.at[slot, w], recv_buf.at[slot, w], sum_recv.at[slot, w]
        ).wait()
        return recv_buf[slot, w].astype(jnp.float32)

    for t in range(4):
        normalise(2 * first_home + t)

    later = [4, *range(width - 1, width - 2 - columns, -1), *range(5, width - 1 - columns)]

    def normalise_next(numbers):
        for n in numbers:
            inward = jnp.where(edge_high, width - 5 - n, 4 + n)
            normalise(jnp.where(is_end, inward, later[n]))

    loads[3][0].wait()
    def hold(n, first_column, count):
        for c, value in enumerate(partial(dests[n], first_column, count)):
            send_buf[n, first_column + c] = value.astype(jnp.bfloat16)
            held[n, first_column + c] = value

    def send(n, pieces_w):
        @pl.when(direct[n])
        def _():
            for w in pieces_w:
                sum_copy(n, w).start()

    first_pair = jnp.where(edge_high, columns - 2, 0)
    third, fourth = jnp.where(edge_high, 1, 2), jnp.where(edge_high, 0, 3)
    hold(0, first_pair, 2)
    send(0, (first_pair, first_pair + 1))
    hold(0, third, 1)
    send(0, (third,))
    upblock([lax.rem(first_home + 2 + n, cols_j) for n in range(cols_j - 2)])
    normalise_next((0,))
    hold(0, fourth, 1)
    send(0, (fourth,))
    normalise_next(range(1, columns + 2))
    relay_far(False, 0)
    for m in range(2):
        hold(1, m * pair_columns, pair_columns)
        send(1, range(m * pair_columns, (m + 1) * pair_columns))
    relay_far(False, 1)
    normalise_next(range(columns + 2, width - 4))
    relay_far(False, 2)
    relay_far(True, 0)
    for m in range(2):
        hold(2, m * pair_columns, pair_columns)
    send(2, range(columns))
    relay_far(False, 3)
    relay_far(True, 1)

    for m in range(2):
        values = partial(sec, m * pair_columns, pair_columns)
        residual = []
        for w in range(pair_columns):
            first = pl.multiple_of(
                (sec * columns + m * pair_columns + w) * tall + 2 * height, height
            )
            residual.append(
                jnp.concatenate([ups[n, pl.ds(first, span), :] for n in range(parts)], axis=1)
            )
        for w, own in enumerate(values):
            acc[m * pair_columns + w] = own + conv_bias[...] + residual[w]

    relay_far(True, 2, 3)

    @pl.when(inner)
    def _():
        for w in range(columns):
            send_buf[2, w] = (held[2, w] + arrived(3, w)).astype(jnp.bfloat16)
            sum_copy(2, w).start()


    def finish(order):
        for n in order[:-1]:
            for w in range(columns):
                acc[w] = acc[w] + arrived(n, w)
        for w in range(columns):
            total = acc[w] + arrived(order[-1], w)
            for c in range(parts):
                final[c, pl.ds(w, span, stride=columns), :] = total[
                    :, c * channels : (c + 1) * channels
                ]


    @pl.when(is_end)
    def _():
        finish((0, 1))

    @pl.when(inner)
    def _():
        finish((1, 0))

    for n in range(parts):
        out[:, n * channels : (n + 1) * channels] = final[n].astype(out.dtype)
    wait_rows(3 * columns * span * half * 2 // 512, sum_send.at[0])
    for c in early:
        c.wait_send()

    @pl.when(core == 0)
    def _():
        pair.wait_send()

    for first in (True, False):

        @pl.when(lead & (has_next != first))
        def _():
            count = 2 * (sections - 1) + (0 if first else 2 * sections) + 1
            wait_rows(count * field_rows, field_send.at[0])


def fused_shards(sizes, *arrays):
    (
        hidden, modulation, time_embed, head_weight, head_bias, noisy, step_size, latent_mean,
        latent_std, in_weight, in_bias, norm_gain, conv_weight, conv_bias,
    ) = arrays
    sections, clips_sp, frames, height, columns, lat, channels = sizes
    rows_i, cols_j, half = height // 2, columns * sections // 2, in_weight.shape[2]
    width, near, tokens, lanes = columns * sections, frames + 2, hidden.shape[0], 4 * lat
    line_size = 8 * lat
    f32, bf16 = jnp.float32, jnp.bfloat16
    vmem, dma = pltpu.VMEM, pltpu.SemaphoreType.DMA
    rows = columns * frames * height
    operands = (
        modulation, time_embed[None], head_bias[None], noisy.reshape(-1, lat),
        latent_std[None], latent_mean[None], in_bias[None], norm_gain.reshape(-1, channels),
        conv_bias[None], hidden, head_weight.T, in_weight, conv_weight,
    )
    operands = [pltpu.with_memory_space_constraint(value, pltpu.HBM) for value in operands]
    far = pl.BlockSpec(memory_space=pltpu.HBM)
    out = pl.pallas_call(
        functools.partial(block_kernel, sizes),
        out_shape=pltpu.VMEM((rows, half), bf16),
        in_specs=[far] * 4
        + [pl.BlockSpec(memory_space=pltpu.SMEM)]
        + [far] * (len(operands) - 4),
        out_specs=pl.BlockSpec(memory_space=pltpu.VMEM),
        scratch_shapes=[vmem(value.shape, value.dtype) for value in operands]
        + [
            vmem((tokens, tokens), bf16),
            vmem((rows // 8, rows), bf16),
            vmem((rows, 2 * lanes), f32),
            vmem((6 * lanes, 2 * line_size), bf16),
            vmem((tokens + 8, 128), f32),
            vmem((tokens + 8, 128), f32),
            vmem(in_weight.shape, bf16),
            vmem((1, half), f32),
            vmem((2, sections, 2, tokens // 2, 2 * lanes), bf16),
            vmem((2 * frames * tokens // 2, 2 * lanes), f32),
            vmem((cols_j + 2, 2 * frames, rows_i, line_size), f32),
            vmem(((cols_j + 2) * near * rows_i, 3 * line_size), bf16),
            vmem((2, 6 * line_size, 4 * half), bf16),
            vmem((2 * half // channels, width * near * height, channels), f32),
            vmem((width * near * height, channels), f32),
            vmem((width + 2, near * height, 3 * channels), bf16),
            vmem((3, columns, rows // columns, half), bf16),
            vmem((4, columns, rows // columns, half), bf16),
            vmem((3, columns, rows // columns, half), f32),
            vmem((columns, rows // columns, half), f32),
            vmem((half // channels, rows, channels), f32),
            dma((5,)),
            dma((3,)),
            dma((3,)),
            dma((1,)),
            dma((1,)),
            dma((1,)),
            dma((4, columns)),
        ],
        compiler_params=pltpu.CompilerParams(
            collective_id=0, has_side_effects=True, vmem_limit_bytes=40 * 2**20
        ),
    )(*operands[:4], step_size, *operands[4:])
    return out.reshape(frames, height, columns, half)


def dispatch(*arrays):
    hidden, noisy, in_weight, conv_weight = arrays[0], arrays[5], arrays[9], arrays[12]
    frames, height, columns, lat = noisy.shape
    sections, cores, clips_sp = (lax.axis_size(axis) for axis in ("section", "tp", "sp"))
    channels, half = conv_weight.shape[1:]
    whole_frame = hidden.shape[0] == height // 2 * (columns * sections // 2)
    if (
        whole_frame
        and cores == 2
        and clips_sp > 1
        and frames == sections
        and sections == 4
        and columns == 4
        and channels % 128 == 0
        and half % channels == 0
        and lat == 16
        and height == 16
    ):
        sizes = (sections, clips_sp, frames, height, columns, lat, channels)
        return fused_shards(sizes, *arrays)
    return shards(*arrays)


def solution(mesh):
    placed = (
        P(("groups", "sp", "section"), "tp"),
        P(None, "tp"),
        P(("groups", "tp")),
        P("tp", None),
        P(),
        P(("groups", "sp"), None, "section", None),
        P("groups"),
        P(),
        P(),
        P(None, None, "tp"),
        P("tp"),
        P(),
        P(None, "section", "tp"),
        P("tp"),
    )
    return jax.shard_map(
        dispatch,
        mesh=mesh,
        in_specs=placed,
        out_specs=P(("groups", "sp"), None, "section", "tp"),
        check_vma=False,
    )
```

```python
import functools

import jax
import jax.numpy as jnp
from jax import lax
from jax.experimental import pallas as pl
from jax.experimental.pallas import tpu as pltpu
from jax.sharding import PartitionSpec as P

D = 6144


def padded_2(value, sides, width):
    for axis, dim in sides:
        count, length = (lax.axis_size(axis), value.shape[dim])
        up = [(i, (i + 1) % count) for i in range(count - 1)]
        down = [(j, i) for i, j in up]
        last = lax.slice_in_dim(value, length - width, length, axis=dim)
        leading = lax.slice_in_dim(value, 0, width, axis=dim)
        before = lax.ppermute(last, axis, up)
        after = lax.ppermute(leading, axis, down)
        value = jnp.concatenate([before, value, after], axis=dim)
    return value


def passed_along(value, axis, by):
    count = lax.axis_size(axis)
    pairs = [(i, i + by) for i in range(count) if 0 <= i + by < count]
    return lax.ppermute(value, axis, pairs)


def conv_taps(padded, weight, frames, height, columns):
    channels = padded.shape[3]
    result = jnp.zeros((frames * height * columns, weight.shape[2]), jnp.float32)
    for offset_time in range(3):
        for offset_row in range(3):
            slab = padded[offset_time : offset_time + frames, offset_row : offset_row + height]
            window = jnp.concatenate(
                [slab[:, :, 0:columns], slab[:, :, 1 : columns + 1], slab[:, :, 2 : columns + 2]],
                axis=3,
            )
            first = 9 * offset_time + 3 * offset_row
            taps = weight[first : first + 3].reshape(3 * channels, weight.shape[2])
            result = result + jnp.dot(
                window.reshape(-1, 3 * channels), taps, preferred_element_type=jnp.float32
            )
    return result


def activate(source, gain_vector):
    values = source.astype(jnp.float32)
    squares = jnp.mean(values * values, axis=-1, keepdims=True)
    return jax.nn.silu(values * lax.rsqrt(squares + 1e-06) * gain_vector).astype(jnp.bfloat16)


def pad_rows(source):
    return jnp.pad(source, ((0, 0), (1, 1), (0, 0), (0, 0)))


def shards(
    hidden,
    modulation,
    time_embed,
    head_weight,
    head_bias,
    noisy,
    step_size,
    latent_mean,
    latent_std,
    in_weight,
    in_bias,
    norm_gain,
    conv_weight,
    conv_bias,
):
    frames, height, columns, lat_channels = noisy.shape
    sections = lax.axis_size("section")
    half_channels = in_weight.shape[2]
    values = hidden.astype(jnp.float32)
    row_sums, square_sums = lax.psum(
        (jnp.sum(values, axis=1), jnp.sum(values * values, axis=1)), "tp"
    )
    average = row_sums / D
    variance = square_sums / D - average * average
    shift_term = modulation[0] + time_embed
    scale_term = modulation[1] + time_embed
    modulated = (
        (values - average[:, None]) * lax.rsqrt(variance[:, None] + 1e-06) * (1.0 + scale_term)
        + shift_term
    ).astype(jnp.bfloat16)
    partial_sum = jnp.dot(modulated, head_weight, preferred_element_type=jnp.float32)
    velocity = (lax.psum(partial_sum, "tp") + head_bias).astype(jnp.bfloat16)
    band_rows = velocity.shape[0] * 2 // (columns * sections)
    outgoing = velocity.reshape(band_rows, sections, -1)
    arrived = lax.all_to_all(outgoing, "section", split_axis=1, concat_axis=0, tiled=True)
    latent_field = arrived.reshape(frames, height // 2, columns // 2, 2, 2, lat_channels)
    latent_field = jnp.transpose(latent_field, (0, 1, 3, 2, 4, 5)).reshape(
        frames, height, columns, lat_channels
    )
    latent = (
        (noisy.astype(jnp.float32) - step_size[0] * latent_field.astype(jnp.float32)) * latent_std
        + latent_mean
    ).astype(jnp.bfloat16)
    latent_wide = padded_2(latent, (("section", 2),), 2)
    earlier = passed_along(latent_wide, "sp", 1)
    stacked = pad_rows(jnp.concatenate([earlier, latent_wide], axis=0))
    extended = (conv_taps(stacked, in_weight, frames + 2, height, columns + 2) + in_bias).astype(
        jnp.bfloat16
    )
    extended = extended.reshape(frames + 2, height, columns + 2, half_channels)
    upblock_half = extended[2:, :, 1 : columns + 1]
    extended_full = lax.all_gather(extended, "tp", axis=3, tiled=True)
    normed = activate(extended_full, norm_gain)
    frame_index = lax.axis_index("sp") * frames - 2 + jnp.arange(frames + 2, dtype=jnp.int32)
    column_index = (
        lax.axis_index("section") * columns - 1 + jnp.arange(columns + 2, dtype=jnp.int32)
    )
    inside_cols = (column_index >= 0) & (column_index < columns * sections)
    inside = (frame_index >= 0)[:, None, None, None] & inside_cols[None, None, :, None]
    conv_input = pad_rows(jnp.where(inside, normed, jnp.zeros_like(normed)))
    full_weight = lax.all_gather(conv_weight, "section", axis=1, tiled=True)
    mixed = conv_taps(conv_input, full_weight, frames, height, columns)
    decoded = (
        upblock_half.astype(jnp.float32).reshape(-1, half_channels) + mixed + conv_bias
    ).astype(jnp.bfloat16)
    return decoded.reshape(frames, height, columns, half_channels)


def iota(shape, dim):
    return lax.broadcasted_iota(jnp.int32, shape, dim)


def dot(left, right):
    return jnp.dot(left, right, preferred_element_type=jnp.float32)


def dot_rows(left, right):
    return lax.dot_general(
        left, right, (((1,), (1,)), ((), ())), preferred_element_type=jnp.float32
    )


def pieces(value):
    high = value.astype(jnp.bfloat16)
    rest = value - high.astype(jnp.float32)
    middle = rest.astype(jnp.bfloat16)
    low = (rest - middle.astype(jnp.float32)).astype(jnp.bfloat16)
    return high.astype(jnp.float32), middle.astype(jnp.float32), low.astype(jnp.float32)


def block_kernel(
    sizes,
    modulation_far,
    time_far,
    head_bias_far,
    noisy_far,
    step_size,
    std_far,
    mean_far,
    in_bias_far,
    gain_far,
    conv_bias_far,
    hidden_far,
    head_far,
    in_far,
    conv_far,
    out,
    modulation,
    time_embed,
    head_bias,
    noisy,
    latent_std,
    latent_mean,
    in_bias,
    norm_gain,
    conv_bias,
    hidden,
    head_weight,
    in_weight,
    weight,
    swap,
    noise_pick,
    noise_mask,
    places,
    part,
    peer_part,
    peer_weight,
    peer_bias,
    fields,
    noise_lines,
    expanded,
    stacked,
    taps_in,
    ups,
    squares,
    wide,
    send_buf,
    recv_buf,
    held,
    acc,
    final,
    load_sems,
    pair_send,
    pair_recv,
    field_send,
    field_recv,
    sum_send,
    sum_recv,
):
    sections, clips_sp, frames, height, columns, lat, channels = sizes
    rows_i, cols_j = height // 2, columns * sections // 2
    width = columns * sections
    tokens = rows_i * cols_j
    near = frames + 2
    half = in_weight.shape[2]
    lanes = 4 * lat
    folded = tokens // 2
    line_size = 4 * 2 * lat
    sec, core, spi = lax.axis_index("section"), lax.axis_index("tp"), lax.axis_index("sp")
    nxt = lax.rem(spi + 1, clips_sp)
    prv = lax.rem(spi + clips_sp - 1, clips_sp)
    has_next, has_prev = spi + 1 < clips_sp, spi > 0
    peer = {"tp": 1 - core}

    lead = core == 1
    unit = jnp.where(core >= 0, 1.0, 0.0)
    barrier = pltpu.get_barrier_semaphore()
    pl.semaphore_signal(barrier, inc=1, device_id=peer)
    for k in range(1, sections):
        pl.semaphore_signal(
            barrier, inc=1, device_id={"section": lax.rem(sec + k, sections), "tp": 1}
        )

    @pl.when(has_prev)
    def _():
        for k in range(sections):
            pl.semaphore_signal(
                barrier,
                inc=1,
                device_id={"section": lax.rem(sec + k, sections), "sp": prv, "tp": 1},
            )


    groups = (
        ((hidden_far, hidden), (head_far, head_weight)),
        ((modulation_far, modulation), (time_far, time_embed)),
        (
            (noisy_far, noisy),
            (in_bias_far, in_bias),
            (head_bias_far, head_bias),
            (std_far, latent_std),
            (mean_far, latent_mean),
            (gain_far, norm_gain),
            (conv_bias_far, conv_bias),
        ),
        ((conv_far, weight),),
        ((in_far, in_weight),),
    )
    loads = [
        [pltpu.make_async_copy(source, target, load_sems.at[n]) for source, target in members]
        for n, members in enumerate(groups)
    ]
    for c in loads[1] + loads[0] + loads[2]:
        c.start()

    def pair_copy(n, source, target):
        return pltpu.make_async_remote_copy(
            source, target, pair_send.at[n], pair_recv.at[n], device_id=peer
        )

    def wait_rows(count, sem):
        view = ups.at[0, pl.ds(0, count), :]
        pltpu.make_async_copy(view, view, sem).wait()

    up_side = sec < sections // 2
    is_end = (sec == 0) | (sec == sections - 1)
    inner = jnp.logical_not(is_end)

    def mirrored(value):
        return jnp.where(up_side, value, sections - 1 - value)

    others = [mirrored(jnp.where(is_end, sections - 1 - n, (3, 2, 0)[n])) for n in range(3)]

    def spread_copy(z, ahead, c):
        slot = lax.rem(z - sec + sections, sections)
        return pltpu.make_async_remote_copy(
            fields.at[0, 0], fields.at[ahead, slot], field_send.at[0], field_recv.at[0],
            device_id={"section": z, "sp": nxt if ahead else spi, "tp": c},
        )

    def spread():
        for z in [*others, sec]:
            for c in (0, 1):
                if z is not sec:
                    spread_copy(z, 0, c).start()

                @pl.when(has_next)
                def _():
                    spread_copy(z, 1, c).start()

        pltpu.make_async_remote_copy(
            fields.at[0, 0], fields.at[0, 0], field_send.at[0], field_recv.at[0], device_id=peer
        ).start()

    field_rows = 2 * folded * 2 * lanes * 2 // 512

    to, at = iota((tokens, tokens), 0), iota((tokens, tokens), 1)
    swap[...] = (lax.rem(to, rows_i) * cols_j + lax.div(to, rows_i) == at).astype(jnp.bfloat16)
    cells = frames * height * columns
    group = frames // 2
    r_line, r_col = lax.div(iota((cells, 2 * lanes), 0), columns), lax.rem(
        iota((cells, 2 * lanes), 0), columns
    )
    r_slot = lax.div(lax.div(r_line, height), group) * 4 + lax.rem(r_line, 2) * 2 + lax.rem(r_col, 2)
    noise_mask[...] = (lax.div(iota((cells, 2 * lanes), 1), lat) == r_slot).astype(jnp.float32)
    packed = cells // 8
    r_at, r_to = iota((packed, cells), 1), iota((packed, cells), 0)
    r_line, r_col = lax.div(r_at, columns), lax.rem(r_at, columns)
    r_home = (
        lax.rem(lax.div(r_line, height), group) * (columns // 2) + lax.div(r_col, 2)
    ) * rows_i + lax.div(lax.rem(r_line, height), 2)
    noise_pick[...] = (r_to == r_home).astype(jnp.bfloat16)
    shape = (2 * lanes, 2 * line_size)
    src, dst = iota(shape, 0), iota(shape, 1)
    same = lax.div(src, lanes) == lax.div(dst, line_size)
    src, dst = lax.rem(src, lanes), lax.rem(dst, line_size)
    places[0 * shape[0] : (0 + 1) * shape[0]] = (same & (src == dst + 2 * lat) & (dst < 2 * lat)).astype(jnp.bfloat16)
    places[1 * shape[0] : (1 + 1) * shape[0]] = (same & (src + 2 * lat == dst)).astype(jnp.bfloat16)
    places[2 * shape[0] : (2 + 1) * shape[0]] = (same & (src + 6 * lat == dst) & (dst >= 6 * lat)).astype(jnp.bfloat16)
    expanded[...] = jnp.zeros_like(expanded)
    taps_in[...] = jnp.zeros_like(taps_in)
    wide[0] = jnp.zeros_like(wide[0])
    wide[width + 1] = jnp.zeros_like(wide[0])

    @pl.when(jnp.logical_not(has_prev))
    def _():
        fields[1] = jnp.zeros_like(fields[1])

    features = hidden.shape[1]
    for c in loads[1]:
        c.wait()
    scale = 1.0 + (modulation[1:2, :] + time_embed[...])
    shift = modulation[0:1, :] + time_embed[...]
    row = iota((8, features), 0)
    lines = jnp.zeros((8, features), jnp.float32)
    for n, piece in enumerate(pieces(scale) + pieces(shift)):
        lines = jnp.where(row == n, piece, lines)
    lines = jnp.concatenate([lines, jnp.zeros_like(lines)], axis=0).astype(jnp.bfloat16)
    for c in loads[0]:
        c.wait()
    loads[4][0].start()
    loads[3][0].start()
    values = hidden[...].astype(jnp.float32)
    own_sum = jnp.sum(values, axis=1, keepdims=True)
    own_square = jnp.sum(values * values, axis=1, keepdims=True)
    center = own_sum / features
    centred = ((values - center) * scale).astype(jnp.bfloat16)
    stack = jnp.concatenate([centred, lines], axis=0)
    cut = features // 2
    made = dot_rows(stack[:, :cut], head_weight[:, :cut])
    made = made + dot_rows(stack[:, cut:], head_weight[:, cut:]) * unit
    part[:tokens, :lanes] = made[:tokens]
    stat_shape = (tokens, 128 - lanes)
    part[:tokens, lanes:] = jnp.where(
        iota(stat_shape, 1) < stat_shape[1] // 2, own_sum, own_square
    )
    made = made[tokens:]
    line = iota(made.shape, 0)
    own_scale = jnp.sum(jnp.where(line < 3, made, 0.0), axis=0, keepdims=True)
    own_shift = jnp.sum(jnp.where(line < 3, 0.0, made), axis=0, keepdims=True)
    part[tokens:, :lanes] = jnp.where(iota((8, lanes), 0) == 0, own_scale, own_shift)
    part[tokens:, lanes:] = jnp.zeros((8, 128 - lanes), jnp.float32)
    pair = pair_copy(0, part, peer_part)
    early = [pair_copy(1, in_weight, peer_weight), pair_copy(2, in_bias, peer_bias)]
    for c in loads[2]:
        c.wait()
    std = jnp.concatenate([latent_std[...]] * 8, axis=1)
    mean_latent = jnp.concatenate([latent_mean[...]] * 8, axis=1)

    @pl.when(core == 0)
    def _():
        pl.semaphore_wait(barrier, 1)
        pair.start()
        loads[4][0].wait()
        for c in early:
            c.start()

    @pl.when(lead)
    def _():
        src, dst = iota((lat, 2 * lanes), 0), iota((lat, 2 * lanes), 1)
        tiled = dot(noisy[...], (src == lax.rem(dst, lat)).astype(jnp.bfloat16))
        tiled = (tiled * noise_mask[...]).astype(jnp.bfloat16)
        fields[0, 0, 1] = dot(noise_pick[...], tiled).astype(jnp.bfloat16)
        pair.wait_recv()
        far_sum = peer_part[:tokens, lanes : lanes + 1]
        far_square = peer_part[
            :tokens, lanes + (128 - lanes) // 2 : lanes + (128 - lanes) // 2 + 1
        ]
        average = (own_sum + far_sum) / D
        variance = (own_square + far_square) / D - average * average
        body = (
            part[:tokens, :lanes]
            + peer_part[:tokens, :lanes]
            - (average - center) * own_scale
            - (average - far_sum / features) * peer_part[tokens : tokens + 1, :lanes]
        )
        velocity = (
            lax.rsqrt(variance + 1e-06) * body
            + (own_shift + peer_part[tokens + 1 : tokens + 2, :lanes])
            + head_bias[...]
        ).astype(jnp.bfloat16)
        field = dot(swap[...], velocity)
        fields[0, 0, 0] = jnp.concatenate([field[:folded], field[folded:]], axis=1).astype(
            jnp.bfloat16
        )
        pl.semaphore_wait(
            barrier, 2 * sections - 1 + jnp.where(has_next, 2 * sections, 0)
        )
        spread()
        loads[4][0].wait()
        for c in early:
            c.start()

    for c in early:
        c.wait_recv()
    for q in range(2):
        for e in range(3):
            col = q + e
            step_j, odd = (col + 1) // 2 - q, (col + 1) % 2
            for a in range(3):
                for b in range(3):
                    tap = 9 * a + 3 * b + e
                    for p in range(2):
                        first = step_j * 3 * line_size + a * line_size + (p + b) * 2 * lat + odd * lat
                        left = p * 2 * half
                        taps_in[q, first : first + lat, left : left + half] = in_weight[tap]
                        taps_in[q, first : first + lat, left + half : left + 2 * half] = peer_weight[tap]

    for on_lead in (True, False):
        for first in (True, False):

            @pl.when((lead == on_lead) & (has_prev != first))
            def _():
                count = sections - 1 + (0 if first else sections) + (0 if on_lead else 1)
                wait_rows(count * field_rows, field_recv.at[0])

    lane = iota((folded, 2 * lanes), 1)
    side = folded // 2
    for slot in (1, 0):
        got = [
            fields[slot, lax.rem(sec + sections - g, sections), 1].astype(jnp.float32)
            for g in range(sections)
        ]
        for f in range(frames):
            r = f % group
            low, high = (
                jnp.concatenate(
                    [got[g][r * side : (r + 1) * side] for g in (2 * t, 2 * t + 1)], axis=0
                )
                for t in range(2)
            )
            if f < group:
                high = pltpu.roll(high, lanes, 1)
            else:
                low = pltpu.roll(low, lanes, 1)
            at_f = ((1 - slot) * frames + f) * folded
            noise_lines[at_f : at_f + folded, :] = jnp.where(lane < lanes, low, high)

    lines_f = jnp.concatenate(
        [
            fields[slot, lax.rem(sec + sections - f, sections), 0]
            for slot in (1, 0)
            for f in range(frames)
        ],
        axis=0,
    ).astype(jnp.float32)
    lines_f = ((noise_lines[...] - step_size[0] * lines_f) * std + mean_latent).astype(
        jnp.bfloat16
    ).astype(jnp.float32)
    count = 2 * frames * folded
    f_row = iota((count, 2 * lanes), 0)
    i_row = lax.rem(f_row, rows_i)
    lines_f = jnp.where((f_row >= frames * folded) | has_prev, lines_f, 0.0)
    before = jnp.where(i_row == 0, 0.0, pltpu.roll(lines_f, 1, 0))
    after = jnp.where(i_row == rows_i - 1, 0.0, pltpu.roll(lines_f, count - 1, 0))
    shifted = jnp.concatenate([before, lines_f, after], axis=1).astype(jnp.bfloat16)
    line_values = jnp.concatenate(
        [
            dot(shifted[n * count // 2 : (n + 1) * count // 2], places[...])
            for n in range(2)
        ],
        axis=0,
    )
    half_j = cols_j // 2
    for f in range(2 * frames):
        for side in range(2):
            expanded[1 + side * half_j : 1 + (side + 1) * half_j, f] = line_values[
                f * folded : (f + 1) * folded, side * line_size : (side + 1) * line_size
            ].reshape(half_j, rows_i, line_size)
    block = near * rows_i
    for j in range(cols_j + 2):
        for a in range(3):
            stacked[j * block : (j + 1) * block, a * line_size : (a + 1) * line_size] = (
                expanded[j, a : a + near].reshape(block, line_size).astype(jnp.bfloat16)
            )
    dests = [
        jnp.where(is_end, mirrored(sections - 1), 0),
        jnp.where(is_end, mirrored(sections - 2), sections - 1),
        mirrored(jnp.where(is_end, 1, sections - 2)),
    ]
    parts = half // channels
    tall = near * height

    def upblock(homes):
        for q in range(2):
            lhs = jnp.concatenate(
                [
                    jnp.concatenate(
                        [
                            stacked[pl.ds(pl.multiple_of((j + q + n) * block, block), block), :]
                            for n in range(2)
                        ],
                        axis=1,
                    )
                    for j in homes
                ],
                axis=0,
            )
            for p in range(2):
                total = jnp.zeros((len(homes) * block, channels), jnp.float32)
                for h in range(2):
                    left = (p * 2 + h) * half
                    bias = in_bias[...] if h == 0 else peer_bias[...]
                    up = dot(lhs, taps_in[q, :, left : left + half]) + bias
                    up = up.astype(jnp.bfloat16).astype(jnp.float32)
                    for n in range(parts):
                        chunk = up[:, n * channels : (n + 1) * channels]
                        total = total + chunk * chunk
                    for m, j in enumerate(homes):
                        at_j = pl.ds(pl.multiple_of(2 * j * tall, tall) + q * tall + p, block, stride=2)
                        for n in range(parts):
                            ups[h * parts + n, at_j, :] = up[
                                m * block : (m + 1) * block, n * channels : (n + 1) * channels
                            ]
                for m, j in enumerate(homes):
                    at_j = pl.ds(pl.multiple_of(2 * j * tall, tall) + q * tall + p, block, stride=2)
                    squares[at_j, :] = total[m * block : (m + 1) * block]

    edge_high = dests[0] > 0
    first_home = jnp.where(edge_high, cols_j - 2, 0)
    upblock([first_home, first_home + 1])

    mine = lax.rem(sec + parts * core, 2 * parts)
    gain = norm_gain[pl.ds(sec, 1), :]
    h_row = lax.rem(iota((tall, channels), 0), height)
    valid = has_prev | (iota((tall, channels), 0) >= 2 * height)

    def normalise(w):
        at_w = pl.ds(pl.multiple_of(w * tall, tall), tall)
        mean = jnp.sum(squares[at_w, :], axis=1, keepdims=True) / (2 * half)
        v = ups[mine, at_w, :] * lax.rsqrt(mean + 1e-06) * gain
        v = jnp.where(valid, v / (1.0 + jnp.exp(-v)), 0.0)
        above = jnp.where(h_row == 0, 0.0, pltpu.roll(v, 1, 0))
        below = jnp.where(h_row == height - 1, 0.0, pltpu.roll(v, tall - 1, 0))
        for b, line_v in enumerate((above, v, below)):
            wide[w + 1, :, b * channels : (b + 1) * channels] = line_v.astype(jnp.bfloat16)

    span = frames * height
    pair_columns = columns // 2

    def partial(d, first_column, count):
        windows, taps = [], []
        for a in range(3):
            for e in range(3):
                window = wide[
                    pl.ds(d * columns + e + first_column, count),
                    a * height : a * height + span,
                    :,
                ]
                windows.append(window.reshape(count * span, 3 * channels))
                taps += [weight[9 * a + 3 * b + e] for b in range(3)]
        low, high = (
            dot(
                jnp.concatenate(windows[first:last], axis=1),
                jnp.concatenate(taps[3 * first : 3 * last], axis=0),
            )
            for first, last in ((0, 5), (5, 9))
        )
        value = low + high * unit
        return [value[w * span : (w + 1) * span] for w in range(count)]

    neighbour = mirrored(1)
    targets = [jnp.where(is_end, neighbour, d) for d in dests]
    far_n = jnp.where(up_side, 1, 0)
    slots = [
        jnp.where(is_end, 2, 1 - far_n),
        jnp.where(is_end, 3, far_n),
        jnp.where(is_end, 0, 1),
    ]
    direct = [is_end | up_side, is_end | jnp.logical_not(up_side), is_end]

    marks = [jnp.where(slot < 2, slot, 2 + (slot - 2) * columns) for slot in slots]
    weights = [jnp.where(slot < 2, 0, 1) for slot in slots]

    def sum_copy(n, w):
        return pltpu.make_async_remote_copy(
            send_buf.at[n, w], recv_buf.at[slots[n], w], sum_send.at[0],
            sum_recv.at[marks[n] + w * weights[n]], device_id={"section": targets[n]},
        )

    def far_copy(w):
        return pltpu.make_async_remote_copy(
            send_buf.at[far_n, w], recv_buf.at[1, w], sum_send.at[0], sum_recv.at[1],
            device_id={"section": mirrored(sections - 1)},
        )

    def relay_far(side, *pieces_w):
        @pl.when(inner & (up_side if side else jnp.logical_not(up_side)))
        def _():
            for n in pieces_w:
                w = jnp.where(up_side, (2, 3, 1, 0)[n], n)
                send_buf[far_n, w] = (held[far_n, w] + arrived(2, w)).astype(jnp.bfloat16)
                far_copy(w).start()

    def arrived(slot, w):
        pltpu.make_async_copy(
            recv_buf.at[slot, w], recv_buf.at[slot, w], sum_recv.at[2 + (slot - 2) * columns + w]
        ).wait()
        return recv_buf[slot, w].astype(jnp.float32)

    for t in range(4):
        normalise(2 * first_home + t)

    later = [4, *range(width - 1, width - 2 - columns, -1), *range(5, width - 1 - columns)]

    def normalise_next(numbers):
        for n in numbers:
            inward = jnp.where(edge_high, width - 5 - n, 4 + n)
            normalise(jnp.where(is_end, inward, later[n]))

    loads[3][0].wait()
    def hold(n, first_column, count):
        for c, value in enumerate(partial(dests[n], first_column, count)):
            send_buf[n, first_column + c] = value.astype(jnp.bfloat16)
            held[n, first_column + c] = value

    def send(n, pieces_w):
        @pl.when(direct[n])
        def _():
            for w in pieces_w:
                sum_copy(n, w).start()

    first_pair = jnp.where(edge_high, columns - 2, 0)
    third, fourth = jnp.where(edge_high, 1, 2), jnp.where(edge_high, 0, 3)
    hold(0, first_pair, 2)
    send(0, (first_pair, first_pair + 1))
    hold(0, third, 1)
    send(0, (third,))
    upblock([lax.rem(first_home + 2 + n, cols_j) for n in range(cols_j - 2)])
    normalise_next((0,))
    hold(0, fourth, 1)
    send(0, (fourth,))
    normalise_next(range(1, columns + 2))
    relay_far(False, 0)
    for m in (1, 0):
        hold(1, m * pair_columns, pair_columns)
        send(1, range(m * pair_columns, (m + 1) * pair_columns))
        if m == 1:
            relay_far(True, 0)
    relay_far(False, 1)
    normalise_next(range(columns + 2, width - 4))
    relay_far(False, 2)
    relay_far(True, 1)
    for m in range(2):
        hold(2, m * pair_columns, pair_columns)
    send(2, range(columns))
    relay_far(False, 3)
    relay_far(True, 2)

    for m in range(2):
        values = partial(sec, m * pair_columns, pair_columns)
        residual = []
        for w in range(pair_columns):
            first = pl.multiple_of(
                (sec * columns + m * pair_columns + w) * tall + 2 * height, height
            )
            residual.append(
                jnp.concatenate([ups[n, pl.ds(first, span), :] for n in range(parts)], axis=1)
            )
        for w, own in enumerate(values):
            acc[m * pair_columns + w] = own + conv_bias[...] + residual[w]

    relay_far(True, 3)

    @pl.when(inner)
    def _():
        for w in (2, 3, 0, 1):
            send_buf[2, w] = (held[2, w] + arrived(3, w)).astype(jnp.bfloat16)
            sum_copy(2, w).start()


    slot_rows = columns * span * half * 2 // 512

    def finish(first, last):
        wait_rows(slot_rows, sum_recv.at[first])
        for w in range(columns):
            acc[w] = acc[w] + recv_buf[first, w].astype(jnp.float32)
        wait_rows(slot_rows, sum_recv.at[last])
        for w in range(columns):
            total = acc[w] + recv_buf[last, w].astype(jnp.float32)
            for c in range(parts):
                final[c, pl.ds(w, span, stride=columns), :] = total[
                    :, c * channels : (c + 1) * channels
                ]


    @pl.when(is_end)
    def _():
        finish(0, 1)

    @pl.when(inner)
    def _():
        finish(1, 0)

    for n in range(parts):
        out[:, n * channels : (n + 1) * channels] = final[n].astype(out.dtype)
    wait_rows(3 * columns * span * half * 2 // 512, sum_send.at[0])
    for c in early:
        c.wait_send()

    @pl.when(core == 0)
    def _():
        pair.wait_send()

    for first in (True, False):

        @pl.when(lead & (has_next != first))
        def _():
            count = 2 * (sections - 1) + (0 if first else 2 * sections) + 1
            wait_rows(count * field_rows, field_send.at[0])


def fused_shards(sizes, *arrays):
    (
        hidden, modulation, time_embed, head_weight, head_bias, noisy, step_size, latent_mean,
        latent_std, in_weight, in_bias, norm_gain, conv_weight, conv_bias,
    ) = arrays
    sections, clips_sp, frames, height, columns, lat, channels = sizes
    rows_i, cols_j, half = height // 2, columns * sections // 2, in_weight.shape[2]
    width, near, tokens, lanes = columns * sections, frames + 2, hidden.shape[0], 4 * lat
    line_size = 8 * lat
    f32, bf16 = jnp.float32, jnp.bfloat16
    vmem, dma = pltpu.VMEM, pltpu.SemaphoreType.DMA
    rows = columns * frames * height
    operands = (
        modulation, time_embed[None], head_bias[None], noisy.reshape(-1, lat),
        latent_std[None], latent_mean[None], in_bias[None], norm_gain.reshape(-1, channels),
        conv_bias[None], hidden, head_weight.T, in_weight, conv_weight,
    )
    operands = [pltpu.with_memory_space_constraint(value, pltpu.HBM) for value in operands]
    far = pl.BlockSpec(memory_space=pltpu.HBM)
    out = pl.pallas_call(
        functools.partial(block_kernel, sizes),
        out_shape=pltpu.VMEM((rows, half), bf16),
        in_specs=[far] * 4
        + [pl.BlockSpec(memory_space=pltpu.SMEM)]
        + [far] * (len(operands) - 4),
        out_specs=pl.BlockSpec(memory_space=pltpu.VMEM),
        scratch_shapes=[vmem(value.shape, value.dtype) for value in operands]
        + [
            vmem((tokens, tokens), bf16),
            vmem((rows // 8, rows), bf16),
            vmem((rows, 2 * lanes), f32),
            vmem((6 * lanes, 2 * line_size), bf16),
            vmem((tokens + 8, 128), f32),
            vmem((tokens + 8, 128), f32),
            vmem(in_weight.shape, bf16),
            vmem((1, half), f32),
            vmem((2, sections, 2, tokens // 2, 2 * lanes), bf16),
            vmem((2 * frames * tokens // 2, 2 * lanes), f32),
            vmem((cols_j + 2, 2 * frames, rows_i, line_size), f32),
            vmem(((cols_j + 2) * near * rows_i, 3 * line_size), bf16),
            vmem((2, 6 * line_size, 4 * half), bf16),
            vmem((2 * half // channels, width * near * height, channels), f32),
            vmem((width * near * height, channels), f32),
            vmem((width + 2, near * height, 3 * channels), bf16),
            vmem((3, columns, rows // columns, half), bf16),
            vmem((4, columns, rows // columns, half), bf16),
            vmem((3, columns, rows // columns, half), f32),
            vmem((columns, rows // columns, half), f32),
            vmem((half // channels, rows, channels), f32),
            dma((5,)),
            dma((3,)),
            dma((3,)),
            dma((1,)),
            dma((1,)),
            dma((1,)),
            dma((2 + 2 * columns,)),
        ],
        compiler_params=pltpu.CompilerParams(
            collective_id=0, has_side_effects=True, vmem_limit_bytes=40 * 2**20
        ),
    )(*operands[:4], step_size, *operands[4:])
    return out.reshape(frames, height, columns, half)


def dispatch(*arrays):
    hidden, noisy, in_weight, conv_weight = arrays[0], arrays[5], arrays[9], arrays[12]
    frames, height, columns, lat = noisy.shape
    sections, cores, clips_sp = (lax.axis_size(axis) for axis in ("section", "tp", "sp"))
    channels, half = conv_weight.shape[1:]
    whole_frame = hidden.shape[0] == height // 2 * (columns * sections // 2)
    if (
        whole_frame
        and cores == 2
        and clips_sp > 1
        and frames == sections
        and sections == 4
        and columns == 4
        and channels % 128 == 0
        and half % channels == 0
        and lat == 16
        and height == 16
    ):
        sizes = (sections, clips_sp, frames, height, columns, lat, channels)
        return fused_shards(sizes, *arrays)
    return shards(*arrays)


def solution(mesh):
    placed = (
        P(("groups", "sp", "section"), "tp"),
        P(None, "tp"),
        P(("groups", "tp")),
        P("tp", None),
        P(),
        P(("groups", "sp"), None, "section", None),
        P("groups"),
        P(),
        P(),
        P(None, None, "tp"),
        P("tp"),
        P(),
        P(None, "section", "tp"),
        P("tp"),
    )
    return jax.shard_map(
        dispatch,
        mesh=mesh,
        in_specs=placed,
        out_specs=P(("groups", "sp"), None, "section", "tp"),
        check_vma=False,
    )
```

```python
import functools

import jax
import jax.numpy as jnp
from jax import lax
from jax.experimental import pallas as pl
from jax.experimental.pallas import tpu as pltpu
from jax.sharding import PartitionSpec as P

D = 6144


def padded_2(value, sides, width):
    for axis, dim in sides:
        count, length = (lax.axis_size(axis), value.shape[dim])
        up = [(i, (i + 1) % count) for i in range(count - 1)]
        down = [(j, i) for i, j in up]
        last = lax.slice_in_dim(value, length - width, length, axis=dim)
        leading = lax.slice_in_dim(value, 0, width, axis=dim)
        before = lax.ppermute(last, axis, up)
        after = lax.ppermute(leading, axis, down)
        value = jnp.concatenate([before, value, after], axis=dim)
    return value


def passed_along(value, axis, by):
    count = lax.axis_size(axis)
    pairs = [(i, i + by) for i in range(count) if 0 <= i + by < count]
    return lax.ppermute(value, axis, pairs)


def conv_taps(padded, weight, frames, height, columns):
    channels = padded.shape[3]
    result = jnp.zeros((frames * height * columns, weight.shape[2]), jnp.float32)
    for offset_time in range(3):
        for offset_row in range(3):
            slab = padded[offset_time : offset_time + frames, offset_row : offset_row + height]
            window = jnp.concatenate(
                [slab[:, :, 0:columns], slab[:, :, 1 : columns + 1], slab[:, :, 2 : columns + 2]],
                axis=3,
            )
            first = 9 * offset_time + 3 * offset_row
            taps = weight[first : first + 3].reshape(3 * channels, weight.shape[2])
            result = result + jnp.dot(
                window.reshape(-1, 3 * channels), taps, preferred_element_type=jnp.float32
            )
    return result


def activate(source, gain_vector):
    values = source.astype(jnp.float32)
    squares = jnp.mean(values * values, axis=-1, keepdims=True)
    return jax.nn.silu(values * lax.rsqrt(squares + 1e-06) * gain_vector).astype(jnp.bfloat16)


def pad_rows(source):
    return jnp.pad(source, ((0, 0), (1, 1), (0, 0), (0, 0)))


def shards(
    hidden,
    modulation,
    time_embed,
    head_weight,
    head_bias,
    noisy,
    step_size,
    latent_mean,
    latent_std,
    in_weight,
    in_bias,
    norm_gain,
    conv_weight,
    conv_bias,
):
    frames, height, columns, lat_channels = noisy.shape
    sections = lax.axis_size("section")
    half_channels = in_weight.shape[2]
    values = hidden.astype(jnp.float32)
    row_sums, square_sums = lax.psum(
        (jnp.sum(values, axis=1), jnp.sum(values * values, axis=1)), "tp"
    )
    average = row_sums / D
    variance = square_sums / D - average * average
    shift_term = modulation[0] + time_embed
    scale_term = modulation[1] + time_embed
    modulated = (
        (values - average[:, None]) * lax.rsqrt(variance[:, None] + 1e-06) * (1.0 + scale_term)
        + shift_term
    ).astype(jnp.bfloat16)
    partial_sum = jnp.dot(modulated, head_weight, preferred_element_type=jnp.float32)
    velocity = (lax.psum(partial_sum, "tp") + head_bias).astype(jnp.bfloat16)
    band_rows = velocity.shape[0] * 2 // (columns * sections)
    outgoing = velocity.reshape(band_rows, sections, -1)
    arrived = lax.all_to_all(outgoing, "section", split_axis=1, concat_axis=0, tiled=True)
    latent_field = arrived.reshape(frames, height // 2, columns // 2, 2, 2, lat_channels)
    latent_field = jnp.transpose(latent_field, (0, 1, 3, 2, 4, 5)).reshape(
        frames, height, columns, lat_channels
    )
    latent = (
        (noisy.astype(jnp.float32) - step_size[0] * latent_field.astype(jnp.float32)) * latent_std
        + latent_mean
    ).astype(jnp.bfloat16)
    latent_wide = padded_2(latent, (("section", 2),), 2)
    earlier = passed_along(latent_wide, "sp", 1)
    stacked = pad_rows(jnp.concatenate([earlier, latent_wide], axis=0))
    extended = (conv_taps(stacked, in_weight, frames + 2, height, columns + 2) + in_bias).astype(
        jnp.bfloat16
    )
    extended = extended.reshape(frames + 2, height, columns + 2, half_channels)
    upblock_half = extended[2:, :, 1 : columns + 1]
    extended_full = lax.all_gather(extended, "tp", axis=3, tiled=True)
    normed = activate(extended_full, norm_gain)
    frame_index = lax.axis_index("sp") * frames - 2 + jnp.arange(frames + 2, dtype=jnp.int32)
    column_index = (
        lax.axis_index("section") * columns - 1 + jnp.arange(columns + 2, dtype=jnp.int32)
    )
    inside_cols = (column_index >= 0) & (column_index < columns * sections)
    inside = (frame_index >= 0)[:, None, None, None] & inside_cols[None, None, :, None]
    conv_input = pad_rows(jnp.where(inside, normed, jnp.zeros_like(normed)))
    full_weight = lax.all_gather(conv_weight, "section", axis=1, tiled=True)
    mixed = conv_taps(conv_input, full_weight, frames, height, columns)
    decoded = (
        upblock_half.astype(jnp.float32).reshape(-1, half_channels) + mixed + conv_bias
    ).astype(jnp.bfloat16)
    return decoded.reshape(frames, height, columns, half_channels)


def iota(shape, dim):
    return lax.broadcasted_iota(jnp.int32, shape, dim)


def dot(left, right):
    return jnp.dot(left, right, preferred_element_type=jnp.float32)


def dot_rows(left, right):
    return lax.dot_general(
        left, right, (((1,), (1,)), ((), ())), preferred_element_type=jnp.float32
    )


def pieces(value):
    high = value.astype(jnp.bfloat16)
    rest = value - high.astype(jnp.float32)
    middle = rest.astype(jnp.bfloat16)
    low = (rest - middle.astype(jnp.float32)).astype(jnp.bfloat16)
    return high.astype(jnp.float32), middle.astype(jnp.float32), low.astype(jnp.float32)


def block_kernel(
    sizes,
    modulation_far,
    time_far,
    head_bias_far,
    noisy_far,
    step_size,
    std_far,
    mean_far,
    in_bias_far,
    gain_far,
    conv_bias_far,
    hidden_far,
    head_far,
    in_far,
    conv_far,
    out,
    modulation,
    time_embed,
    head_bias,
    noisy,
    latent_std,
    latent_mean,
    in_bias,
    norm_gain,
    conv_bias,
    hidden,
    head_weight,
    in_weight,
    weight,
    swap,
    noise_pick,
    noise_mask,
    places,
    part,
    peer_part,
    peer_weight,
    peer_bias,
    fields,
    noise_lines,
    expanded,
    stacked,
    taps_in,
    ups,
    squares,
    wide,
    send_buf,
    recv_buf,
    held,
    acc,
    final,
    load_sems,
    pair_send,
    pair_recv,
    field_send,
    field_recv,
    sum_send,
    sum_recv,
):
    sections, clips_sp, frames, height, columns, lat, channels = sizes
    rows_i, cols_j = height // 2, columns * sections // 2
    width = columns * sections
    tokens = rows_i * cols_j
    near = frames + 2
    half = in_weight.shape[2]
    lanes = 4 * lat
    folded = tokens // 2
    line_size = 4 * 2 * lat
    sec, core, spi = lax.axis_index("section"), lax.axis_index("tp"), lax.axis_index("sp")
    nxt = lax.rem(spi + 1, clips_sp)
    prv = lax.rem(spi + clips_sp - 1, clips_sp)
    has_next, has_prev = spi + 1 < clips_sp, spi > 0
    peer = {"tp": 1 - core}

    lead = core == 1
    unit = jnp.where(core >= 0, 1.0, 0.0)
    groups = (
        ((hidden_far, hidden), (head_far, head_weight)),
        ((modulation_far, modulation), (time_far, time_embed)),
        (
            (noisy_far, noisy),
            (in_bias_far, in_bias),
            (head_bias_far, head_bias),
            (std_far, latent_std),
            (mean_far, latent_mean),
            (gain_far, norm_gain),
            (conv_bias_far, conv_bias),
        ),
        ((conv_far, weight),),
        ((in_far, in_weight),),
    )
    loads = [
        [pltpu.make_async_copy(source, target, load_sems.at[n]) for source, target in members]
        for n, members in enumerate(groups)
    ]
    for c in loads[1] + loads[0]:
        c.start()

    barrier = pltpu.get_barrier_semaphore()
    pl.semaphore_signal(barrier, inc=1, device_id=peer)
    for k in range(1, sections):
        pl.semaphore_signal(
            barrier, inc=1, device_id={"section": lax.rem(sec + k, sections), "tp": 1}
        )

    @pl.when(has_prev)
    def _():
        for k in range(sections):
            pl.semaphore_signal(
                barrier,
                inc=1,
                device_id={"section": lax.rem(sec + k, sections), "sp": prv, "tp": 1},
            )


    for c in loads[2]:
        c.start()

    def pair_copy(n, source, target):
        return pltpu.make_async_remote_copy(
            source, target, pair_send.at[n], pair_recv.at[n], device_id=peer
        )

    def wait_rows(count, sem):
        view = ups.at[0, pl.ds(0, count), :]
        pltpu.make_async_copy(view, view, sem).wait()

    up_side = sec < sections // 2
    is_end = (sec == 0) | (sec == sections - 1)
    inner = jnp.logical_not(is_end)

    def mirrored(value):
        return jnp.where(up_side, value, sections - 1 - value)

    others = [mirrored(jnp.where(is_end, sections - 1 - n, (3, 2, 0)[n])) for n in range(3)]

    def spread_copy(z, ahead, c):
        slot = lax.rem(z - sec + sections, sections)
        return pltpu.make_async_remote_copy(
            fields.at[0, 0], fields.at[ahead, slot], field_send.at[0], field_recv.at[0],
            device_id={"section": z, "sp": nxt if ahead else spi, "tp": c},
        )

    def spread():
        for z in [*others, sec]:
            for c in (0, 1):
                if z is not sec:
                    spread_copy(z, 0, c).start()

                @pl.when(has_next)
                def _():
                    spread_copy(z, 1, c).start()

        pltpu.make_async_remote_copy(
            fields.at[0, 0], fields.at[0, 0], field_send.at[0], field_recv.at[0], device_id=peer
        ).start()

    field_rows = 2 * folded * 2 * lanes * 2 // 512

    to, at = iota((tokens, tokens), 0), iota((tokens, tokens), 1)
    swap[...] = (lax.rem(to, rows_i) * cols_j + lax.div(to, rows_i) == at).astype(jnp.bfloat16)
    cells = frames * height * columns
    group = frames // 2
    r_line, r_col = lax.div(iota((cells, 2 * lanes), 0), columns), lax.rem(
        iota((cells, 2 * lanes), 0), columns
    )
    r_slot = lax.div(lax.div(r_line, height), group) * 4 + lax.rem(r_line, 2) * 2 + lax.rem(r_col, 2)
    noise_mask[...] = (lax.div(iota((cells, 2 * lanes), 1), lat) == r_slot).astype(jnp.float32)
    packed = cells // 8
    r_at, r_to = iota((packed, cells), 1), iota((packed, cells), 0)
    r_line, r_col = lax.div(r_at, columns), lax.rem(r_at, columns)
    r_home = (
        lax.rem(lax.div(r_line, height), group) * (columns // 2) + lax.div(r_col, 2)
    ) * rows_i + lax.div(lax.rem(r_line, height), 2)
    noise_pick[...] = (r_to == r_home).astype(jnp.bfloat16)
    shape = (2 * lanes, 2 * line_size)
    src, dst = iota(shape, 0), iota(shape, 1)
    same = lax.div(src, lanes) == lax.div(dst, line_size)
    src, dst = lax.rem(src, lanes), lax.rem(dst, line_size)
    places[0 * shape[0] : (0 + 1) * shape[0]] = (same & (src == dst + 2 * lat) & (dst < 2 * lat)).astype(jnp.bfloat16)
    places[1 * shape[0] : (1 + 1) * shape[0]] = (same & (src + 2 * lat == dst)).astype(jnp.bfloat16)
    places[2 * shape[0] : (2 + 1) * shape[0]] = (same & (src + 6 * lat == dst) & (dst >= 6 * lat)).astype(jnp.bfloat16)
    expanded[...] = jnp.zeros_like(expanded)
    taps_in[...] = jnp.zeros_like(taps_in)
    wide[0] = jnp.zeros_like(wide[0])
    wide[width + 1] = jnp.zeros_like(wide[0])

    @pl.when(jnp.logical_not(has_prev))
    def _():
        fields[1] = jnp.zeros_like(fields[1])

    features = hidden.shape[1]
    for c in loads[1]:
        c.wait()
    scale = 1.0 + (modulation[1:2, :] + time_embed[...])
    shift = modulation[0:1, :] + time_embed[...]
    row = iota((8, features), 0)
    lines = jnp.zeros((8, features), jnp.float32)
    for n, piece in enumerate(pieces(scale) + pieces(shift)):
        lines = jnp.where(row == n, piece, lines)
    lines = jnp.concatenate([lines, jnp.zeros_like(lines)], axis=0).astype(jnp.bfloat16)
    for c in loads[0]:
        c.wait()
    loads[4][0].start()
    loads[3][0].start()
    values = hidden[...].astype(jnp.float32)
    own_sum = jnp.sum(values, axis=1, keepdims=True)
    own_square = jnp.sum(values * values, axis=1, keepdims=True)
    center = own_sum / features
    centred = ((values - center) * scale).astype(jnp.bfloat16)
    stack = jnp.concatenate([centred, lines], axis=0)
    cut = features // 2
    made = dot_rows(stack[:, :cut], head_weight[:, :cut])
    made = made + dot_rows(stack[:, cut:], head_weight[:, cut:]) * unit
    part[:tokens, :lanes] = made[:tokens]
    stat_shape = (tokens, 128 - lanes)
    part[:tokens, lanes:] = jnp.where(
        iota(stat_shape, 1) < stat_shape[1] // 2, own_sum, own_square
    )
    made = made[tokens:]
    line = iota(made.shape, 0)
    own_scale = jnp.sum(jnp.where(line < 3, made, 0.0), axis=0, keepdims=True)
    own_shift = jnp.sum(jnp.where(line < 3, 0.0, made), axis=0, keepdims=True)
    part[tokens:, :lanes] = jnp.where(iota((8, lanes), 0) == 0, own_scale, own_shift)
    part[tokens:, lanes:] = jnp.zeros((8, 128 - lanes), jnp.float32)
    pair = pair_copy(0, part, peer_part)
    early = [pair_copy(1, in_weight, peer_weight), pair_copy(2, in_bias, peer_bias)]
    for c in loads[2]:
        c.wait()
    std = jnp.concatenate([latent_std[...]] * 8, axis=1)
    mean_latent = jnp.concatenate([latent_mean[...]] * 8, axis=1)

    @pl.when(core == 0)
    def _():
        pl.semaphore_wait(barrier, 1)
        pair.start()
        loads[4][0].wait()
        for c in early:
            c.start()

    @pl.when(lead)
    def _():
        src, dst = iota((lat, 2 * lanes), 0), iota((lat, 2 * lanes), 1)
        tiled = dot(noisy[...], (src == lax.rem(dst, lat)).astype(jnp.bfloat16))
        tiled = (tiled * noise_mask[...]).astype(jnp.bfloat16)
        fields[0, 0, 1] = dot(noise_pick[...], tiled).astype(jnp.bfloat16)
        pair.wait_recv()
        far_sum = peer_part[:tokens, lanes : lanes + 1]
        far_square = peer_part[
            :tokens, lanes + (128 - lanes) // 2 : lanes + (128 - lanes) // 2 + 1
        ]
        average = (own_sum + far_sum) / D
        variance = (own_square + far_square) / D - average * average
        body = (
            part[:tokens, :lanes]
            + peer_part[:tokens, :lanes]
            - (average - center) * own_scale
            - (average - far_sum / features) * peer_part[tokens : tokens + 1, :lanes]
        )
        velocity = (
            lax.rsqrt(variance + 1e-06) * body
            + (own_shift + peer_part[tokens + 1 : tokens + 2, :lanes])
            + head_bias[...]
        ).astype(jnp.bfloat16)
        field = dot(swap[...], velocity)
        fields[0, 0, 0] = jnp.concatenate([field[:folded], field[folded:]], axis=1).astype(
            jnp.bfloat16
        )
        pl.semaphore_wait(
            barrier, 2 * sections - 1 + jnp.where(has_next, 2 * sections, 0)
        )
        spread()
        loads[4][0].wait()
        for c in early:
            c.start()

    for c in early:
        c.wait_recv()
    for q in range(2):
        for e in range(3):
            col = q + e
            step_j, odd = (col + 1) // 2 - q, (col + 1) % 2
            for a in range(3):
                for b in range(3):
                    tap = 9 * a + 3 * b + e
                    for p in range(2):
                        first = step_j * 3 * line_size + a * line_size + (p + b) * 2 * lat + odd * lat
                        left = p * 2 * half
                        taps_in[q, first : first + lat, left : left + half] = in_weight[tap]
                        taps_in[q, first : first + lat, left + half : left + 2 * half] = peer_weight[tap]

    for on_lead in (True, False):
        for first in (True, False):

            @pl.when((lead == on_lead) & (has_prev != first))
            def _():
                count = sections - 1 + (0 if first else sections) + (0 if on_lead else 1)
                wait_rows(count * field_rows, field_recv.at[0])

    lane = iota((folded, 2 * lanes), 1)
    side = folded // 2
    for slot in (1, 0):
        got = [
            fields[slot, lax.rem(sec + sections - g, sections), 1].astype(jnp.float32)
            for g in range(sections)
        ]
        for f in range(frames):
            r = f % group
            low, high = (
                jnp.concatenate(
                    [got[g][r * side : (r + 1) * side] for g in (2 * t, 2 * t + 1)], axis=0
                )
                for t in range(2)
            )
            if f < group:
                high = pltpu.roll(high, lanes, 1)
            else:
                low = pltpu.roll(low, lanes, 1)
            at_f = ((1 - slot) * frames + f) * folded
            noise_lines[at_f : at_f + folded, :] = jnp.where(lane < lanes, low, high)

    loads[3][0].wait()
    lines_f = jnp.concatenate(
        [
            fields[slot, lax.rem(sec + sections - f, sections), 0]
            for slot in (1, 0)
            for f in range(frames)
        ],
        axis=0,
    ).astype(jnp.float32)
    lines_f = ((noise_lines[...] - step_size[0] * lines_f) * std + mean_latent).astype(
        jnp.bfloat16
    ).astype(jnp.float32)
    count = 2 * frames * folded
    f_row = iota((count, 2 * lanes), 0)
    i_row = lax.rem(f_row, rows_i)
    lines_f = jnp.where((f_row >= frames * folded) | has_prev, lines_f, 0.0)
    before = jnp.where(i_row == 0, 0.0, pltpu.roll(lines_f, 1, 0))
    after = jnp.where(i_row == rows_i - 1, 0.0, pltpu.roll(lines_f, count - 1, 0))
    shifted = jnp.concatenate([before, lines_f, after], axis=1).astype(jnp.bfloat16)
    line_values = jnp.concatenate(
        [
            dot(shifted[n * count // 2 : (n + 1) * count // 2], places[...])
            for n in range(2)
        ],
        axis=0,
    )
    half_j = cols_j // 2
    for f in range(2 * frames):
        for side in range(2):
            expanded[1 + side * half_j : 1 + (side + 1) * half_j, f] = line_values[
                f * folded : (f + 1) * folded, side * line_size : (side + 1) * line_size
            ].reshape(half_j, rows_i, line_size)
    block = near * rows_i
    for j in range(cols_j + 2):
        for a in range(3):
            stacked[j * block : (j + 1) * block, a * line_size : (a + 1) * line_size] = (
                expanded[j, a : a + near].reshape(block, line_size).astype(jnp.bfloat16)
            )
    dests = [
        jnp.where(is_end, mirrored(sections - 1), 0),
        jnp.where(is_end, mirrored(sections - 2), sections - 1),
        mirrored(jnp.where(is_end, 1, sections - 2)),
    ]
    parts = half // channels
    tall = near * height

    def upblock(homes, after=None):
        for q in range(2):
            lhs = jnp.concatenate(
                [
                    jnp.concatenate(
                        [
                            stacked[pl.ds(pl.multiple_of((j + q + n) * block, block), block), :]
                            for n in range(2)
                        ],
                        axis=1,
                    )
                    for j in homes
                ],
                axis=0,
            )
            for p in range(2):
                total = jnp.zeros((len(homes) * block, channels), jnp.float32)
                for h in range(2):
                    left = (p * 2 + h) * half
                    bias = in_bias[...] if h == 0 else peer_bias[...]
                    up = dot(lhs, taps_in[q, :, left : left + half]) + bias
                    up = up.astype(jnp.bfloat16).astype(jnp.float32)
                    for n in range(parts):
                        chunk = up[:, n * channels : (n + 1) * channels]
                        total = total + chunk * chunk
                    for m, j in enumerate(homes):
                        at_j = pl.ds(pl.multiple_of(2 * j * tall, tall) + q * tall + p, block, stride=2)
                        for n in range(parts):
                            ups[h * parts + n, at_j, :] = up[
                                m * block : (m + 1) * block, n * channels : (n + 1) * channels
                            ]
                for m, j in enumerate(homes):
                    at_j = pl.ds(pl.multiple_of(2 * j * tall, tall) + q * tall + p, block, stride=2)
                    squares[at_j, :] = total[m * block : (m + 1) * block]
            if after is not None:
                for j in homes:
                    after(2 * j + q)

    edge_high = dests[0] > 0
    first_home = jnp.where(edge_high, cols_j - 2, 0)

    mine = lax.rem(sec + parts * core, 2 * parts)
    gain = norm_gain[pl.ds(sec, 1), :]
    h_row = lax.rem(iota((tall, channels), 0), height)
    valid = has_prev | (iota((tall, channels), 0) >= 2 * height)

    def normalise(w):
        at_w = pl.ds(pl.multiple_of(w * tall, tall), tall)
        mean = jnp.sum(squares[at_w, :], axis=1, keepdims=True) / (2 * half)
        v = ups[mine, at_w, :] * lax.rsqrt(mean + 1e-06) * gain
        v = jnp.where(valid, v / (1.0 + jnp.exp(-v)), 0.0)
        above = jnp.where(h_row == 0, 0.0, pltpu.roll(v, 1, 0))
        below = jnp.where(h_row == height - 1, 0.0, pltpu.roll(v, tall - 1, 0))
        for b, line_v in enumerate((above, v, below)):
            wide[w + 1, :, b * channels : (b + 1) * channels] = line_v.astype(jnp.bfloat16)

    span = frames * height
    pair_columns = columns // 2

    def partial(d, first_column, count):
        windows, taps = [], []
        for a in range(3):
            for e in range(3):
                window = wide[
                    pl.ds(d * columns + e + first_column, count),
                    a * height : a * height + span,
                    :,
                ]
                windows.append(window.reshape(count * span, 3 * channels))
                taps += [weight[9 * a + 3 * b + e] for b in range(3)]
        low, high = (
            dot(
                jnp.concatenate(windows[first:last], axis=1),
                jnp.concatenate(taps[3 * first : 3 * last], axis=0),
            )
            for first, last in ((0, 5), (5, 9))
        )
        value = low + high * unit
        return [value[w * span : (w + 1) * span] for w in range(count)]

    neighbour = mirrored(1)
    targets = [jnp.where(is_end, neighbour, d) for d in dests]
    far_n = jnp.where(up_side, 1, 0)
    slots = [
        jnp.where(is_end, 2, 1 - far_n),
        jnp.where(is_end, 3, far_n),
        jnp.where(is_end, 0, 1),
    ]
    direct = [is_end | up_side, is_end | jnp.logical_not(up_side), is_end]

    marks = [jnp.where(slot < 2, slot, 2 + (slot - 2) * columns) for slot in slots]
    weights = [jnp.where(slot < 2, 0, 1) for slot in slots]

    def sum_copy(n, w):
        return pltpu.make_async_remote_copy(
            send_buf.at[n, w], recv_buf.at[slots[n], w], sum_send.at[0],
            sum_recv.at[marks[n] + w * weights[n]], device_id={"section": targets[n]},
        )

    def far_copy(w):
        return pltpu.make_async_remote_copy(
            send_buf.at[far_n, w], recv_buf.at[1, w], sum_send.at[0], sum_recv.at[1],
            device_id={"section": mirrored(sections - 1)},
        )

    def relay_far(side, *pieces_w):
        @pl.when(inner & (up_side if side else jnp.logical_not(up_side)))
        def _():
            for n in pieces_w:
                w = jnp.where(up_side, (2, 3, 1, 0)[n], n)
                send_buf[far_n, w] = (held[far_n, w] + arrived(2, w)).astype(jnp.bfloat16)
                far_copy(w).start()

    def arrived(slot, w):
        pltpu.make_async_copy(
            recv_buf.at[slot, w], recv_buf.at[slot, w], sum_recv.at[2 + (slot - 2) * columns + w]
        ).wait()
        return recv_buf[slot, w].astype(jnp.float32)

    upblock([first_home, first_home + 1], normalise)

    later = [4, *range(width - 1, width - 2 - columns, -1), *range(5, width - 1 - columns)]

    def normalise_next(numbers):
        for n in numbers:
            inward = jnp.where(edge_high, width - 5 - n, 4 + n)
            normalise(jnp.where(is_end, inward, later[n]))

    def hold(n, first_column, count):
        for c, value in enumerate(partial(dests[n], first_column, count)):
            send_buf[n, first_column + c] = value.astype(jnp.bfloat16)
            held[n, first_column + c] = value

    def send(n, pieces_w):
        @pl.when(direct[n])
        def _():
            for w in pieces_w:
                sum_copy(n, w).start()

    first_pair = jnp.where(edge_high, columns - 2, 0)
    third, fourth = jnp.where(edge_high, 1, 2), jnp.where(edge_high, 0, 3)
    hold(0, first_pair, 2)
    send(0, (first_pair, first_pair + 1))
    hold(0, third, 1)
    send(0, (third,))
    upblock([lax.rem(first_home + 2 + n, cols_j) for n in range(cols_j - 2)])
    normalise_next((0,))
    hold(0, fourth, 1)
    send(0, (fourth,))
    normalise_next(range(1, columns + 2))
    relay_far(False, 0)
    for m in (1, 0):
        hold(1, m * pair_columns, pair_columns)
        send(1, range(m * pair_columns, (m + 1) * pair_columns))
        if m == 1:
            relay_far(True, 0)
    relay_far(False, 1)
    normalise_next(range(columns + 2, width - 4))
    relay_far(False, 2)
    relay_far(True, 1)
    for m in range(2):
        hold(2, m * pair_columns, pair_columns)
    send(2, range(columns))
    relay_far(False, 3)
    relay_far(True, 2)

    for m in range(2):
        values = partial(sec, m * pair_columns, pair_columns)
        residual = []
        for w in range(pair_columns):
            first = pl.multiple_of(
                (sec * columns + m * pair_columns + w) * tall + 2 * height, height
            )
            residual.append(
                jnp.concatenate([ups[n, pl.ds(first, span), :] for n in range(parts)], axis=1)
            )
        for w, own in enumerate(values):
            acc[m * pair_columns + w] = own + conv_bias[...] + residual[w]

    relay_far(True, 3)

    @pl.when(inner)
    def _():
        for w in (2, 3, 0, 1):
            send_buf[2, w] = (held[2, w] + arrived(3, w)).astype(jnp.bfloat16)
            sum_copy(2, w).start()


    slot_rows = columns * span * half * 2 // 512

    def finish(first, last):
        wait_rows(slot_rows, sum_recv.at[first])
        for w in range(columns):
            acc[w] = acc[w] + recv_buf[first, w].astype(jnp.float32)
        wait_rows(slot_rows, sum_recv.at[last])
        for w in range(columns):
            total = acc[w] + recv_buf[last, w].astype(jnp.float32)
            for c in range(parts):
                final[c, pl.ds(w, span, stride=columns), :] = total[
                    :, c * channels : (c + 1) * channels
                ]


    @pl.when(is_end)
    def _():
        finish(0, 1)

    @pl.when(inner)
    def _():
        finish(1, 0)

    for n in range(parts):
        out[:, n * channels : (n + 1) * channels] = final[n].astype(out.dtype)
    wait_rows(3 * columns * span * half * 2 // 512, sum_send.at[0])
    for c in early:
        c.wait_send()

    @pl.when(core == 0)
    def _():
        pair.wait_send()

    for first in (True, False):

        @pl.when(lead & (has_next != first))
        def _():
            count = 2 * (sections - 1) + (0 if first else 2 * sections) + 1
            wait_rows(count * field_rows, field_send.at[0])


def fused_shards(sizes, *arrays):
    (
        hidden, modulation, time_embed, head_weight, head_bias, noisy, step_size, latent_mean,
        latent_std, in_weight, in_bias, norm_gain, conv_weight, conv_bias,
    ) = arrays
    sections, clips_sp, frames, height, columns, lat, channels = sizes
    rows_i, cols_j, half = height // 2, columns * sections // 2, in_weight.shape[2]
    width, near, tokens, lanes = columns * sections, frames + 2, hidden.shape[0], 4 * lat
    line_size = 8 * lat
    f32, bf16 = jnp.float32, jnp.bfloat16
    vmem, dma = pltpu.VMEM, pltpu.SemaphoreType.DMA
    rows = columns * frames * height
    operands = (
        modulation, time_embed[None], head_bias[None], noisy.reshape(-1, lat),
        latent_std[None], latent_mean[None], in_bias[None], norm_gain.reshape(-1, channels),
        conv_bias[None], hidden, head_weight.T, in_weight, conv_weight,
    )
    operands = [pltpu.with_memory_space_constraint(value, pltpu.HBM) for value in operands]
    far = pl.BlockSpec(memory_space=pltpu.HBM)
    out = pl.pallas_call(
        functools.partial(block_kernel, sizes),
        out_shape=pltpu.VMEM((rows, half), bf16),
        in_specs=[far] * 4
        + [pl.BlockSpec(memory_space=pltpu.SMEM)]
        + [far] * (len(operands) - 4),
        out_specs=pl.BlockSpec(memory_space=pltpu.VMEM),
        scratch_shapes=[vmem(value.shape, value.dtype) for value in operands]
        + [
            vmem((tokens, tokens), bf16),
            vmem((rows // 8, rows), bf16),
            vmem((rows, 2 * lanes), f32),
            vmem((6 * lanes, 2 * line_size), bf16),
            vmem((tokens + 8, 128), f32),
            vmem((tokens + 8, 128), f32),
            vmem(in_weight.shape, bf16),
            vmem((1, half), f32),
            vmem((2, sections, 2, tokens // 2, 2 * lanes), bf16),
            vmem((2 * frames * tokens // 2, 2 * lanes), f32),
            vmem((cols_j + 2, 2 * frames, rows_i, line_size), f32),
            vmem(((cols_j + 2) * near * rows_i, 3 * line_size), bf16),
            vmem((2, 6 * line_size, 4 * half), bf16),
            vmem((2 * half // channels, width * near * height, channels), f32),
            vmem((width * near * height, channels), f32),
            vmem((width + 2, near * height, 3 * channels), bf16),
            vmem((3, columns, rows // columns, half), bf16),
            vmem((4, columns, rows // columns, half), bf16),
            vmem((3, columns, rows // columns, half), f32),
            vmem((columns, rows // columns, half), f32),
            vmem((half // channels, rows, channels), f32),
            dma((5,)),
            dma((3,)),
            dma((3,)),
            dma((1,)),
            dma((1,)),
            dma((1,)),
            dma((2 + 2 * columns,)),
        ],
        compiler_params=pltpu.CompilerParams(
            collective_id=0, has_side_effects=True, vmem_limit_bytes=40 * 2**20
        ),
    )(*operands[:4], step_size, *operands[4:])
    return out.reshape(frames, height, columns, half)


def dispatch(*arrays):
    hidden, noisy, in_weight, conv_weight = arrays[0], arrays[5], arrays[9], arrays[12]
    frames, height, columns, lat = noisy.shape
    sections, cores, clips_sp = (lax.axis_size(axis) for axis in ("section", "tp", "sp"))
    channels, half = conv_weight.shape[1:]
    whole_frame = hidden.shape[0] == height // 2 * (columns * sections // 2)
    if (
        whole_frame
        and cores == 2
        and clips_sp > 1
        and frames == sections
        and sections == 4
        and columns == 4
        and channels % 128 == 0
        and half % channels == 0
        and lat == 16
        and height == 16
    ):
        sizes = (sections, clips_sp, frames, height, columns, lat, channels)
        return fused_shards(sizes, *arrays)
    return shards(*arrays)


def solution(mesh):
    placed = (
        P(("groups", "sp", "section"), "tp"),
        P(None, "tp"),
        P(("groups", "tp")),
        P("tp", None),
        P(),
        P(("groups", "sp"), None, "section", None),
        P("groups"),
        P(),
        P(),
        P(None, None, "tp"),
        P("tp"),
        P(),
        P(None, "section", "tp"),
        P("tp"),
    )
    return jax.shard_map(
        dispatch,
        mesh=mesh,
        in_specs=placed,
        out_specs=P(("groups", "sp"), None, "section", "tp"),
        check_vma=False,
    )
```

```python
import functools

import jax
import jax.numpy as jnp
from jax import lax
from jax.experimental import pallas as pl
from jax.experimental.pallas import tpu as pltpu
from jax.sharding import PartitionSpec as P

D = 6144


def padded_2(value, sides, width):
    for axis, dim in sides:
        count, length = (lax.axis_size(axis), value.shape[dim])
        up = [(i, (i + 1) % count) for i in range(count - 1)]
        down = [(j, i) for i, j in up]
        last = lax.slice_in_dim(value, length - width, length, axis=dim)
        leading = lax.slice_in_dim(value, 0, width, axis=dim)
        before = lax.ppermute(last, axis, up)
        after = lax.ppermute(leading, axis, down)
        value = jnp.concatenate([before, value, after], axis=dim)
    return value


def passed_along(value, axis, by):
    count = lax.axis_size(axis)
    pairs = [(i, i + by) for i in range(count) if 0 <= i + by < count]
    return lax.ppermute(value, axis, pairs)


def conv_taps(padded, weight, frames, height, columns):
    channels = padded.shape[3]
    result = jnp.zeros((frames * height * columns, weight.shape[2]), jnp.float32)
    for offset_time in range(3):
        for offset_row in range(3):
            slab = padded[offset_time : offset_time + frames, offset_row : offset_row + height]
            window = jnp.concatenate(
                [slab[:, :, 0:columns], slab[:, :, 1 : columns + 1], slab[:, :, 2 : columns + 2]],
                axis=3,
            )
            first = 9 * offset_time + 3 * offset_row
            taps = weight[first : first + 3].reshape(3 * channels, weight.shape[2])
            result = result + jnp.dot(
                window.reshape(-1, 3 * channels), taps, preferred_element_type=jnp.float32
            )
    return result


def activate(source, gain_vector):
    values = source.astype(jnp.float32)
    squares = jnp.mean(values * values, axis=-1, keepdims=True)
    return jax.nn.silu(values * lax.rsqrt(squares + 1e-06) * gain_vector).astype(jnp.bfloat16)


def pad_rows(source):
    return jnp.pad(source, ((0, 0), (1, 1), (0, 0), (0, 0)))


def shards(
    hidden,
    modulation,
    time_embed,
    head_weight,
    head_bias,
    noisy,
    step_size,
    latent_mean,
    latent_std,
    in_weight,
    in_bias,
    norm_gain,
    conv_weight,
    conv_bias,
):
    frames, height, columns, lat_channels = noisy.shape
    sections = lax.axis_size("section")
    half_channels = in_weight.shape[2]
    values = hidden.astype(jnp.float32)
    row_sums, square_sums = lax.psum(
        (jnp.sum(values, axis=1), jnp.sum(values * values, axis=1)), "tp"
    )
    average = row_sums / D
    variance = square_sums / D - average * average
    shift_term = modulation[0] + time_embed
    scale_term = modulation[1] + time_embed
    modulated = (
        (values - average[:, None]) * lax.rsqrt(variance[:, None] + 1e-06) * (1.0 + scale_term)
        + shift_term
    ).astype(jnp.bfloat16)
    partial_sum = jnp.dot(modulated, head_weight, preferred_element_type=jnp.float32)
    velocity = (lax.psum(partial_sum, "tp") + head_bias).astype(jnp.bfloat16)
    band_rows = velocity.shape[0] * 2 // (columns * sections)
    outgoing = velocity.reshape(band_rows, sections, -1)
    arrived = lax.all_to_all(outgoing, "section", split_axis=1, concat_axis=0, tiled=True)
    latent_field = arrived.reshape(frames, height // 2, columns // 2, 2, 2, lat_channels)
    latent_field = jnp.transpose(latent_field, (0, 1, 3, 2, 4, 5)).reshape(
        frames, height, columns, lat_channels
    )
    latent = (
        (noisy.astype(jnp.float32) - step_size[0] * latent_field.astype(jnp.float32)) * latent_std
        + latent_mean
    ).astype(jnp.bfloat16)
    latent_wide = padded_2(latent, (("section", 2),), 2)
    earlier = passed_along(latent_wide, "sp", 1)
    stacked = pad_rows(jnp.concatenate([earlier, latent_wide], axis=0))
    extended = (conv_taps(stacked, in_weight, frames + 2, height, columns + 2) + in_bias).astype(
        jnp.bfloat16
    )
    extended = extended.reshape(frames + 2, height, columns + 2, half_channels)
    upblock_half = extended[2:, :, 1 : columns + 1]
    extended_full = lax.all_gather(extended, "tp", axis=3, tiled=True)
    normed = activate(extended_full, norm_gain)
    frame_index = lax.axis_index("sp") * frames - 2 + jnp.arange(frames + 2, dtype=jnp.int32)
    column_index = (
        lax.axis_index("section") * columns - 1 + jnp.arange(columns + 2, dtype=jnp.int32)
    )
    inside_cols = (column_index >= 0) & (column_index < columns * sections)
    inside = (frame_index >= 0)[:, None, None, None] & inside_cols[None, None, :, None]
    conv_input = pad_rows(jnp.where(inside, normed, jnp.zeros_like(normed)))
    full_weight = lax.all_gather(conv_weight, "section", axis=1, tiled=True)
    mixed = conv_taps(conv_input, full_weight, frames, height, columns)
    decoded = (
        upblock_half.astype(jnp.float32).reshape(-1, half_channels) + mixed + conv_bias
    ).astype(jnp.bfloat16)
    return decoded.reshape(frames, height, columns, half_channels)


def iota(shape, dim):
    return lax.broadcasted_iota(jnp.int32, shape, dim)


def dot(left, right):
    return jnp.dot(left, right, preferred_element_type=jnp.float32)


def dot_rows(left, right):
    return lax.dot_general(
        left, right, (((1,), (1,)), ((), ())), preferred_element_type=jnp.float32
    )


def pieces(value):
    high = value.astype(jnp.bfloat16)
    rest = value - high.astype(jnp.float32)
    middle = rest.astype(jnp.bfloat16)
    low = (rest - middle.astype(jnp.float32)).astype(jnp.bfloat16)
    return high.astype(jnp.float32), middle.astype(jnp.float32), low.astype(jnp.float32)


def block_kernel(
    sizes,
    modulation_far,
    time_far,
    head_bias_far,
    noisy_far,
    step_size,
    std_far,
    mean_far,
    in_bias_far,
    gain_far,
    conv_bias_far,
    hidden_far,
    head_far,
    in_far,
    conv_far,
    out,
    modulation,
    time_embed,
    head_bias,
    noisy,
    latent_std,
    latent_mean,
    in_bias,
    norm_gain,
    conv_bias,
    hidden,
    head_weight,
    in_weight,
    weight,
    swap,
    noise_pick,
    noise_mask,
    places,
    part,
    peer_part,
    peer_weight,
    peer_bias,
    fields,
    noise_lines,
    expanded,
    stacked,
    taps_in,
    ups,
    squares,
    wide,
    send_buf,
    recv_buf,
    held,
    acc,
    final,
    load_sems,
    pair_send,
    pair_recv,
    field_send,
    field_recv,
    sum_send,
    sum_recv,
):
    sections, clips_sp, frames, height, columns, lat, channels = sizes
    rows_i, cols_j = height // 2, columns * sections // 2
    width = columns * sections
    tokens = rows_i * cols_j
    near = frames + 2
    half = in_weight.shape[2]
    lanes = 4 * lat
    folded = tokens // 2
    line_size = 4 * 2 * lat
    sec, core, spi = lax.axis_index("section"), lax.axis_index("tp"), lax.axis_index("sp")
    nxt = lax.rem(spi + 1, clips_sp)
    prv = lax.rem(spi + clips_sp - 1, clips_sp)
    has_next, has_prev = spi + 1 < clips_sp, spi > 0
    peer = {"tp": 1 - core}

    lead = core == 1
    unit = jnp.where(core >= 0, 1.0, 0.0)
    groups = (
        ((hidden_far, hidden), (head_far, head_weight)),
        ((modulation_far, modulation), (time_far, time_embed)),
        (
            (noisy_far, noisy),
            (in_bias_far, in_bias),
            (head_bias_far, head_bias),
            (std_far, latent_std),
            (mean_far, latent_mean),
            (gain_far, norm_gain),
            (conv_bias_far, conv_bias),
        ),
        ((conv_far, weight),),
        ((in_far, in_weight),),
    )
    loads = [
        [pltpu.make_async_copy(source, target, load_sems.at[n]) for source, target in members]
        for n, members in enumerate(groups)
    ]
    for c in loads[1] + loads[0]:
        c.start()

    barrier = pltpu.get_barrier_semaphore()
    pl.semaphore_signal(barrier, inc=1, device_id=peer)
    for k in range(1, sections):
        pl.semaphore_signal(
            barrier, inc=1, device_id={"section": lax.rem(sec + k, sections), "tp": 1}
        )

    @pl.when(has_prev)
    def _():
        for k in range(sections):
            pl.semaphore_signal(
                barrier,
                inc=1,
                device_id={"section": lax.rem(sec + k, sections), "sp": prv, "tp": 1},
            )


    for c in loads[2]:
        c.start()

    def pair_copy(n, source, target):
        return pltpu.make_async_remote_copy(
            source, target, pair_send.at[n], pair_recv.at[n], device_id=peer
        )

    def wait_rows(count, sem):
        view = ups.at[0, pl.ds(0, count), :]
        pltpu.make_async_copy(view, view, sem).wait()

    up_side = sec < sections // 2
    is_end = (sec == 0) | (sec == sections - 1)
    inner = jnp.logical_not(is_end)

    def mirrored(value):
        return jnp.where(up_side, value, sections - 1 - value)

    others = [mirrored(jnp.where(is_end, sections - 1 - n, (3, 2, 0)[n])) for n in range(3)]

    def spread_copy(z, ahead, c):
        slot = lax.rem(z - sec + sections, sections)
        return pltpu.make_async_remote_copy(
            fields.at[0, 0], fields.at[ahead, slot], field_send.at[0], field_recv.at[0],
            device_id={"section": z, "sp": nxt if ahead else spi, "tp": c},
        )

    def spread():
        for z in [*others, sec]:
            if z is not sec:
                spread_copy(z, 0, 0).start()

            @pl.when(has_next)
            def _():
                for c in (0, 1):
                    spread_copy(z, 1, c).start()

            if z is not sec:
                spread_copy(z, 0, 1).start()

        pltpu.make_async_remote_copy(
            fields.at[0, 0], fields.at[0, 0], field_send.at[0], field_recv.at[0], device_id=peer
        ).start()

    field_rows = 2 * folded * 2 * lanes * 2 // 512

    to, at = iota((tokens, tokens), 0), iota((tokens, tokens), 1)
    swap[...] = (lax.rem(to, rows_i) * cols_j + lax.div(to, rows_i) == at).astype(jnp.bfloat16)
    cells = frames * height * columns
    group = frames // 2
    r_line, r_col = lax.div(iota((cells, 2 * lanes), 0), columns), lax.rem(
        iota((cells, 2 * lanes), 0), columns
    )
    r_slot = lax.div(lax.div(r_line, height), group) * 4 + lax.rem(r_line, 2) * 2 + lax.rem(r_col, 2)
    noise_mask[...] = (lax.div(iota((cells, 2 * lanes), 1), lat) == r_slot).astype(jnp.float32)
    packed = cells // 8
    r_at, r_to = iota((packed, cells), 1), iota((packed, cells), 0)
    r_line, r_col = lax.div(r_at, columns), lax.rem(r_at, columns)
    r_home = (
        lax.rem(lax.div(r_line, height), group) * (columns // 2) + lax.div(r_col, 2)
    ) * rows_i + lax.div(lax.rem(r_line, height), 2)
    noise_pick[...] = (r_to == r_home).astype(jnp.bfloat16)
    shape = (2 * lanes, 2 * line_size)
    src, dst = iota(shape, 0), iota(shape, 1)
    same = lax.div(src, lanes) == lax.div(dst, line_size)
    src, dst = lax.rem(src, lanes), lax.rem(dst, line_size)
    places[0 * shape[0] : (0 + 1) * shape[0]] = (same & (src == dst + 2 * lat) & (dst < 2 * lat)).astype(jnp.bfloat16)
    places[1 * shape[0] : (1 + 1) * shape[0]] = (same & (src + 2 * lat == dst)).astype(jnp.bfloat16)
    places[2 * shape[0] : (2 + 1) * shape[0]] = (same & (src + 6 * lat == dst) & (dst >= 6 * lat)).astype(jnp.bfloat16)
    expanded[...] = jnp.zeros_like(expanded)
    taps_in[...] = jnp.zeros_like(taps_in)
    wide[0] = jnp.zeros_like(wide[0])
    wide[width + 1] = jnp.zeros_like(wide[0])

    @pl.when(jnp.logical_not(has_prev))
    def _():
        fields[1] = jnp.zeros_like(fields[1])

    features = hidden.shape[1]
    for c in loads[1]:
        c.wait()
    scale = 1.0 + (modulation[1:2, :] + time_embed[...])
    shift = modulation[0:1, :] + time_embed[...]
    row = iota((8, features), 0)
    lines = jnp.zeros((8, features), jnp.float32)
    for n, piece in enumerate(pieces(scale) + pieces(shift)):
        lines = jnp.where(row == n, piece, lines)
    lines = jnp.concatenate([lines, jnp.zeros_like(lines)], axis=0).astype(jnp.bfloat16)
    for c in loads[0]:
        c.wait()
    loads[4][0].start()
    loads[3][0].start()
    values = hidden[...].astype(jnp.float32)
    own_sum = jnp.sum(values, axis=1, keepdims=True)
    own_square = jnp.sum(values * values, axis=1, keepdims=True)
    center = own_sum / features
    centred = ((values - center) * scale).astype(jnp.bfloat16)
    stack = jnp.concatenate([centred, lines], axis=0)
    cut = features // 2
    made = dot_rows(stack[:, :cut], head_weight[:, :cut])
    made = made + dot_rows(stack[:, cut:], head_weight[:, cut:]) * unit
    part[:tokens, :lanes] = made[:tokens]
    stat_shape = (tokens, 128 - lanes)
    part[:tokens, lanes:] = jnp.where(
        iota(stat_shape, 1) < stat_shape[1] // 2, own_sum, own_square
    )
    made = made[tokens:]
    line = iota(made.shape, 0)
    own_scale = jnp.sum(jnp.where(line < 3, made, 0.0), axis=0, keepdims=True)
    own_shift = jnp.sum(jnp.where(line < 3, 0.0, made), axis=0, keepdims=True)
    part[tokens:, :lanes] = jnp.where(iota((8, lanes), 0) == 0, own_scale, own_shift)
    part[tokens:, lanes:] = jnp.zeros((8, 128 - lanes), jnp.float32)
    pair = pair_copy(0, part, peer_part)
    early = [pair_copy(1, in_weight, peer_weight), pair_copy(2, in_bias, peer_bias)]
    for c in loads[2]:
        c.wait()
    std = jnp.concatenate([latent_std[...]] * 8, axis=1)
    mean_latent = jnp.concatenate([latent_mean[...]] * 8, axis=1)

    @pl.when(core == 0)
    def _():
        pl.semaphore_wait(barrier, 1)
        pair.start()
        loads[4][0].wait()
        for c in early:
            c.start()

    @pl.when(lead)
    def _():
        src, dst = iota((lat, 2 * lanes), 0), iota((lat, 2 * lanes), 1)
        tiled = dot(noisy[...], (src == lax.rem(dst, lat)).astype(jnp.bfloat16))
        tiled = (tiled * noise_mask[...]).astype(jnp.bfloat16)
        fields[0, 0, 1] = dot(noise_pick[...], tiled).astype(jnp.bfloat16)
        pair.wait_recv()
        far_sum = peer_part[:tokens, lanes : lanes + 1]
        far_square = peer_part[
            :tokens, lanes + (128 - lanes) // 2 : lanes + (128 - lanes) // 2 + 1
        ]
        average = (own_sum + far_sum) / D
        variance = (own_square + far_square) / D - average * average
        body = (
            part[:tokens, :lanes]
            + peer_part[:tokens, :lanes]
            - (average - center) * own_scale
            - (average - far_sum / features) * peer_part[tokens : tokens + 1, :lanes]
        )
        velocity = (
            lax.rsqrt(variance + 1e-06) * body
            + (own_shift + peer_part[tokens + 1 : tokens + 2, :lanes])
            + head_bias[...]
        ).astype(jnp.bfloat16)
        field = dot(swap[...], velocity)
        fields[0, 0, 0] = jnp.concatenate([field[:folded], field[folded:]], axis=1).astype(
            jnp.bfloat16
        )
        pl.semaphore_wait(
            barrier, 2 * sections - 1 + jnp.where(has_next, 2 * sections, 0)
        )
        spread()
        loads[4][0].wait()
        for c in early:
            c.start()

    for c in early:
        c.wait_recv()
    for q in range(2):
        for e in range(3):
            col = q + e
            step_j, odd = (col + 1) // 2 - q, (col + 1) % 2
            for a in range(3):
                for b in range(3):
                    tap = 9 * a + 3 * b + e
                    for p in range(2):
                        first = step_j * 3 * line_size + a * line_size + (p + b) * 2 * lat + odd * lat
                        left = p * 2 * half
                        taps_in[q, first : first + lat, left : left + half] = in_weight[tap]
                        taps_in[q, first : first + lat, left + half : left + 2 * half] = peer_weight[tap]

    for on_lead in (True, False):
        for first in (True, False):

            @pl.when((lead == on_lead) & (has_prev != first))
            def _():
                count = sections - 1 + (0 if first else sections) + (0 if on_lead else 1)
                wait_rows(count * field_rows, field_recv.at[0])

    lane = iota((folded, 2 * lanes), 1)
    side = folded // 2
    for slot in (1, 0):
        got = [
            fields[slot, lax.rem(sec + sections - g, sections), 1].astype(jnp.float32)
            for g in range(sections)
        ]
        for f in range(frames):
            r = f % group
            low, high = (
                jnp.concatenate(
                    [got[g][r * side : (r + 1) * side] for g in (2 * t, 2 * t + 1)], axis=0
                )
                for t in range(2)
            )
            if f < group:
                high = pltpu.roll(high, lanes, 1)
            else:
                low = pltpu.roll(low, lanes, 1)
            at_f = ((1 - slot) * frames + f) * folded
            noise_lines[at_f : at_f + folded, :] = jnp.where(lane < lanes, low, high)

    loads[3][0].wait()
    lines_f = jnp.concatenate(
        [
            fields[slot, lax.rem(sec + sections - f, sections), 0]
            for slot in (1, 0)
            for f in range(frames)
        ],
        axis=0,
    ).astype(jnp.float32)
    lines_f = ((noise_lines[...] - step_size[0] * lines_f) * std + mean_latent).astype(
        jnp.bfloat16
    ).astype(jnp.float32)
    count = 2 * frames * folded
    f_row = iota((count, 2 * lanes), 0)
    i_row = lax.rem(f_row, rows_i)
    lines_f = jnp.where((f_row >= frames * folded) | has_prev, lines_f, 0.0)
    before = jnp.where(i_row == 0, 0.0, pltpu.roll(lines_f, 1, 0))
    after = jnp.where(i_row == rows_i - 1, 0.0, pltpu.roll(lines_f, count - 1, 0))
    shifted = jnp.concatenate([before, lines_f, after], axis=1).astype(jnp.bfloat16)
    line_values = jnp.concatenate(
        [
            dot(shifted[n * count // 2 : (n + 1) * count // 2], places[...])
            for n in range(2)
        ],
        axis=0,
    )
    half_j = cols_j // 2
    for f in range(2 * frames):
        for side in range(2):
            expanded[1 + side * half_j : 1 + (side + 1) * half_j, f] = line_values[
                f * folded : (f + 1) * folded, side * line_size : (side + 1) * line_size
            ].reshape(half_j, rows_i, line_size)
    block = near * rows_i
    for j in range(cols_j + 2):
        for a in range(3):
            stacked[j * block : (j + 1) * block, a * line_size : (a + 1) * line_size] = (
                expanded[j, a : a + near].reshape(block, line_size).astype(jnp.bfloat16)
            )
    dests = [
        jnp.where(is_end, mirrored(sections - 1), 0),
        jnp.where(is_end, mirrored(sections - 2), sections - 1),
        mirrored(jnp.where(is_end, 1, sections - 2)),
    ]
    parts = half // channels
    tall = near * height

    def upblock(homes, after=None):
        for q in range(2):
            lhs = jnp.concatenate(
                [
                    jnp.concatenate(
                        [
                            stacked[pl.ds(pl.multiple_of((j + q + n) * block, block), block), :]
                            for n in range(2)
                        ],
                        axis=1,
                    )
                    for j in homes
                ],
                axis=0,
            )
            for p in range(2):
                total = jnp.zeros((len(homes) * block, channels), jnp.float32)
                for h in range(2):
                    left = (p * 2 + h) * half
                    bias = in_bias[...] if h == 0 else peer_bias[...]
                    up = dot(lhs, taps_in[q, :, left : left + half]) + bias
                    up = up.astype(jnp.bfloat16).astype(jnp.float32)
                    for n in range(parts):
                        chunk = up[:, n * channels : (n + 1) * channels]
                        total = total + chunk * chunk
                    for m, j in enumerate(homes):
                        at_j = pl.ds(pl.multiple_of(2 * j * tall, tall) + q * tall + p, block, stride=2)
                        for n in range(parts):
                            ups[h * parts + n, at_j, :] = up[
                                m * block : (m + 1) * block, n * channels : (n + 1) * channels
                            ]
                for m, j in enumerate(homes):
                    at_j = pl.ds(pl.multiple_of(2 * j * tall, tall) + q * tall + p, block, stride=2)
                    squares[at_j, :] = total[m * block : (m + 1) * block]
            if after is not None:
                for j in homes:
                    after(2 * j + q)

    edge_high = dests[0] > 0
    first_home = jnp.where(edge_high, cols_j - 2, 0)

    mine = lax.rem(sec + parts * core, 2 * parts)
    gain = norm_gain[pl.ds(sec, 1), :]
    h_row = lax.rem(iota((tall, channels), 0), height)
    valid = has_prev | (iota((tall, channels), 0) >= 2 * height)

    def normalise(w):
        at_w = pl.ds(pl.multiple_of(w * tall, tall), tall)
        mean = jnp.sum(squares[at_w, :], axis=1, keepdims=True) / (2 * half)
        v = ups[mine, at_w, :] * lax.rsqrt(mean + 1e-06) * gain
        v = jnp.where(valid, v / (1.0 + jnp.exp(-v)), 0.0)
        above = jnp.where(h_row == 0, 0.0, pltpu.roll(v, 1, 0))
        below = jnp.where(h_row == height - 1, 0.0, pltpu.roll(v, tall - 1, 0))
        for b, line_v in enumerate((above, v, below)):
            wide[w + 1, :, b * channels : (b + 1) * channels] = line_v.astype(jnp.bfloat16)

    span = frames * height
    pair_columns = columns // 2

    def partial(d, first_column, count):
        windows, taps = [], []
        for a in range(3):
            for e in range(3):
                window = wide[
                    pl.ds(d * columns + e + first_column, count),
                    a * height : a * height + span,
                    :,
                ]
                windows.append(window.reshape(count * span, 3 * channels))
                taps += [weight[9 * a + 3 * b + e] for b in range(3)]
        low, high = (
            dot(
                jnp.concatenate(windows[first:last], axis=1),
                jnp.concatenate(taps[3 * first : 3 * last], axis=0),
            )
            for first, last in ((0, 5), (5, 9))
        )
        value = low + high * unit
        return [value[w * span : (w + 1) * span] for w in range(count)]

    neighbour = mirrored(1)
    targets = [jnp.where(is_end, neighbour, d) for d in dests]
    far_n = jnp.where(up_side, 1, 0)
    slots = [
        jnp.where(is_end, 2, 1 - far_n),
        jnp.where(is_end, 3, far_n),
        jnp.where(is_end, 0, 1),
    ]
    direct = [is_end | up_side, is_end | jnp.logical_not(up_side), is_end]

    marks = [jnp.where(slot < 2, slot, 2 + (slot - 2) * columns) for slot in slots]
    weights = [jnp.where(slot < 2, 0, 1) for slot in slots]

    def sum_copy(n, w):
        return pltpu.make_async_remote_copy(
            send_buf.at[n, w], recv_buf.at[slots[n], w], sum_send.at[0],
            sum_recv.at[marks[n] + w * weights[n]], device_id={"section": targets[n]},
        )

    def far_copy(w):
        return pltpu.make_async_remote_copy(
            send_buf.at[far_n, w], recv_buf.at[1, w], sum_send.at[0], sum_recv.at[1],
            device_id={"section": mirrored(sections - 1)},
        )

    def relay_far(side, *pieces_w):
        @pl.when(inner & (up_side if side else jnp.logical_not(up_side)))
        def _():
            for n in pieces_w:
                w = jnp.where(up_side, (2, 3, 1, 0)[n], n)
                send_buf[far_n, w] = (held[far_n, w] + arrived(2, w)).astype(jnp.bfloat16)
                far_copy(w).start()

    def arrived(slot, w):
        pltpu.make_async_copy(
            recv_buf.at[slot, w], recv_buf.at[slot, w], sum_recv.at[2 + (slot - 2) * columns + w]
        ).wait()
        return recv_buf[slot, w].astype(jnp.float32)

    upblock([first_home, first_home + 1], normalise)

    later = [4, *range(width - 1, width - 2 - columns, -1), *range(5, width - 1 - columns)]

    def normalise_next(numbers):
        for n in numbers:
            inward = jnp.where(edge_high, width - 5 - n, 4 + n)
            normalise(jnp.where(is_end, inward, later[n]))

    def hold(n, first_column, count):
        for c, value in enumerate(partial(dests[n], first_column, count)):
            send_buf[n, first_column + c] = value.astype(jnp.bfloat16)
            held[n, first_column + c] = value

    def send(n, pieces_w):
        @pl.when(direct[n])
        def _():
            for w in pieces_w:
                sum_copy(n, w).start()

    first_pair = jnp.where(edge_high, columns - 2, 0)
    third, fourth = jnp.where(edge_high, 1, 2), jnp.where(edge_high, 0, 3)
    hold(0, first_pair, 2)
    send(0, (first_pair, first_pair + 1))
    hold(0, third, 1)
    send(0, (third,))
    upblock([lax.rem(first_home + 2 + n, cols_j) for n in range(cols_j - 2)])
    normalise_next((0,))
    hold(0, fourth, 1)
    send(0, (fourth,))
    normalise_next(range(1, columns + 2))
    relay_far(False, 0)
    for m in (1, 0):
        hold(1, m * pair_columns, pair_columns)
        send(1, range(m * pair_columns, (m + 1) * pair_columns))
        if m == 1:
            relay_far(True, 0)
    relay_far(False, 1)
    normalise_next(range(columns + 2, width - 4))
    relay_far(False, 2)
    relay_far(True, 1)
    for m in range(2):
        hold(2, m * pair_columns, pair_columns)
    send(2, range(columns))
    relay_far(False, 3)
    relay_far(True, 2)

    for m in range(2):
        values = partial(sec, m * pair_columns, pair_columns)
        residual = []
        for w in range(pair_columns):
            first = pl.multiple_of(
                (sec * columns + m * pair_columns + w) * tall + 2 * height, height
            )
            residual.append(
                jnp.concatenate([ups[n, pl.ds(first, span), :] for n in range(parts)], axis=1)
            )
        for w, own in enumerate(values):
            acc[m * pair_columns + w] = own + conv_bias[...] + residual[w]

    relay_far(True, 3)

    @pl.when(inner)
    def _():
        for w in (2, 3, 0, 1):
            send_buf[2, w] = (held[2, w] + arrived(3, w)).astype(jnp.bfloat16)
            sum_copy(2, w).start()


    slot_rows = columns * span * half * 2 // 512

    def finish(first, last):
        wait_rows(slot_rows, sum_recv.at[first])
        for w in range(columns):
            acc[w] = acc[w] + recv_buf[first, w].astype(jnp.float32)
        wait_rows(slot_rows, sum_recv.at[last])
        for w in range(columns):
            total = acc[w] + recv_buf[last, w].astype(jnp.float32)
            for c in range(parts):
                final[c, pl.ds(w, span, stride=columns), :] = total[
                    :, c * channels : (c + 1) * channels
                ]


    @pl.when(is_end)
    def _():
        finish(0, 1)

    @pl.when(inner)
    def _():
        finish(1, 0)

    for n in range(parts):
        out[:, n * channels : (n + 1) * channels] = final[n].astype(out.dtype)
    wait_rows(3 * columns * span * half * 2 // 512, sum_send.at[0])
    for c in early:
        c.wait_send()

    @pl.when(core == 0)
    def _():
        pair.wait_send()

    for first in (True, False):

        @pl.when(lead & (has_next != first))
        def _():
            count = 2 * (sections - 1) + (0 if first else 2 * sections) + 1
            wait_rows(count * field_rows, field_send.at[0])


def fused_shards(sizes, *arrays):
    (
        hidden, modulation, time_embed, head_weight, head_bias, noisy, step_size, latent_mean,
        latent_std, in_weight, in_bias, norm_gain, conv_weight, conv_bias,
    ) = arrays
    sections, clips_sp, frames, height, columns, lat, channels = sizes
    rows_i, cols_j, half = height // 2, columns * sections // 2, in_weight.shape[2]
    width, near, tokens, lanes = columns * sections, frames + 2, hidden.shape[0], 4 * lat
    line_size = 8 * lat
    f32, bf16 = jnp.float32, jnp.bfloat16
    vmem, dma = pltpu.VMEM, pltpu.SemaphoreType.DMA
    rows = columns * frames * height
    operands = (
        modulation, time_embed[None], head_bias[None], noisy.reshape(-1, lat),
        latent_std[None], latent_mean[None], in_bias[None], norm_gain.reshape(-1, channels),
        conv_bias[None], hidden, head_weight.T, in_weight, conv_weight,
    )
    operands = [pltpu.with_memory_space_constraint(value, pltpu.HBM) for value in operands]
    far = pl.BlockSpec(memory_space=pltpu.HBM)
    out = pl.pallas_call(
        functools.partial(block_kernel, sizes),
        out_shape=pltpu.VMEM((rows, half), bf16),
        in_specs=[far] * 4
        + [pl.BlockSpec(memory_space=pltpu.SMEM)]
        + [far] * (len(operands) - 4),
        out_specs=pl.BlockSpec(memory_space=pltpu.VMEM),
        scratch_shapes=[vmem(value.shape, value.dtype) for value in operands]
        + [
            vmem((tokens, tokens), bf16),
            vmem((rows // 8, rows), bf16),
            vmem((rows, 2 * lanes), f32),
            vmem((6 * lanes, 2 * line_size), bf16),
            vmem((tokens + 8, 128), f32),
            vmem((tokens + 8, 128), f32),
            vmem(in_weight.shape, bf16),
            vmem((1, half), f32),
            vmem((2, sections, 2, tokens // 2, 2 * lanes), bf16),
            vmem((2 * frames * tokens // 2, 2 * lanes), f32),
            vmem((cols_j + 2, 2 * frames, rows_i, line_size), f32),
            vmem(((cols_j + 2) * near * rows_i, 3 * line_size), bf16),
            vmem((2, 6 * line_size, 4 * half), bf16),
            vmem((2 * half // channels, width * near * height, channels), f32),
            vmem((width * near * height, channels), f32),
            vmem((width + 2, near * height, 3 * channels), bf16),
            vmem((3, columns, rows // columns, half), bf16),
            vmem((4, columns, rows // columns, half), bf16),
            vmem((3, columns, rows // columns, half), f32),
            vmem((columns, rows // columns, half), f32),
            vmem((half // channels, rows, channels), f32),
            dma((5,)),
            dma((3,)),
            dma((3,)),
            dma((1,)),
            dma((1,)),
            dma((1,)),
            dma((2 + 2 * columns,)),
        ],
        compiler_params=pltpu.CompilerParams(
            collective_id=0, has_side_effects=True, vmem_limit_bytes=40 * 2**20
        ),
    )(*operands[:4], step_size, *operands[4:])
    return out.reshape(frames, height, columns, half)


def dispatch(*arrays):
    hidden, noisy, in_weight, conv_weight = arrays[0], arrays[5], arrays[9], arrays[12]
    frames, height, columns, lat = noisy.shape
    sections, cores, clips_sp = (lax.axis_size(axis) for axis in ("section", "tp", "sp"))
    channels, half = conv_weight.shape[1:]
    whole_frame = hidden.shape[0] == height // 2 * (columns * sections // 2)
    if (
        whole_frame
        and cores == 2
        and clips_sp > 1
        and frames == sections
        and sections == 4
        and columns == 4
        and channels % 128 == 0
        and half % channels == 0
        and lat == 16
        and height == 16
    ):
        sizes = (sections, clips_sp, frames, height, columns, lat, channels)
        return fused_shards(sizes, *arrays)
    return shards(*arrays)


def solution(mesh):
    placed = (
        P(("groups", "sp", "section"), "tp"),
        P(None, "tp"),
        P(("groups", "tp")),
        P("tp", None),
        P(),
        P(("groups", "sp"), None, "section", None),
        P("groups"),
        P(),
        P(),
        P(None, None, "tp"),
        P("tp"),
        P(),
        P(None, "section", "tp"),
        P("tp"),
    )
    return jax.shard_map(
        dispatch,
        mesh=mesh,
        in_specs=placed,
        out_specs=P(("groups", "sp"), None, "section", "tp"),
        check_vma=False,
    )
```
